128 devices in a mesh: gx: 32 (over x, y, core), gy: 4 (over z).
Axes of the slice: x: 4, y: 4, z: 4, core: 2. Of those that a mesh axis runs over, the one named last changes fastest.
Arguments:
- signals: float32 [64, 32, 16, 128], P('gx', 'gy'), may hold values from -6 to 6
- tiles: bfloat16 [64, 32, 4, 128, 128], P('gx', 'gy'), may hold values from 0 to 0.00390625
- tile_dir: int32 [64, 32, 4], P('gx', 'gy'), may hold values from 0 to 8
- tile_mask: int32 [64, 32, 4], P('gx', 'gy'), may hold values 0 or 1
- live_rows: int32 [64, 32], P('gx', 'gy'), may hold values from 32 to 128
- bound_rows: int32 [64, 32], P('gx', 'gy'), may hold values from 1 to 32, as said below
- scale_coeffs: float32 [6, 5], replicated, may hold values from -1 to 1
- spectral_bound: float32 [1], replicated, may hold values from 2.5 to 4
Outputs:
- coefficients: float32 [6, 64, 32, 16, 128], P(None, 'gx', 'gy')
- energy: float32 [6, 16], replicated
The draws below stay inside these ranges and needn't reach their ends.
Inputs may be any that keep to these rules, and one draw needn't show every extreme that they name: `bound_rows`: in every draw, some blocks on every device have exactly 32 boundary rows.
All inputs are finite; a program needn't handle non-finite values. No bound on the sum of `tile_mask` on one device may be relied on, other than what follows from the above.
Results may differ from the reference program's by a relative error of at most 0.0003.
Values may be sent and summed in bfloat16 or wider, within the bound.
A program may use at most 64 MiB of HBM per device.

```python
import jax
import jax.numpy as jnp
from jax import lax

SIG = 16
SCALES = 6
DEG = 4
SLOTS = 4
TILE = 128
BMAX = 32
BY = 8
NBX = 64
NBY = 32


def draw_bound_rows(key, part):
    drawn = jax.random.randint(key, (NBX, NBY), 1, BMAX + 1, dtype=jnp.int32)
    columns = lax.broadcasted_iota(jnp.int32, (NBX, NBY), 1)
    return jnp.where(columns % BY == 0, jnp.int32(BMAX), drawn)


def with_ends(values, own_key, low, high):
    spot = [jax.random.randint(jax.random.fold_in(own_key, axis), (), 0, length) for axis, length in enumerate(values.shape)]
    main_axis = values.shape.index(max(values.shape))
    next_to = spot[:main_axis] + [(spot[main_axis] + 1) % values.shape[main_axis]] + spot[main_axis + 1:]
    return values.at[tuple(spot)].set(low).at[tuple(next_to)].set(high)


def steps_of(key, shape, cuts, low, high):
    def one(position, shards_of):
        steps = jax.random.uniform(jax.random.fold_in(jax.random.fold_in(key, 6), position), (shards_of,), jnp.float32, low / len(cuts), high / len(cuts))
        return jnp.repeat(jnp.exp(steps), shape[position] // shards_of).reshape((-1,) + (1,) * (len(shape) - position - 1))

    factor_of = one(*cuts[0])
    for cut in cuts[1:]:
        factor_of = factor_of * one(*cut)
    return factor_of


def scatter_about(key, dims, spread, limit, cuts=(), held_as=jnp.bfloat16):
    values = jax.random.normal(key, dims, jnp.float32) * spread
    if len(cuts) > 0:
        values = steps_of(key, dims, cuts, -0.22, 0.18) * values
    return jnp.clip(values, min=-limit, max=limit).astype(held_as)


def setup_inputs(seed: int = 0) -> dict:
    key_list = jax.random.split(jax.random.key(seed), 9)
    return {
        "signals": scatter_about(key_list[0], (NBX, NBY, SIG, TILE), 1.0, 6.0, ((0, 32), (1, 4)), jnp.float32),
        "tiles": jnp.clip(0.00390625 * jax.random.uniform(key_list[1], (NBX, NBY, SLOTS, TILE, TILE), jnp.float32) ** steps_of(key_list[1], (NBX, NBY, SLOTS, TILE, TILE), ((0, 32), (1, 4)), -0.2, 0.2), 0.0, 0.00390625).astype(jnp.bfloat16),
        "tile_dir": with_ends(jax.random.randint(key_list[2], (NBX, NBY, SLOTS), 0, 9), jax.random.fold_in(key_list[2], 1), 0, 8).astype(jnp.int32),
        "tile_mask": with_ends((jax.random.randint(key_list[3], (NBX, NBY, SLOTS), 0, 4) < 3).astype(jnp.int32), jax.random.fold_in(key_list[3], 1), 0, 1),
        "live_rows": with_ends(jax.random.randint(key_list[4], (NBX, NBY), TILE // 4, TILE + 1), jax.random.fold_in(key_list[4], 1), TILE // 4, TILE).astype(jnp.int32),
        "bound_rows": draw_bound_rows(jax.random.fold_in(key_list[8], 71), 0),
        "scale_coeffs": jnp.clip(jax.random.uniform(key_list[6], (SCALES, DEG + 1), jnp.float32, -1.0, 1.0), -1.0, 1.0),
        "spectral_bound": jnp.clip(jax.random.uniform(key_list[7], (1,), jnp.float32, 2.5, 4.0), 2.5, 4.0),
    }


def adjacency(values, tiles, tile_dir, tile_mask, bound_ind):
    own_rows = values.astype(jnp.bfloat16)
    edge_rows = (values * bound_ind[:, :, None, :]).astype(jnp.bfloat16)
    padded = jnp.pad(edge_rows, ((1, 1), (1, 1), (0, 0), (0, 0)))
    extent_x = values.shape[0]
    extent_y = values.shape[1]
    slot_list = []
    for slot_index in range(SLOTS):
        picked = jnp.zeros_like(own_rows)
        for direction in range(9):
            step_x = direction // 3 - 1
            step_y = direction % 3 - 1
            if direction == 4:
                source = own_rows
            else:
                source = padded[1 + step_x:1 + step_x + extent_x, 1 + step_y:1 + step_y + extent_y]
            matches = (tile_dir[:, :, slot_index] == direction)[:, :, None, None]
            picked = jnp.where(matches, source, picked)
        kept_mask = (tile_mask[:, :, slot_index] == 1)[:, :, None, None]
        picked = jnp.where(kept_mask, picked, jnp.zeros_like(picked))
        slot_list.append(picked)
    inputs = jnp.stack(slot_list, axis=2)

    def one_row(bundle):
        tile_row, input_row = bundle
        return jnp.einsum("jsrc,jsgc->jgr", tile_row.astype(jnp.float32), input_row.astype(jnp.float32))

    return lax.map(one_row, (tiles, inputs))


def scaled_laplacian(values, adjacent, degree, factor):
    return factor * (degree * values - adjacent) - values


def reference(signals, tiles, tile_dir, tile_mask, live_rows, bound_rows, scale_coeffs, spectral_bound):
    positions = lax.broadcasted_iota(jnp.int32, (1, 1, TILE), 2)
    live_ind = (positions < live_rows[:, :, None]).astype(jnp.float32)
    bound_ind = (positions < bound_rows[:, :, None]).astype(jnp.float32)
    initial = signals * live_ind[:, :, None, :]
    joined = jnp.concatenate([initial, live_ind[:, :, None, :]], axis=2)
    first_pass = adjacency(joined, tiles, tile_dir, tile_mask, bound_ind) * live_ind[:, :, None, :]
    degree = first_pass[:, :, SIG:, :]
    factor = 2.0 / spectral_bound[0]
    previous = initial
    current = scaled_laplacian(initial, first_pass[:, :, :SIG, :], degree, factor)
    totals = 0.5 * scale_coeffs[:, 0][:, None, None, None, None] * initial[None]
    totals = totals + scale_coeffs[:, 1][:, None, None, None, None] * current[None]
    for degree_index in range(2, DEG + 1):
        adjacent = adjacency(current, tiles, tile_dir, tile_mask, bound_ind) * live_ind[:, :, None, :]
        following = 2.0 * scaled_laplacian(current, adjacent, degree, factor) - previous
        previous = current
        current = following
        totals = totals + scale_coeffs[:, degree_index][:, None, None, None, None] * current[None]
    energy = jnp.sum(totals * totals, axis=(1, 2, 4)) / (NBX * NBY * TILE)
    return totals, energy
```

```python
import functools

import jax
import jax.numpy as jnp
from jax import lax
from jax.experimental import pallas as pl
from jax.experimental.pallas import tpu as pltpu
from jax.sharding import Mesh
from jax.sharding import PartitionSpec as P

MESH = pl.DeviceIdType.MESH
SIG, SCALES, DEG, SLOTS, TILE = 16, 6, 4, 4, 128
BX, BY = 2, 8
NB = BX * BY
GXN, GYN = 32, 4
ZERO = NB + (BX + 2) * (BY + 2)
NX = ZERO + 1
NODES = 64 * 32 * 128
DIRS = [(-1, 0), (1, 0), (0, -1), (0, 1), (-1, -1), (-1, 1), (1, -1), (1, 1)]
OPP = [DIRS.index((-dx, -dy)) for dx, dy in DIRS]


def coords(gx, gy):
    return (gx // 8, (gx // 2) % 4, gx % 2, gy)


def kernel(sig_h, til_h, dir_s, msk_s, liv_s, bnd_s, cof_s, spb_s,
           out_h, en_ref,
           sig, til, idx, x1, x2, x3, x4, cheb, tot, amul, op1, op2, op3, op4,
           rv1, rv2, rv3, rv4, ga, gb,
           ld_sem, snd, rcv, sa, ra, sb, rb, o_sem):
    x, y, c, z = (lax.axis_index(a) for a in ("gx_0", "gx_1", "gx_2", "gy"))
    gx = (x * 4 + y) * 2 + c
    gy = z
    sig_cp = pltpu.make_async_copy(sig_h, sig, ld_sem.at[NB])
    sig_cp.start()
    til_cp = []
    for b in range(NB):
        cp = pltpu.make_async_copy(til_h.at[b // BY, b % BY], til.at[b], ld_sem.at[b])
        cp.start()
        til_cp.append(cp)

    def exists(d):
        dx, dy = DIRS[d]
        ok = None
        for step, pos, n in ((dx, gx, GXN), (dy, gy, GYN)):
            if step == 0:
                continue
            this = pos > 0 if step < 0 else pos < n - 1
            ok = this if ok is None else jnp.logical_and(ok, this)
        return ok

    have = [exists(d) for d in range(8)]
    peer = [coords(gx + dx, gy + dy) for dx, dy in DIRS]
    xy = x * 4 + y
    zc = z * 2 + c
    a_peer = []
    for o in range(1, 8):
        t = (zc + o) % 8
        a_peer.append((x, y, t % 2, t // 2))
    b_peer = []
    for o in range(1, 16):
        t = (xy + o) % 16
        b_peer.append((t // 4, t % 4, c, z))

    recvs = (rv1, rv2, rv3, rv4)
    for rv in recvs:
        rv[...] = jnp.zeros_like(rv)
    bar = pltpu.get_barrier_semaphore()
    for d in range(8):
        @pl.when(have[d])
        def _(d=d):
            pl.semaphore_signal(bar, inc=1, device_id=peer[d], device_id_type=MESH)
    for p in a_peer + b_peer:
        pl.semaphore_signal(bar, inc=1, device_id=p, device_id_type=MESH)
    count = jnp.int32(22)
    for d in range(8):
        count = count + have[d].astype(jnp.int32)

    lane = lax.broadcasted_iota(jnp.int32, (1, TILE), 1)
    low = lane < 32
    f = 2.0 / spb_s[0, 0]

    for b in range(NB):
        i, j = b // BY, b % BY
        for s in range(SLOTS):
            d = dir_s[i, s, j]
            r = (d * 11) >> 5
            off = NB + (i + r) * (BY + 2) + (j + d - 3 * r)
            off = jnp.where(d == 4, b, off)
            idx[b * SLOTS + s] = jnp.where(msk_s[i, s, j] == 1, off, ZERO)

    def live_of(b):
        return (lane < liv_s[b // BY, b % BY]).astype(jnp.float32)

    def edge_of(b):
        return (lane < bnd_s[b // BY, b % BY]).astype(jnp.float32)

    for xb in (x1, x2, x3, x4):
        xb[ZERO] = jnp.zeros(xb.shape[1:], xb.dtype)

    def place(b, v, xb, packs):
        i, j = b // BY, b % BY
        xb[b] = v.astype(jnp.bfloat16)
        e = v * edge_of(b)
        xb[NB + (i + 1) * (BY + 2) + j + 1] = e.astype(jnp.bfloat16)
        jj = j + 2
        t, q = jj // 4, jj % 4
        e = pltpu.roll(e, 32 * q, 1) if q else e
        key = (i, t)
        packs[key] = e if key not in packs else packs[key] + e

    def flush(packs, op):
        for (i, t), v in packs.items():
            op[i, t] = v.astype(jnp.bfloat16)

    def copies(k, op, rv, d):
        dx, dy = DIRS[d]
        o = OPP[d]
        rows = {-1: pl.ds(0, 1), 1: pl.ds(1, 1), 0: pl.ds(0, 2)}[dx]
        cols = {-1: pl.ds(0, 1), 1: pl.ds(2, 1), 0: pl.ds(0, 3)}[dy]
        return pltpu.make_async_remote_copy(
            src_ref=op.at[rows, cols], dst_ref=rv.at[o, rows, cols],
            send_sem=snd.at[k, d], recv_sem=rcv.at[k, o],
            device_id=peer[d], device_id_type=MESH)

    def send(k, op, rv):
        for d in range(8):
            @pl.when(have[d])
            def _(d=d):
                copies(k, op, rv, d).start()

    def wait_recv(k, op, rv):
        for d in range(8):
            @pl.when(have[d])
            def _(d=d):
                dx, dy = DIRS[d]
                rows = {-1: pl.ds(1, 1), 1: pl.ds(0, 1), 0: pl.ds(0, 2)}[dx]
                cols = {-1: pl.ds(2, 1), 1: pl.ds(0, 1), 0: pl.ds(0, 3)}[dy]
                pltpu.make_async_remote_copy(
                    src_ref=op.at[rows, cols], dst_ref=rv.at[d, rows, cols],
                    send_sem=snd.at[k, d], recv_sem=rcv.at[k, d],
                    device_id=peer[d], device_id_type=MESH).wait_recv()

    def unpack(rv, xb):
        U, D, L, R, UL, UR, DL, DR = range(8)
        f32 = lambda a: a.astype(jnp.float32)
        rows = []
        rows.append((0, {0: f32(rv[U, 1, 0]) + f32(rv[UL, 1, 2]), 1: f32(rv[U, 1, 1]),
                         2: f32(rv[U, 1, 2]) + f32(rv[UR, 1, 0])}, range(1, 11)))
        for i in range(2):
            rows.append((i + 1, {0: f32(rv[L, i, 2]), 2: f32(rv[R, i, 0])}, (1, 10)))
        rows.append((3, {0: f32(rv[D, 0, 0]) + f32(rv[DL, 0, 2]), 1: f32(rv[D, 0, 1]),
                         2: f32(rv[D, 0, 2]) + f32(rv[DR, 0, 0])}, range(1, 11)))
        for r, tiles, cols in rows:
            for jj in cols:
                t, q = jj // 4, jj % 4
                v = tiles[t]
                v = pltpu.roll(v, TILE - 32 * q, 1) if q else v
                xb[NB + r * (BY + 2) + jj - 1] = jnp.where(low, v, 0.0).astype(jnp.bfloat16)

    def product(b, xb):
        acc = None
        for h in range(2):
            lhs = jnp.concatenate([xb[idx[b * SLOTS + 2 * h]], xb[idx[b * SLOTS + 2 * h + 1]]], axis=1)
            rhs = jnp.concatenate([til[b, 2 * h], til[b, 2 * h + 1]], axis=1)
            p = lax.dot_general(lhs, rhs, (((1,), (1,)), ((), ())), preferred_element_type=jnp.float32)
            acc = p if acc is None else acc + p
        return acc

    sig_cp.wait()
    packs = {}
    pad = lax.broadcasted_iota(jnp.int32, (16, TILE), 0) == 0
    for b in range(NB):
        live = live_of(b)
        v = sig[b // BY, b % BY] * live
        cheb[0, b] = v
        v32 = jnp.concatenate([v, jnp.where(pad, live, 0.0)], axis=0)
        place(b, v32, x1, packs)
    flush(packs, op1)
    pl.semaphore_wait(bar, count)
    send(0, op1, rv1)

    def add_totals(k):
        for s in range(SCALES):
            a = cof_s[s, k] * 0.5 if k == 0 else cof_s[s, k]
            for b in range(NB):
                t = a * cheb[k, b]
                tot[s, b] = t if k == 0 else tot[s, b] + t

    add_totals(0)
    for b in range(NB):
        til_cp[b].wait()
    wait_recv(0, op1, rv1)
    unpack(rv1, x1)
    packs = {}
    for b in range(NB):
        acc = product(b, x1)
        live = live_of(b)
        v = cheb[0, b]
        am = f * (acc[SIG:SIG + 1] * live) - 1.0
        amul[b] = jnp.broadcast_to(am, (8, TILE))
        cur = am * v - (f * live) * acc[:SIG]
        cheb[1, b] = cur
        place(b, cur, x2, packs)
    flush(packs, op2)
    send(1, op2, rv2)

    stages = ((1, x2, op2, rv2, x3, op3, rv3), (2, x3, op3, rv3, x4, op4, rv4), (3, x4, op4, rv4, None, None, None))
    for k, xb, op, rv, xn, opn, rvn in stages:
        add_totals(k)
        wait_recv(k, op, rv)
        unpack(rv, xb)
        packs = {}
        sq = [None] * SCALES
        for b in range(NB):
            acc = product(b, xb)
            am = amul[b]
            am = 2.0 * jnp.concatenate([am, am], axis=0)
            cur = am * cheb[k, b] - (2.0 * f * live_of(b)) * acc - cheb[k - 1, b]
            if k < 3:
                cheb[k + 1, b] = cur
                place(b, cur, xn, packs)
            else:
                for s in range(SCALES):
                    t = tot[s, b] + cof_s[s, 4] * cur
                    tot[s, b] = t
                    sq[s] = t * t if sq[s] is None else sq[s] + t * t
        if k < 3:
            flush(packs, opn)
            send(k + 1, opn, rvn)

    out_cp = pltpu.make_async_copy(tot, out_h, o_sem)
    out_cp.start()

    m = jnp.concatenate(sq, axis=0)
    hi = m.astype(jnp.bfloat16)
    r1 = m - hi.astype(jnp.float32)
    mid = r1.astype(jnp.bfloat16)
    lo = (r1 - mid.astype(jnp.float32)).astype(jnp.bfloat16)
    ones = jnp.ones((16, TILE), jnp.bfloat16)
    row = None
    for part in (lo, mid, hi):
        p = lax.dot_general(ones, part, (((1,), (1,)), ((), ())), preferred_element_type=jnp.float32)
        row = p if row is None else row + p
    row = jnp.concatenate([row[0:1], jnp.zeros((1, TILE - SCALES * SIG), jnp.float32)], axis=1)

    def phase(buf, mine, n, peers, s_sem, r_sem, value):
        buf[mine] = value
        for o, p in enumerate(peers):
            pltpu.make_async_remote_copy(
                src_ref=buf.at[mine], dst_ref=buf.at[mine], send_sem=s_sem.at[o],
                recv_sem=r_sem.at[mine], device_id=p, device_id_type=MESH).start()
        for o, p in enumerate(peers):
            src = (mine + o + 1) % n
            pltpu.make_async_remote_copy(
                src_ref=buf.at[mine], dst_ref=buf.at[src], send_sem=s_sem.at[o],
                recv_sem=r_sem.at[src], device_id=p, device_id_type=MESH).wait_recv()
        total = buf[0]
        for q in range(1, n):
            total = total + buf[q]
        return total

    part = phase(ga, zc, 8, a_peer, sa, ra, row)
    full = phase(gb, xy, 16, b_peer, sb, rb, part) * (1.0 / NODES)
    res = jnp.zeros((8, TILE), jnp.float32)
    sub = lax.broadcasted_iota(jnp.int32, (8, TILE), 0)
    full8 = jnp.broadcast_to(full, (8, TILE))
    for s in range(SCALES):
        v = pltpu.roll(full8, TILE - 16 * s, 1) if s else full8
        res = jnp.where(sub == s, v, res)
    en_ref[...] = res[:SCALES, :SIG]

    out_cp.wait()
    for k, (op, rv) in enumerate(((op1, rv1), (op2, rv2), (op3, rv3), (op4, rv4))):
        for d in range(8):
            @pl.when(have[d])
            def _(k=k, op=op, rv=rv, d=d):
                copies(k, op, rv, d).wait_send()
    for o, p in enumerate(a_peer):
        pltpu.make_async_remote_copy(
            src_ref=ga.at[zc], dst_ref=ga.at[zc], send_sem=sa.at[o], recv_sem=ra.at[zc],
            device_id=p, device_id_type=MESH).wait_send()
    for o, p in enumerate(b_peer):
        pltpu.make_async_remote_copy(
            src_ref=gb.at[xy], dst_ref=gb.at[xy], send_sem=sb.at[o], recv_sem=rb.at[xy],
            device_id=p, device_id_type=MESH).wait_send()


def shards(signals, tiles, tile_dir, tile_mask, live_rows, bound_rows, scale_coeffs, spectral_bound):
    bf, f32 = jnp.bfloat16, jnp.float32
    vm = pltpu.VMEM
    smem = pl.BlockSpec(memory_space=pltpu.SMEM)
    hbm = pl.BlockSpec(memory_space=pl.ANY)
    dma = pltpu.SemaphoreType.DMA
    out, energy = pl.pallas_call(
        kernel,
        out_shape=(jax.ShapeDtypeStruct((SCALES, NB, SIG, TILE), f32),
                   jax.ShapeDtypeStruct((SCALES, SIG), f32)),
        in_specs=[hbm, hbm] + [smem] * 6,
        out_specs=(hbm, pl.BlockSpec(memory_space=pltpu.VMEM)),
        scratch_shapes=[
            vm((BX, BY, SIG, TILE), f32), vm((NB, SLOTS, TILE, TILE), bf), pltpu.SMEM((NB * SLOTS,), jnp.int32),
            vm((NX, 32, TILE), bf), vm((NX, SIG, TILE), bf), vm((NX, SIG, TILE), bf), vm((NX, SIG, TILE), bf),
            vm((DEG, NB, SIG, TILE), f32), vm((SCALES, NB, SIG, TILE), f32), vm((NB, 8, TILE), f32),
            vm((2, 3, 32, TILE), bf), vm((2, 3, SIG, TILE), bf), vm((2, 3, SIG, TILE), bf), vm((2, 3, SIG, TILE), bf),
            vm((8, 2, 3, 32, TILE), bf), vm((8, 2, 3, SIG, TILE), bf), vm((8, 2, 3, SIG, TILE), bf), vm((8, 2, 3, SIG, TILE), bf),
            vm((8, 1, TILE), f32), vm((16, 1, TILE), f32),
            dma((NB + 1,)), dma((4, 8)), dma((4, 8)), dma((7,)), dma((8,)), dma((15,)), dma((16,)), dma,
        ],
        compiler_params=pltpu.CompilerParams(collective_id=0, has_side_effects=True),
        name="wavelet",
    )(signals, tiles, jnp.swapaxes(tile_dir, 1, 2), jnp.swapaxes(tile_mask, 1, 2), live_rows, bound_rows,
      scale_coeffs, spectral_bound.reshape(1, 1))
    return out.reshape(SCALES, BX, BY, SIG, TILE), energy


def solution(mesh):
    torus = Mesh(mesh.devices.reshape(4, 4, 2, mesh.shape["gy"]), ("gx_0", "gx_1", "gx_2", "gy"))
    gxs = ("gx_0", "gx_1", "gx_2")
    placed = (
        P(gxs, "gy", None, None),
        P(gxs, "gy", None, None, None),
        P(gxs, "gy", None),
        P(gxs, "gy", None),
        P(gxs, "gy"),
        P(gxs, "gy"),
        P(),
        P(),
    )
    return jax.shard_map(
        shards,
        mesh=torus,
        in_specs=placed,
        out_specs=(P(None, gxs, "gy", None, None), P()),
        check_vma=False,
    )
```

```python
import functools

import jax
import jax.numpy as jnp
from jax import lax
from jax.experimental import pallas as pl
from jax.experimental.pallas import tpu as pltpu
from jax.sharding import Mesh
from jax.sharding import PartitionSpec as P

MESH = pl.DeviceIdType.MESH
SIG, SCALES, DEG, SLOTS, TILE = 16, 6, 4, 4, 128
BX, BY = 2, 8
NB = BX * BY
GXN, GYN = 32, 4
ZERO = NB + (BX + 2) * (BY + 2)
NX = ZERO + 1
NODES = 64 * 32 * 128
DIRS = [(-1, 0), (1, 0), (0, -1), (0, 1), (-1, -1), (-1, 1), (1, -1), (1, 1)]
OPP = [DIRS.index((-dx, -dy)) for dx, dy in DIRS]


def coords(gx, gy):
    return (gx // 8, (gx // 2) % 4, gx % 2, gy)


def kernel(sig_h, til_h, dir_s, msk_s, liv_s, bnd_s, cof_s, spb_s,
           out_h, en_ref,
           sig, til, idx, loc, x1, x2, x3, x4, cheb, tot, amul, op1, op3, sp1, sp3, tp,
           rv1, rv3, rs1, rs3, tr, ga, gb,
           ld_sem, vs, vr, ss, sr, ts, tr_sem, sa, ra, sb, rb, o_sem):
    x, y, c, z = (lax.axis_index(a) for a in ("gx_0", "gx_1", "gx_2", "gy"))
    gx = (x * 4 + y) * 2 + c
    gy = z
    sig_cp = pltpu.make_async_copy(sig_h, sig, ld_sem.at[NB])
    sig_cp.start()
    til_cp = []
    for b in range(NB):
        cp = pltpu.make_async_copy(til_h.at[b // BY, b % BY], til.at[b], ld_sem.at[b])
        cp.start()
        til_cp.append(cp)

    def exists(d):
        dx, dy = DIRS[d]
        ok = None
        for step, pos, n in ((dx, gx, GXN), (dy, gy, GYN)):
            if step == 0:
                continue
            this = pos > 0 if step < 0 else pos < n - 1
            ok = this if ok is None else jnp.logical_and(ok, this)
        return ok

    have = [exists(d) for d in range(8)]
    peer = [coords(gx + dx, gy + dy) for dx, dy in DIRS]
    xy = x * 4 + y
    zc = z * 2 + c
    a_peer = []
    for o in range(1, 8):
        t = (zc + o) % 8
        a_peer.append((x, y, t % 2, t // 2))
    b_peer = []
    for o in range(1, 16):
        t = (xy + o) % 16
        b_peer.append((t // 4, t % 4, c, z))

    for buf in (rv1, rv3, rs1, rs3, tr):
        buf[...] = jnp.zeros_like(buf)
    bar = pltpu.get_barrier_semaphore()
    for d in range(8):
        @pl.when(have[d])
        def _(d=d):
            pl.semaphore_signal(bar, inc=1, device_id=peer[d], device_id_type=MESH)
    for p in a_peer + b_peer:
        pl.semaphore_signal(bar, inc=1, device_id=p, device_id_type=MESH)
    count = jnp.int32(22)
    for d in range(8):
        count = count + have[d].astype(jnp.int32)

    lane = lax.broadcasted_iota(jnp.int32, (1, TILE), 1)
    low = lane < 32
    f = 2.0 / spb_s[0, 0]
    bf16 = lambda a: a.astype(jnp.bfloat16)
    f32 = lambda a: a.astype(jnp.float32)

    for b in range(NB):
        i, j = b // BY, b % BY
        for s in range(SLOTS):
            d = dir_s[i, s, j]
            r = (d * 11) >> 5
            q = d - 3 * r
            off = NB + (i + r) * (BY + 2) + (j + q)
            off = jnp.where(d == 4, b, off)
            off = jnp.where(msk_s[i, s, j] == 1, off, ZERO)
            idx[b * SLOTS + s] = off
            away = r == 2 * i
            if j in (0, BY - 1):
                away = jnp.logical_or(away, q == (0 if j == 0 else 2))
            loc[b * SLOTS + s] = jnp.where(away, ZERO, off)

    def live_of(b):
        return (lane < liv_s[b // BY, b % BY]).astype(jnp.float32)

    def edge_of(b):
        return (lane < bnd_s[b // BY, b % BY]).astype(jnp.float32)

    RING = [(r, q) for r in (1, 4) for q in range(1, 11)] + [(r, q) for r in (2, 3) for q in (1, 10)]
    slot_of = lambda er, ec: NB + (er - 1) * (BY + 2) + ec - 1
    for xb in (x1, x2, x3, x4):
        xb[ZERO] = jnp.zeros(xb.shape[1:], xb.dtype)
    for xb in (x2, x4):
        for er, ec in RING:
            xb[slot_of(er, ec)] = jnp.zeros(xb.shape[1:], xb.dtype)

    def shift(v, q):
        q = q % 4
        return pltpu.roll(v, 32 * q, 1) if q else v

    def add_to(packs, i, j, v):
        key = (i, (j + 2) // 4)
        v = shift(v, j + 2)
        packs[key] = v if key not in packs else packs[key] + v

    def place(b, v, xb, packs=None):
        i, j = b // BY, b % BY
        xb[b] = bf16(v)
        e = v * edge_of(b)
        xb[slot_of(i + 2, j + 2)] = bf16(e)
        if packs is not None:
            add_to(packs, i, j, e)

    def flush(packs, buf, tile_first):
        for (i, t), v in packs.items():
            if tile_first:
                buf[t, i] = bf16(v)
            else:
                buf[i, t] = bf16(v)

    def part_v(dx, dy):
        return ({-1: pl.ds(0, 1), 1: pl.ds(2, 1), 0: pl.ds(0, 3)}[dy],)

    def part_s(dx, dy):
        return ({-1: pl.ds(0, 1), 1: pl.ds(1, 1), 0: pl.ds(0, 2)}[dx],
                {-1: pl.ds(0, 1), 1: pl.ds(2, 1), 0: pl.ds(0, 3)}[dy])

    def part_t(dx, dy):
        return ({-1: pl.ds(0, 1), 1: pl.ds(1, 1), 0: pl.ds(0, 2)}[dx],
                {-1: pl.ds(0, 2), 1: pl.ds(8, 2), 0: pl.ds(0, 10)}[dy])

    def descriptor(src, dst, part, s_sem, r_sem, d, o, at):
        return pltpu.make_async_remote_copy(
            src_ref=src.at[at], dst_ref=dst.at[(o,) + at], send_sem=s_sem.at[d],
            recv_sem=r_sem.at[o], device_id=peer[d], device_id_type=MESH)

    started = []

    def send(src, dst, part, s_sem, r_sem):
        started.append((src, dst, part, s_sem, r_sem))
        for d in (4, 5, 6, 7, 0, 1, 2, 3):
            @pl.when(have[d])
            def _(d=d):
                descriptor(src, dst, part, s_sem, r_sem, d, OPP[d], part(*DIRS[d])).start()

    def wait_recv(src, dst, part, s_sem, r_sem):
        for d in range(8):
            @pl.when(have[d])
            def _(d=d):
                descriptor(src, dst, part, s_sem, r_sem, d, d, part(*DIRS[OPP[d]])).wait_recv()

    v_args = ((op1, rv1, part_v, vs.at[0], vr.at[0]), (op3, rv3, part_v, vs.at[1], vr.at[1]))
    s_args = ((sp1, rs1, part_s, ss.at[0], sr.at[0]), (sp3, rs3, part_s, ss.at[1], sr.at[1]))
    t_args = (tp, tr, part_t, ts, tr_sem)
    U, D, L, R, UL, UR, DL, DR = range(8)
    left = lane < 64

    def rows_of(op, rv):
        rows = []
        for r in range(6):
            i = r % 2
            if r in (2, 3):
                lo, hi, mine = rv[L, 2, i], rv[R, 0, i], [op[t, i] for t in range(3)]
            else:
                u, ul, ur = (U, UL, UR) if r < 2 else (D, DL, DR)
                lo, hi, mine = rv[ul, 2, i], rv[ur, 0, i], [rv[u, t, i] for t in range(3)]
            mine = [f32(v) for v in mine]
            rows.append([jnp.where(left, f32(lo), mine[0]), mine[1], jnp.where(left, mine[2], f32(hi))])
        return rows

    def unpack(rows, xb):
        for er, ec in RING:
            v = jnp.where(low, shift(rows[er][ec // 4], -ec), 0.0)
            xb[slot_of(er, ec)] = bf16(v)

    def contract(lhs, rhs):
        return lax.dot_general(lhs, rhs, (((1,), (1,)), ((), ())), preferred_element_type=jnp.float32)

    def product(b, xb, table, rows=TILE):
        acc = None
        for h in range(2):
            pick = [xb[table[b * SLOTS + 2 * h + n]] for n in range(2)]
            rhs = [til[b, 2 * h + n, :rows] for n in range(2)]
            p = contract(jnp.concatenate(pick, axis=1), jnp.concatenate(rhs, axis=1))
            acc = p if acc is None else acc + p
        return acc

    sig_cp.wait()
    packs = {}
    pad = lax.broadcasted_iota(jnp.int32, (16, TILE), 0) == 0
    for b in range(NB):
        live = live_of(b)
        v = sig[b // BY, b % BY] * live
        cheb[0, b] = v
        place(b, jnp.concatenate([v, jnp.where(pad, live, 0.0)], axis=0), x1, packs)
    flush(packs, op1, True)

    def corner(b, wanted):
        i, j = b // BY, b % BY
        total = None
        for d, group in wanted:
            acc = None
            for s in range(SLOTS):
                on = jnp.logical_and(dir_s[i, s, j] == d, msk_s[i, s, j] == 1).astype(jnp.float32)
                t = f32(til[b, s, :32]) * on
                acc = t if acc is None else acc + t
            acc = shift(jnp.where(low, acc, 0.0), group)
            total = acc if total is None else total + acc
        inside = lax.broadcasted_iota(jnp.int32, (32, TILE), 0) < bnd_s[i, j]
        return bf16(jnp.where(inside, total, 0.0))

    def local_part(b, xb, scale, prev, first, packs):
        acc = product(b, xb, loc, 32)
        v = cheb[2 * (1 - first), b, :, :32]
        fl = scale * live_of(b)[:, :32]
        if first:
            am = fl * acc[SIG:SIG + 1] - 1.0
            out = am * v - fl * acc[:SIG]
        else:
            am = amul[b, :1, :32]
            out = 2.0 * am * v - fl * acc - prev
        out = out * edge_of(b)[:, :32]
        add_to(packs, b // BY, b % BY, jnp.concatenate([out, jnp.zeros((SIG, TILE - 32), jnp.float32)], axis=1))

    packs = {}
    for b in range(NB):
        til_cp[b].wait()
        i, j = b // BY, b % BY
        dx = 2 * i
        tp[i, 1 + j] = corner(b, [(3 * dx + q, j + 1 + q) for q in range(3)])
        if j == 0:
            tp[i, 0] = corner(b, [(3 - 3 * i, 1), (6 - 3 * i, 2)])
        if j == BY - 1:
            tp[i, 9] = corner(b, [(5 - 3 * i, 2), (8 - 3 * i, 3)])
        local_part(b, x1, f, None, 1, packs)
    flush(packs, sp1, False)

    pl.semaphore_wait(bar, count)
    send(*v_args[0])
    send(*s_args[0])
    send(*t_args)

    def add_totals(k):
        for s in range(SCALES):
            a = cof_s[s, k] * 0.5 if k == 0 else cof_s[s, k]
            for b in range(NB):
                t = a * cheb[k, b]
                tot[s, b] = t if k == 0 else tot[s, b] + t

    def advance_ring(rows, rs, xn, first):
        wide = [[bf16(v) for v in r] for r in rows]

        def row_input(er, ec):
            t, q = ec // 4, ec % 4
            if q == 0:
                return bf16(jnp.where(lane >= 96, rows[er][t - 1], rows[er][t]))
            if q == 3:
                return bf16(jnp.where(low, rows[er][t + 1], rows[er][t]))
            return wide[er][t]

        def column_input(er, ec):
            g = (ec + 1) % 4
            at = jnp.logical_and(lane >= 32 * g, lane < 32 * g + 32)
            return bf16(jnp.where(at, shift(rows[er + 1][ec // 4], 1), rows[er][ec // 4]))

        inputs = {}
        for er, ec in RING:
            side = 0 if ec == 1 else 2 if ec == 10 else 1
            level = 0 if er == 1 else 2 if er == 4 else 1
            owner = {(0, 0): UL, (0, 1): U, (0, 2): UR, (1, 0): L, (1, 2): R,
                     (2, 0): DL, (2, 1): D, (2, 2): DR}[(level, side)]
            i = {1: 1, 2: 0, 3: 1, 4: 0}[er]
            j = (ec - 2) % BY
            base = er - i
            lhs, rhs = row_input(er + (1 if i else -1), ec), tr[owner, i, 1 + j]
            if j in (0, BY - 1):
                col = ec - 1 if j == 0 else ec + 1
                if (base, col) not in inputs:
                    inputs[(base, col)] = column_input(base, col)
                lhs = jnp.concatenate([lhs, inputs[(base, col)]], axis=1)
                rhs = jnp.concatenate([rhs, tr[owner, i, 0 if j == 0 else 9]], axis=1)
            acc = contract(lhs, rhs)
            own = shift(f32(rs[owner, i, ((j + 2) // 4)]), -ec)[:, :32]
            if first:
                v = shift(rows[er][ec // 4], -ec)[:SIG, :32]
                new = own + f * (acc[SIG:SIG + 1] * v - acc[:SIG])
            else:
                new = own - (2.0 * f) * acc
            xn[slot_of(er, ec), :, pl.ds(0, 32)] = bf16(new)

    add_totals(0)
    wait_recv(*v_args[0])
    rows = rows_of(op1, rv1)
    unpack(rows, x1)
    for b in range(NB):
        acc = product(b, x1, idx)
        live = live_of(b)
        v = cheb[0, b]
        am = f * (acc[SIG:SIG + 1] * live) - 1.0
        amul[b] = jnp.broadcast_to(am, (8, TILE))
        cur = am * v - (f * live) * acc[:SIG]
        cheb[1, b] = cur
        place(b, cur, x2)
    wait_recv(*s_args[0])
    wait_recv(*t_args)
    advance_ring(rows, rs1, x2, 1)

    def step(b, k, xb):
        acc = product(b, xb, idx)
        am = amul[b]
        am = 2.0 * jnp.concatenate([am, am], axis=0)
        return am * cheb[k, b] - (2.0 * f * live_of(b)) * acc - cheb[k - 1, b]

    packs = {}
    for b in range(NB):
        cur = step(b, 1, x2)
        cheb[2, b] = cur
        place(b, cur, x3, packs)
    flush(packs, op3, True)
    send(*v_args[1])
    packs = {}
    for b in range(NB):
        local_part(b, x3, 2.0 * f, cheb[1, b, :, :32], 0, packs)
    flush(packs, sp3, False)
    send(*s_args[1])
    add_totals(1)
    add_totals(2)

    wait_recv(*v_args[1])
    rows = rows_of(op3, rv3)
    unpack(rows, x3)
    for b in range(NB):
        cur = step(b, 2, x3)
        cheb[3, b] = cur
        place(b, cur, x4)
    wait_recv(*s_args[1])
    advance_ring(rows, rs3, x4, 0)
    sq = [None] * SCALES
    for b in range(NB):
        cur = step(b, 3, x4)
        for s in range(SCALES):
            t = tot[s, b] + cof_s[s, 3] * cheb[3, b] + cof_s[s, 4] * cur
            tot[s, b] = t
            sq[s] = t * t if sq[s] is None else sq[s] + t * t

    out_cp = pltpu.make_async_copy(tot, out_h, o_sem)
    out_cp.start()

    m = jnp.concatenate(sq, axis=0)
    hi = m.astype(jnp.bfloat16)
    r1 = m - hi.astype(jnp.float32)
    mid = r1.astype(jnp.bfloat16)
    lo = (r1 - mid.astype(jnp.float32)).astype(jnp.bfloat16)
    ones = jnp.ones((16, TILE), jnp.bfloat16)
    row = None
    for part in (lo, mid, hi):
        p = lax.dot_general(ones, part, (((1,), (1,)), ((), ())), preferred_element_type=jnp.float32)
        row = p if row is None else row + p
    row = jnp.concatenate([row[0:1], jnp.zeros((1, TILE - SCALES * SIG), jnp.float32)], axis=1)

    def phase(buf, mine, n, peers, s_sem, r_sem, value):
        buf[mine] = value
        for o, p in enumerate(peers):
            pltpu.make_async_remote_copy(
                src_ref=buf.at[mine], dst_ref=buf.at[mine], send_sem=s_sem.at[o],
                recv_sem=r_sem.at[mine], device_id=p, device_id_type=MESH).start()
        for o, p in enumerate(peers):
            src = (mine + o + 1) % n
            pltpu.make_async_remote_copy(
                src_ref=buf.at[mine], dst_ref=buf.at[src], send_sem=s_sem.at[o],
                recv_sem=r_sem.at[src], device_id=p, device_id_type=MESH).wait_recv()
        total = buf[0]
        for q in range(1, n):
            total = total + buf[q]
        return total

    part = phase(ga, zc, 8, a_peer, sa, ra, row)
    full = phase(gb, xy, 16, b_peer, sb, rb, part) * (1.0 / NODES)
    res = jnp.zeros((8, TILE), jnp.float32)
    sub = lax.broadcasted_iota(jnp.int32, (8, TILE), 0)
    full8 = jnp.broadcast_to(full, (8, TILE))
    for s in range(SCALES):
        v = pltpu.roll(full8, TILE - 16 * s, 1) if s else full8
        res = jnp.where(sub == s, v, res)
    en_ref[...] = res[:SCALES, :SIG]

    out_cp.wait()
    for src, dst, part, s_sem, r_sem in started:
        for d in range(8):
            @pl.when(have[d])
            def _(src=src, dst=dst, part=part, s_sem=s_sem, r_sem=r_sem, d=d):
                descriptor(src, dst, part, s_sem, r_sem, d, OPP[d], part(*DIRS[d])).wait_send()
    for o, p in enumerate(a_peer):
        pltpu.make_async_remote_copy(
            src_ref=ga.at[zc], dst_ref=ga.at[zc], send_sem=sa.at[o], recv_sem=ra.at[zc],
            device_id=p, device_id_type=MESH).wait_send()
    for o, p in enumerate(b_peer):
        pltpu.make_async_remote_copy(
            src_ref=gb.at[xy], dst_ref=gb.at[xy], send_sem=sb.at[o], recv_sem=rb.at[xy],
            device_id=p, device_id_type=MESH).wait_send()


def shards(signals, tiles, tile_dir, tile_mask, live_rows, bound_rows, scale_coeffs, spectral_bound):
    bf, f32 = jnp.bfloat16, jnp.float32
    vm = pltpu.VMEM
    smem = pl.BlockSpec(memory_space=pltpu.SMEM)
    hbm = pl.BlockSpec(memory_space=pl.ANY)
    dma = pltpu.SemaphoreType.DMA
    out, energy = pl.pallas_call(
        kernel,
        out_shape=(jax.ShapeDtypeStruct((SCALES, NB, SIG, TILE), f32),
                   jax.ShapeDtypeStruct((SCALES, SIG), f32)),
        in_specs=[hbm, hbm] + [smem] * 6,
        out_specs=(hbm, pl.BlockSpec(memory_space=pltpu.VMEM)),
        scratch_shapes=[
            vm((BX, BY, SIG, TILE), f32), vm((NB, SLOTS, TILE, TILE), bf),
            pltpu.SMEM((NB * SLOTS,), jnp.int32), pltpu.SMEM((NB * SLOTS,), jnp.int32),
            vm((NX, 32, TILE), bf), vm((NX, SIG, TILE), bf), vm((NX, SIG, TILE), bf), vm((NX, SIG, TILE), bf),
            vm((DEG, NB, SIG, TILE), f32), vm((SCALES, NB, SIG, TILE), f32), vm((NB, 8, TILE), f32),
            vm((3, 2, 32, TILE), bf), vm((3, 2, SIG, TILE), bf),
            vm((2, 3, SIG, TILE), bf), vm((2, 3, SIG, TILE), bf), vm((2, 10, 32, TILE), bf),
            vm((8, 3, 2, 32, TILE), bf), vm((8, 3, 2, SIG, TILE), bf),
            vm((8, 2, 3, SIG, TILE), bf), vm((8, 2, 3, SIG, TILE), bf), vm((8, 2, 10, 32, TILE), bf),
            vm((8, 1, TILE), f32), vm((16, 1, TILE), f32),
            dma((NB + 1,)), dma((2, 8)), dma((2, 8)), dma((2, 8)), dma((2, 8)), dma((8,)), dma((8,)),
            dma((7,)), dma((8,)), dma((15,)), dma((16,)), dma,
        ],
        compiler_params=pltpu.CompilerParams(collective_id=0, has_side_effects=True),
        name="wavelet",
    )(signals, tiles, jnp.swapaxes(tile_dir, 1, 2), jnp.swapaxes(tile_mask, 1, 2), live_rows, bound_rows,
      scale_coeffs, spectral_bound.reshape(1, 1))
    return out.reshape(SCALES, BX, BY, SIG, TILE), energy


def solution(mesh):
    torus = Mesh(mesh.devices.reshape(4, 4, 2, mesh.shape["gy"]), ("gx_0", "gx_1", "gx_2", "gy"))
    gxs = ("gx_0", "gx_1", "gx_2")
    placed = (
        P(gxs, "gy", None, None),
        P(gxs, "gy", None, None, None),
        P(gxs, "gy", None),
        P(gxs, "gy", None),
        P(gxs, "gy"),
        P(gxs, "gy"),
        P(),
        P(),
    )
    return jax.shard_map(
        shards,
        mesh=torus,
        in_specs=placed,
        out_specs=(P(None, gxs, "gy", None, None), P()),
        check_vma=False,
    )
```

```python
import functools

import jax
import jax.numpy as jnp
from jax import lax
from jax.experimental import pallas as pl
from jax.experimental.pallas import tpu as pltpu
from jax.sharding import Mesh
from jax.sharding import PartitionSpec as P

MESH = pl.DeviceIdType.MESH
SIG, SCALES, DEG, SLOTS, TILE = 16, 6, 4, 4, 128
BX, BY = 2, 8
NB = BX * BY
GXN, GYN = 32, 4
ZERO = NB + (BX + 2) * (BY + 2)
NX = ZERO + 1
NODES = 64 * 32 * 128
DIRS = [(-1, 0), (1, 0), (0, -1), (0, 1), (-1, -1), (-1, 1), (1, -1), (1, 1)]
OPP = [DIRS.index((-dx, -dy)) for dx, dy in DIRS]


def coords(gx, gy):
    return (gx // 8, (gx // 2) % 4, gx % 2, gy)


def kernel(sig_h, til_h, dir_h, msk_h, liv_h, bnd_h, cof_h, spb_h,
           tot, en_ref,
           dir_s, msk_s, liv_s, bnd_s, cof_s, spb_s, sig, til, idx, loc, x1, x2, x3, x4, cheb, amul, op1, op3, sp1, sp3, tp,
           rv1, rv3, rs1, rs3, tr, ga, gb,
           ld_sem, vs, vr, ss, sr, ts, tr_sem, sa, ra, sb, rb):
    x, y, c, z = (lax.axis_index(a) for a in ("gx_0", "gx_1", "gx_2", "gy"))
    gx = (x * 4 + y) * 2 + c
    gy = z
    early = []
    for n, (src, dst) in enumerate(((sig_h, sig), (liv_h, liv_s), (bnd_h, bnd_s), (dir_h, dir_s), (msk_h, msk_s),
                                    (cof_h, cof_s), (spb_h, spb_s))):
        cp = pltpu.make_async_copy(src, dst, ld_sem.at[n])
        cp.start()
        early.append(cp)

    def exists(d):
        dx, dy = DIRS[d]
        ok = None
        for step, pos, n in ((dx, gx, GXN), (dy, gy, GYN)):
            if step == 0:
                continue
            this = pos > 0 if step < 0 else pos < n - 1
            ok = this if ok is None else jnp.logical_and(ok, this)
        return ok

    have = [exists(d) for d in range(8)]
    peer = [coords(gx + dx, gy + dy) for dx, dy in DIRS]
    xy = x * 4 + y
    zc = z * 2 + c
    a_peer = []
    for o in range(1, 8):
        t = (zc + o) % 8
        a_peer.append((x, y, t % 2, t // 2))
    b_peer = []
    for o in range(1, 16):
        t = (xy + o) % 16
        b_peer.append((t // 4, t % 4, c, z))

    bar = pltpu.get_barrier_semaphore()
    for d in (4, 5, 6, 7, 0, 1, 2, 3):
        @pl.when(have[d])
        def _(d=d):
            pl.semaphore_signal(bar, inc=1, device_id=peer[d], device_id_type=MESH)
    for p in a_peer + b_peer:
        pl.semaphore_signal(bar, inc=1, device_id=p, device_id_type=MESH)
    count = jnp.int32(22)
    for d in range(8):
        count = count + have[d].astype(jnp.int32)
    til_cp = []
    for n in range(4):
        cp = pltpu.make_async_copy(til_h.at[n // 2, pl.ds(4 * (n % 2), 4)], til.at[pl.ds(4 * n, 4)], ld_sem.at[7 + n])
        cp.start()
        til_cp.append(cp)
    for cp in early:
        cp.wait()

    lane = lax.broadcasted_iota(jnp.int32, (1, TILE), 1)
    low = lane < 32
    f = 2.0 / spb_s[0]
    bf16 = lambda a: a.astype(jnp.bfloat16)
    f32 = lambda a: a.astype(jnp.float32)

    def live_of(b):
        return (lane < liv_s[b // BY, b % BY]).astype(jnp.float32)

    def edge_of(b):
        return (lane < bnd_s[b // BY, b % BY]).astype(jnp.float32)

    RING = [(r, q) for r in (1, 4) for q in range(1, 11)] + [(r, q) for r in (2, 3) for q in (1, 10)]
    slot_of = lambda er, ec: NB + (er - 1) * (BY + 2) + ec - 1
    def shift(v, q):
        q = q % 4
        return pltpu.roll(v, 32 * q, 1) if q else v

    def add_to(packs, i, j, v):
        key = (i, (j + 2) // 4)
        v = shift(v, j + 2)
        packs[key] = v if key not in packs else packs[key] + v

    def place(b, v, xb, packs=None):
        i, j = b // BY, b % BY
        xb[b] = bf16(v)
        e = v * edge_of(b)
        xb[slot_of(i + 2, j + 2)] = bf16(e)
        if packs is not None:
            add_to(packs, i, j, e)

    def flush(packs, buf, tile_first):
        for (i, t), v in packs.items():
            if tile_first:
                buf[t, i] = bf16(v)
            else:
                buf[i, t] = v

    def part_v(dx, dy):
        return ({-1: pl.ds(0, 1), 1: pl.ds(2, 1), 0: pl.ds(0, 3)}[dy],)

    def part_s(dx, dy):
        return ({-1: pl.ds(0, 1), 1: pl.ds(1, 1), 0: pl.ds(0, 2)}[dx],
                {-1: pl.ds(0, 1), 1: pl.ds(2, 1), 0: pl.ds(0, 3)}[dy])

    def part_t(dx, dy):
        return ({-1: pl.ds(0, 1), 1: pl.ds(1, 1), 0: pl.ds(0, 2)}[dx],
                {-1: pl.ds(0, 2), 1: pl.ds(8, 2), 0: pl.ds(0, 10)}[dy])

    def descriptor(src, dst, part, s_sem, r_sem, d, o, at):
        return pltpu.make_async_remote_copy(
            src_ref=src.at[at], dst_ref=dst.at[(o,) + at], send_sem=s_sem.at[d],
            recv_sem=r_sem.at[o], device_id=peer[d], device_id_type=MESH)

    started = []

    def send(src, dst, part, s_sem, r_sem):
        started.append((src, dst, part, s_sem, r_sem))
        for d in (4, 5, 6, 7, 0, 1, 2, 3):
            @pl.when(have[d])
            def _(d=d):
                descriptor(src, dst, part, s_sem, r_sem, d, OPP[d], part(*DIRS[d])).start()

    def wait_recv(src, dst, part, s_sem, r_sem):
        for d in range(8):
            @pl.when(have[d])
            def _(d=d):
                descriptor(src, dst, part, s_sem, r_sem, d, d, part(*DIRS[OPP[d]])).wait_recv()

    v_args = ((op1, rv1, part_v, vs.at[0], vr.at[0]), (op3, rv3, part_v, vs.at[1], vr.at[1]))
    s_args = ((sp1, rs1, part_s, ss.at[0], sr.at[0]), (sp3, rs3, part_s, ss.at[1], sr.at[1]))
    t_args = (tp, tr, part_t, ts, tr_sem)
    U, D, L, R, UL, UR, DL, DR = range(8)
    left = lane < 64

    def rows_of(op, rv):
        rows = []
        for r in range(6):
            i = r % 2
            if r in (2, 3):
                lo, hi, mine = rv[L, 2, i], rv[R, 0, i], [op[t, i] for t in range(3)]
            else:
                u, ul, ur = (U, UL, UR) if r < 2 else (D, DL, DR)
                lo, hi, mine = rv[ul, 2, i], rv[ur, 0, i], [rv[u, t, i] for t in range(3)]
            mine = [f32(v) for v in mine]
            rows.append([jnp.where(left, f32(lo), mine[0]), mine[1], jnp.where(left, mine[2], f32(hi))])
        return rows

    def unpack(rows, xb):
        for er, ec in RING:
            v = jnp.where(low, shift(rows[er][ec // 4], -ec), 0.0)
            xb[slot_of(er, ec)] = bf16(v)

    def contract(lhs, rhs):
        return lax.dot_general(lhs, rhs, (((1,), (1,)), ((), ())), preferred_element_type=jnp.float32)

    def product(b, xb, table, rows=TILE):
        acc = None
        for h in range(2):
            pick = [xb[table[b * SLOTS + 2 * h + n]] for n in range(2)]
            rhs = [til[b, 2 * h + n, :rows] for n in range(2)]
            p = contract(jnp.concatenate(pick, axis=1), jnp.concatenate(rhs, axis=1))
            acc = p if acc is None else acc + p
        return acc

    packs = {}
    pad = lax.broadcasted_iota(jnp.int32, (16, TILE), 0) == 0
    for b in range(NB):
        live = live_of(b)
        v = sig[b // BY, b % BY] * live
        cheb[0, b] = v
        place(b, jnp.concatenate([v, jnp.where(pad, live, 0.0)], axis=0), x1, packs)
    flush(packs, op1, True)
    pl.semaphore_wait(bar, count)
    send(*v_args[0])

    for d in range(8):
        @pl.when(jnp.logical_not(have[d]))
        def _(d=d):
            for buf in (rv1, rv3, rs1, rs3, tr):
                buf[d] = jnp.zeros(buf.shape[1:], buf.dtype)

    for b in range(NB):
        i, j = b // BY, b % BY
        for s in range(SLOTS):
            d = dir_s[i, s, j]
            r = (d * 11) >> 5
            q = d - 3 * r
            off = NB + (i + r) * (BY + 2) + (j + q)
            off = jnp.where(d == 4, b, off)
            off = jnp.where(msk_s[i, s, j] == 1, off, ZERO)
            idx[b * SLOTS + s] = off
            away = r == 2 * i
            if j in (0, BY - 1):
                away = jnp.logical_or(away, q == (0 if j == 0 else 2))
            loc[b * SLOTS + s] = jnp.where(away, ZERO, off)

    for xb in (x1, x2, x3, x4):
        xb[ZERO] = jnp.zeros(xb.shape[1:], xb.dtype)
    for xb in (x2, x4):
        for er, ec in RING:
            xb[slot_of(er, ec)] = jnp.zeros(xb.shape[1:], xb.dtype)


    def corner(b, wanted):
        i, j = b // BY, b % BY
        total = None
        for d, group in wanted:
            acc = None
            for s in range(SLOTS):
                on = jnp.logical_and(dir_s[i, s, j] == d, msk_s[i, s, j] == 1).astype(jnp.float32)
                t = f32(til[b, s, :32]) * on
                acc = t if acc is None else acc + t
            acc = shift(jnp.where(low, acc, 0.0), group)
            total = acc if total is None else total + acc
        inside = lax.broadcasted_iota(jnp.int32, (32, TILE), 0) < bnd_s[i, j]
        return bf16(jnp.where(inside, total, 0.0))

    def local_part(b, xb, scale, prev, first, packs):
        acc = product(b, xb, loc, 32)
        v = cheb[2 * (1 - first), b, :, :32]
        fl = scale * live_of(b)[:, :32]
        if first:
            am = fl * acc[SIG:SIG + 1] - 1.0
            out = am * v - fl * acc[:SIG]
        else:
            am = amul[b, :1, :32]
            out = 2.0 * am * v - fl * acc - prev
        out = out * edge_of(b)[:, :32]
        add_to(packs, b // BY, b % BY, jnp.concatenate([out, jnp.zeros((SIG, TILE - 32), jnp.float32)], axis=1))

    packs = {}
    for cp in til_cp:
        cp.wait()
    for b in range(NB):
        i, j = b // BY, b % BY
        dx = 2 * i
        tp[i, 1 + j] = corner(b, [(3 * dx + q, j + 1 + q) for q in range(3)])
        if j == 0:
            tp[i, 0] = corner(b, [(3 - 3 * i, 1), (6 - 3 * i, 2)])
        if j == BY - 1:
            tp[i, 9] = corner(b, [(5 - 3 * i, 2), (8 - 3 * i, 3)])
        local_part(b, x1, f, None, 1, packs)
    flush(packs, sp1, False)

    send(*s_args[0])
    send(*t_args)

    def add_totals(k):
        for s in range(SCALES):
            a = cof_s[s, k] * 0.5 if k == 0 else cof_s[s, k]
            for b in range(NB):
                t = a * cheb[k, b]
                tot[s, b] = t if k == 0 else tot[s, b] + t

    def advance_ring(rows, rs, xn, first):
        wide = [[bf16(v) for v in r] for r in rows]

        def row_input(er, ec):
            t, q = ec // 4, ec % 4
            if q == 0:
                return bf16(jnp.where(lane >= 96, rows[er][t - 1], rows[er][t]))
            if q == 3:
                return bf16(jnp.where(low, rows[er][t + 1], rows[er][t]))
            return wide[er][t]

        def column_input(er, ec):
            g = (ec + 1) % 4
            at = jnp.logical_and(lane >= 32 * g, lane < 32 * g + 32)
            return bf16(jnp.where(at, shift(rows[er + 1][ec // 4], 1), rows[er][ec // 4]))

        inputs = {}
        for er, ec in RING:
            side = 0 if ec == 1 else 2 if ec == 10 else 1
            level = 0 if er == 1 else 2 if er == 4 else 1
            owner = {(0, 0): UL, (0, 1): U, (0, 2): UR, (1, 0): L, (1, 2): R,
                     (2, 0): DL, (2, 1): D, (2, 2): DR}[(level, side)]
            i = {1: 1, 2: 0, 3: 1, 4: 0}[er]
            j = (ec - 2) % BY
            base = er - i
            lhs, rhs = row_input(er + (1 if i else -1), ec), tr[owner, i, 1 + j]
            if j in (0, BY - 1):
                col = ec - 1 if j == 0 else ec + 1
                if (base, col) not in inputs:
                    inputs[(base, col)] = column_input(base, col)
                lhs = jnp.concatenate([lhs, inputs[(base, col)]], axis=1)
                rhs = jnp.concatenate([rhs, tr[owner, i, 0 if j == 0 else 9]], axis=1)
            acc = contract(lhs, rhs)
            own = shift(rs[owner, i, (j + 2) // 4], -ec)[:, :32]
            if first:
                v = shift(rows[er][ec // 4], -ec)[:SIG, :32]
                new = own + f * (acc[SIG:SIG + 1] * v - acc[:SIG])
            else:
                new = own - (2.0 * f) * acc
            xn[slot_of(er, ec), :, pl.ds(0, 32)] = bf16(new)

    add_totals(0)
    wait_recv(*v_args[0])
    rows = rows_of(op1, rv1)
    unpack(rows, x1)
    for b in range(NB):
        acc = product(b, x1, idx)
        live = live_of(b)
        v = cheb[0, b]
        am = f * (acc[SIG:SIG + 1] * live) - 1.0
        amul[b] = jnp.broadcast_to(am, (8, TILE))
        cur = am * v - (f * live) * acc[:SIG]
        cheb[1, b] = cur
        place(b, cur, x2)
    wait_recv(*s_args[0])
    wait_recv(*t_args)
    advance_ring(rows, rs1, x2, 1)

    def step(b, k, xb):
        acc = product(b, xb, idx)
        am = amul[b]
        am = 2.0 * jnp.concatenate([am, am], axis=0)
        return am * cheb[k, b] - (2.0 * f * live_of(b)) * acc - cheb[k - 1, b]

    packs = {}
    for b in range(NB):
        cur = step(b, 1, x2)
        cheb[2, b] = cur
        place(b, cur, x3, packs)
    flush(packs, op3, True)
    send(*v_args[1])
    packs = {}
    for b in range(NB):
        local_part(b, x3, 2.0 * f, cheb[1, b, :, :32], 0, packs)
    flush(packs, sp3, False)
    send(*s_args[1])
    add_totals(1)
    add_totals(2)

    wait_recv(*v_args[1])
    rows = rows_of(op3, rv3)
    unpack(rows, x3)
    for b in range(NB):
        cur = step(b, 2, x3)
        cheb[3, b] = cur
        place(b, cur, x4)
    wait_recv(*s_args[1])
    advance_ring(rows, rs3, x4, 0)
    sq = [None] * SCALES
    for b in range(NB):
        cur = step(b, 3, x4)
        for s in range(SCALES):
            t = tot[s, b] + cof_s[s, 3] * cheb[3, b] + cof_s[s, 4] * cur
            tot[s, b] = t
            sq[s] = t * t if sq[s] is None else sq[s] + t * t

    m = jnp.concatenate(sq, axis=0)
    hi = m.astype(jnp.bfloat16)
    r1 = m - hi.astype(jnp.float32)
    mid = r1.astype(jnp.bfloat16)
    lo = (r1 - mid.astype(jnp.float32)).astype(jnp.bfloat16)
    ones = jnp.ones((16, TILE), jnp.bfloat16)
    row = None
    for part in (lo, mid, hi):
        p = lax.dot_general(ones, part, (((1,), (1,)), ((), ())), preferred_element_type=jnp.float32)
        row = p if row is None else row + p
    row = jnp.concatenate([row[0:1], jnp.zeros((1, TILE - SCALES * SIG), jnp.float32)], axis=1)

    def phase(buf, mine, n, peers, s_sem, r_sem, value):
        buf[mine] = value
        for o, p in enumerate(peers):
            pltpu.make_async_remote_copy(
                src_ref=buf.at[mine], dst_ref=buf.at[mine], send_sem=s_sem.at[o],
                recv_sem=r_sem.at[mine], device_id=p, device_id_type=MESH).start()
        for o, p in enumerate(peers):
            src = (mine + o + 1) % n
            pltpu.make_async_remote_copy(
                src_ref=buf.at[mine], dst_ref=buf.at[src], send_sem=s_sem.at[o],
                recv_sem=r_sem.at[src], device_id=p, device_id_type=MESH).wait_recv()
        total = buf[0]
        for q in range(1, n):
            total = total + buf[q]
        return total

    part = phase(ga, zc, 8, a_peer, sa, ra, row)
    full = phase(gb, xy, 16, b_peer, sb, rb, part) * (1.0 / NODES)
    res = jnp.zeros((8, TILE), jnp.float32)
    sub = lax.broadcasted_iota(jnp.int32, (8, TILE), 0)
    full8 = jnp.broadcast_to(full, (8, TILE))
    for s in range(SCALES):
        v = pltpu.roll(full8, TILE - 16 * s, 1) if s else full8
        res = jnp.where(sub == s, v, res)
    en_ref[...] = res[:SCALES, :SIG]

    for src, dst, part, s_sem, r_sem in started:
        for d in range(8):
            @pl.when(have[d])
            def _(src=src, dst=dst, part=part, s_sem=s_sem, r_sem=r_sem, d=d):
                descriptor(src, dst, part, s_sem, r_sem, d, OPP[d], part(*DIRS[d])).wait_send()
    for o, p in enumerate(a_peer):
        pltpu.make_async_remote_copy(
            src_ref=ga.at[zc], dst_ref=ga.at[zc], send_sem=sa.at[o], recv_sem=ra.at[zc],
            device_id=p, device_id_type=MESH).wait_send()
    for o, p in enumerate(b_peer):
        pltpu.make_async_remote_copy(
            src_ref=gb.at[xy], dst_ref=gb.at[xy], send_sem=sb.at[o], recv_sem=rb.at[xy],
            device_id=p, device_id_type=MESH).wait_send()


def finish(tot, en, out_h, en_h, sem):
    a = pltpu.make_async_copy(tot, out_h, sem.at[0])
    b = pltpu.make_async_copy(en, en_h, sem.at[1])
    a.start()
    b.start()
    a.wait()
    b.wait()


def shards(signals, tiles, tile_dir, tile_mask, live_rows, bound_rows, scale_coeffs, spectral_bound):
    bf, f32, i32 = jnp.bfloat16, jnp.float32, jnp.int32
    vm, sm = pltpu.VMEM, pltpu.SMEM
    in_vmem = pl.BlockSpec(memory_space=pltpu.VMEM)
    hbm = pl.BlockSpec(memory_space=pl.ANY)
    dma = pltpu.SemaphoreType.DMA
    tot, energy = pl.pallas_call(
        kernel,
        out_shape=(pltpu.VMEM((SCALES, NB, SIG, TILE), f32), pltpu.VMEM((SCALES, SIG), f32)),
        in_specs=[hbm] * 7 + [pl.BlockSpec(memory_space=pltpu.HBM)],
        out_specs=(in_vmem, in_vmem),
        scratch_shapes=[
            sm((BX, SLOTS, BY), i32), sm((BX, SLOTS, BY), i32), sm((BX, BY), i32), sm((BX, BY), i32),
            sm((SCALES, DEG + 1), f32), sm((1,), f32),
            vm((BX, BY, SIG, TILE), f32), vm((NB, SLOTS, TILE, TILE), bf),
            sm((NB * SLOTS,), i32), sm((NB * SLOTS,), i32),
            vm((NX, 32, TILE), bf), vm((NX, SIG, TILE), bf), vm((NX, SIG, TILE), bf), vm((NX, SIG, TILE), bf),
            vm((DEG, NB, SIG, TILE), f32), vm((NB, 8, TILE), f32),
            vm((3, 2, 32, TILE), bf), vm((3, 2, SIG, TILE), bf),
            vm((2, 3, SIG, TILE), f32), vm((2, 3, SIG, TILE), f32), vm((2, 10, 32, TILE), bf),
            vm((8, 3, 2, 32, TILE), bf), vm((8, 3, 2, SIG, TILE), bf),
            vm((8, 2, 3, SIG, TILE), f32), vm((8, 2, 3, SIG, TILE), f32), vm((8, 2, 10, 32, TILE), bf),
            vm((8, 1, TILE), f32), vm((16, 1, TILE), f32),
            dma((11,)), dma((2, 8)), dma((2, 8)), dma((2, 8)), dma((2, 8)), dma((8,)), dma((8,)),
            dma((7,)), dma((8,)), dma((15,)), dma((16,)),
        ],
        compiler_params=pltpu.CompilerParams(collective_id=0, has_side_effects=True),
        name="wavelet",
    )(signals, tiles, jnp.swapaxes(tile_dir, 1, 2), jnp.swapaxes(tile_mask, 1, 2), live_rows, bound_rows,
      scale_coeffs, spectral_bound)
    out, energy = pl.pallas_call(
        finish,
        out_shape=(jax.ShapeDtypeStruct((SCALES, NB, SIG, TILE), f32), jax.ShapeDtypeStruct((SCALES, SIG), f32)),
        in_specs=[in_vmem, in_vmem],
        out_specs=(hbm, hbm),
        scratch_shapes=[dma((2,))],
        name="finish",
    )(pltpu.with_memory_space_constraint(tot, pltpu.VMEM), pltpu.with_memory_space_constraint(energy, pltpu.VMEM))
    return out.reshape(SCALES, BX, BY, SIG, TILE), energy


def solution(mesh):
    torus = Mesh(mesh.devices.reshape(4, 4, 2, mesh.shape["gy"]), ("gx_0", "gx_1", "gx_2", "gy"))
    gxs = ("gx_0", "gx_1", "gx_2")
    placed = (
        P(gxs, "gy", None, None),
        P(gxs, "gy", None, None, None),
        P(gxs, "gy", None),
        P(gxs, "gy", None),
        P(gxs, "gy"),
        P(gxs, "gy"),
        P(),
        P(),
    )
    return jax.shard_map(
        shards,
        mesh=torus,
        in_specs=placed,
        out_specs=(P(None, gxs, "gy", None, None), P()),
        check_vma=False,
    )
```

```python
import jax
import jax.numpy as jnp
from jax import lax
from jax.experimental import pallas as pl
from jax.experimental.pallas import tpu as pltpu
from jax.sharding import PartitionSpec as P

MESH = pl.DeviceIdType.MESH
SIG, SCALES, DEG, SLOTS, TILE = 16, 6, 4, 4, 128
BX, BY = 2, 8
NB = BX * BY
GXN, GYN = 32, 4
ZERO = NB + (BX + 2) * (BY + 2)
NX = ZERO + 1
NODES = 64 * 32 * 128
DIRS = [(-1, 0), (1, 0), (0, -1), (0, 1), (-1, -1), (-1, 1), (1, -1), (1, 1)]
OPP = [DIRS.index((-dx, -dy)) for dx, dy in DIRS]


def hops(o):
    ring = (0, 1, 2, 1)
    return ring[o & 3] + ring[o >> 3 & 3] + ring[o >> 5 & 3] + 0.1 * (o >> 2 & 1)


DEVICES = 128
FAR_FIRST = sorted(range(1, DEVICES), key=lambda o: (-hops(o), o))


def kernel(sig_h, til_h, dir_h, msk_h, liv_h, bnd_h, cof_h, spb_h,
           tot, en_ref,
           dir_s, msk_s, liv_s, bnd_s, cof_s, spb_s, sig, til, idx, loc, x1, x2, x3, x4, cheb, amul, op1, op3, sp1, sp3, tp,
           rv1, rv3, rs1, rs3, tr, ga,
           ld_sem, vs, vr, ss, sr, ts, tr_sem, sa, ra, in_y, in_xy):
    gx, gy = lax.axis_index("gx"), lax.axis_index("gy")
    me = gx * GYN + gy
    early = []
    for n, (src, dst) in enumerate(((sig_h, sig), (liv_h, liv_s), (bnd_h, bnd_s), (dir_h, dir_s), (msk_h, msk_s),
                                    (cof_h, cof_s), (spb_h, spb_s))):
        cp = pltpu.make_async_copy(src, dst, ld_sem.at[n])
        cp.start()
        early.append(cp)

    def exists(d):
        dx, dy = DIRS[d]
        ok = None
        for step, pos, n in ((dx, gx, GXN), (dy, gy, GYN)):
            if step == 0:
                continue
            this = pos > 0 if step < 0 else pos < n - 1
            ok = this if ok is None else jnp.logical_and(ok, this)
        return ok

    have = [exists(d) for d in range(8)]
    peer = [(gx + dx, gy + dy) for dx, dy in DIRS]
    flip = lambda v: (v, v + 1 - 2 * (v % 2), (v + 2) % 4, 3 - v)
    xs, ys, zs = flip(gx // 8), flip(gx // 2 % 4), flip(gy)
    xyc = [8 * u + 2 * v + w for u in xs for v in ys for w in (gx % 2, 1 - gx % 2)]
    other = lambda o: (xyc[(o >> 5) * 8 + (o >> 3) % 4 * 2 + (o >> 2) % 2], zs[o % 4])
    rest = (1, 2, 3, 4, 5, 6, 7)
    ring_y, ring_x = (8, 16, 24), (32, 64, 96)
    bar = pltpu.get_barrier_semaphore()
    for d in (4, 5, 6, 7, 0, 1, 2, 3):
        @pl.when(have[d])
        def _(d=d):
            pl.semaphore_signal(bar, inc=1, device_id=peer[d], device_id_type=MESH)
    for o in ring_x + ring_y + rest:
        pl.semaphore_signal(bar, inc=1, device_id=other(o), device_id_type=MESH)
    count = jnp.int32(13)
    for d in range(8):
        count = count + have[d].astype(jnp.int32)
    til_cp = []
    for n in range(4):
        cp = pltpu.make_async_copy(til_h.at[n // 2, pl.ds(4 * (n % 2), 4)], til.at[pl.ds(4 * n, 4)], ld_sem.at[7 + n])
        cp.start()
        til_cp.append(cp)
    for cp in early:
        cp.wait()

    lane = lax.broadcasted_iota(jnp.int32, (1, TILE), 1)
    low = lane < 32
    f = 2.0 / spb_s[0]
    bf16 = lambda a: a.astype(jnp.bfloat16)
    f32 = lambda a: a.astype(jnp.float32)

    def live_of(b):
        return (lane < liv_s[b // BY, b % BY]).astype(jnp.float32)

    def edge_of(b):
        return (lane < bnd_s[b // BY, b % BY]).astype(jnp.float32)

    RING = [(r, q) for r in (1, 4) for q in range(1, 11)] + [(r, q) for r in (2, 3) for q in (1, 10)]
    slot_of = lambda er, ec: NB + (er - 1) * (BY + 2) + ec - 1
    def shift(v, q):
        q = q % 4
        return pltpu.roll(v, 32 * q, 1) if q else v

    def add_to(packs, i, j, v):
        key = (i, (j + 2) // 4)
        v = shift(v, j + 2)
        packs[key] = v if key not in packs else packs[key] + v

    def place(b, v, xb, packs=None):
        i, j = b // BY, b % BY
        xb[b] = bf16(v)
        e = v * edge_of(b)
        xb[slot_of(i + 2, j + 2)] = bf16(e)
        if packs is not None:
            add_to(packs, i, j, e)

    def flush(packs, buf, tile_first):
        for (i, t), v in packs.items():
            if tile_first:
                buf[t, i] = bf16(v)
            else:
                buf[i, t] = v

    def part_v(dx, dy):
        return ({-1: pl.ds(0, 1), 1: pl.ds(2, 1), 0: pl.ds(0, 3)}[dy],)

    def part_s(dx, dy):
        return ({-1: pl.ds(0, 1), 1: pl.ds(1, 1), 0: pl.ds(0, 2)}[dx],
                {-1: pl.ds(0, 1), 1: pl.ds(2, 1), 0: pl.ds(0, 3)}[dy])

    def part_t(dx, dy):
        return ({-1: pl.ds(0, 1), 1: pl.ds(1, 1), 0: pl.ds(0, 2)}[dx],
                {-1: pl.ds(0, 2), 1: pl.ds(8, 2), 0: pl.ds(0, 10)}[dy])

    def descriptor(src, dst, part, s_sem, r_sem, d, o, at):
        return pltpu.make_async_remote_copy(
            src_ref=src.at[at], dst_ref=dst.at[(o,) + at], send_sem=s_sem.at[d],
            recv_sem=r_sem.at[o], device_id=peer[d], device_id_type=MESH)

    started = []

    def send(src, dst, part, s_sem, r_sem):
        started.append((src, dst, part, s_sem, r_sem))
        for d in (4, 5, 6, 7, 0, 1, 2, 3):
            @pl.when(have[d])
            def _(d=d):
                descriptor(src, dst, part, s_sem, r_sem, d, OPP[d], part(*DIRS[d])).start()

    def wait_recv(src, dst, part, s_sem, r_sem):
        for d in range(8):
            @pl.when(have[d])
            def _(d=d):
                descriptor(src, dst, part, s_sem, r_sem, d, d, part(*DIRS[OPP[d]])).wait_recv()

    v_args = ((op1, rv1, part_v, vs.at[0], vr.at[0]), (op3, rv3, part_v, vs.at[1], vr.at[1]))
    s_args = ((sp1, rs1, part_s, ss.at[0], sr.at[0]), (sp3, rs3, part_s, ss.at[1], sr.at[1]))
    t_args = (tp, tr, part_t, ts, tr_sem)
    U, D, L, R, UL, UR, DL, DR = range(8)
    left = lane < 64

    def rows_of(op, rv):
        rows = []
        for r in range(6):
            i = r % 2
            if r in (2, 3):
                lo, hi, mine = rv[L, 2, i], rv[R, 0, i], [op[t, i] for t in range(3)]
            else:
                u, ul, ur = (U, UL, UR) if r < 2 else (D, DL, DR)
                lo, hi, mine = rv[ul, 2, i], rv[ur, 0, i], [rv[u, t, i] for t in range(3)]
            mine = [f32(v) for v in mine]
            rows.append([jnp.where(left, f32(lo), mine[0]), mine[1], jnp.where(left, mine[2], f32(hi))])
        return rows

    def unpack(rows, xb):
        for er, ec in RING:
            v = jnp.where(low, shift(rows[er][ec // 4], -ec), 0.0)
            xb[slot_of(er, ec)] = bf16(v)

    def contract(lhs, rhs):
        return lax.dot_general(lhs, rhs, (((1,), (1,)), ((), ())), preferred_element_type=jnp.float32)

    def product(b, xb, table, rows=TILE):
        acc = None
        for h in range(2):
            pick = [xb[table[b * SLOTS + 2 * h + n]] for n in range(2)]
            rhs = [til[b, 2 * h + n, :rows] for n in range(2)]
            p = contract(jnp.concatenate(pick, axis=1), jnp.concatenate(rhs, axis=1))
            acc = p if acc is None else acc + p
        return acc

    packs = {}
    pad = lax.broadcasted_iota(jnp.int32, (16, TILE), 0) == 0
    for b in range(NB):
        live = live_of(b)
        v = sig[b // BY, b % BY] * live
        cheb[0, b] = v
        place(b, jnp.concatenate([v, jnp.where(pad, live, 0.0)], axis=0), x1, packs)
    flush(packs, op1, True)
    pl.semaphore_wait(bar, count)
    send(*v_args[0])
    for o in ring_x:
        pl.semaphore_signal(in_y, inc=1, device_id=other(o), device_id_type=MESH)

    for d in range(8):
        @pl.when(jnp.logical_not(have[d]))
        def _(d=d):
            for buf in (rv1, rv3, rs1, rs3, tr):
                buf[d] = jnp.zeros(buf.shape[1:], buf.dtype)

    for b in range(NB):
        i, j = b // BY, b % BY
        for s in range(SLOTS):
            d = dir_s[i, s, j]
            r = (d * 11) >> 5
            q = d - 3 * r
            off = NB + (i + r) * (BY + 2) + (j + q)
            off = jnp.where(d == 4, b, off)
            off = jnp.where(msk_s[i, s, j] == 1, off, ZERO)
            idx[b * SLOTS + s] = off
            away = r == 2 * i
            if j in (0, BY - 1):
                away = jnp.logical_or(away, q == (0 if j == 0 else 2))
            loc[b * SLOTS + s] = jnp.where(away, ZERO, off)

    for xb in (x1, x2, x3, x4):
        xb[ZERO] = jnp.zeros(xb.shape[1:], xb.dtype)
    for xb in (x2, x4):
        for er, ec in RING:
            xb[slot_of(er, ec)] = jnp.zeros(xb.shape[1:], xb.dtype)


    def corner(b, wanted):
        i, j = b // BY, b % BY
        total = None
        for d, group in wanted:
            acc = None
            for s in range(SLOTS):
                on = jnp.logical_and(dir_s[i, s, j] == d, msk_s[i, s, j] == 1).astype(jnp.float32)
                t = f32(til[b, s, :32]) * on
                acc = t if acc is None else acc + t
            acc = shift(jnp.where(low, acc, 0.0), group)
            total = acc if total is None else total + acc
        inside = lax.broadcasted_iota(jnp.int32, (32, TILE), 0) < bnd_s[i, j]
        return bf16(jnp.where(inside, total, 0.0))

    def local_part(b, xb, scale, prev, first, packs):
        acc = product(b, xb, loc, 32)
        v = cheb[2 * (1 - first), b, :, :32]
        fl = scale * live_of(b)[:, :32]
        if first:
            am = fl * acc[SIG:SIG + 1] - 1.0
            out = am * v - fl * acc[:SIG]
        else:
            am = amul[b, :1, :32]
            out = 2.0 * am * v - fl * acc - prev
        out = out * edge_of(b)[:, :32]
        add_to(packs, b // BY, b % BY, jnp.concatenate([out, jnp.zeros((SIG, TILE - 32), jnp.float32)], axis=1))

    packs = {}
    for cp in til_cp:
        cp.wait()
    for b in range(NB):
        i, j = b // BY, b % BY
        dx = 2 * i
        tp[i, 1 + j] = corner(b, [(3 * dx + q, j + 1 + q) for q in range(3)])
        if j == 0:
            tp[i, 0] = corner(b, [(3 - 3 * i, 1), (6 - 3 * i, 2)])
        if j == BY - 1:
            tp[i, 9] = corner(b, [(5 - 3 * i, 2), (8 - 3 * i, 3)])
        local_part(b, x1, f, None, 1, packs)
    flush(packs, sp1, False)

    send(*s_args[0])
    send(*t_args)

    def add_totals(k):
        for s in range(SCALES):
            a = cof_s[s, k] * 0.5 if k == 0 else cof_s[s, k]
            for b in range(NB):
                t = a * cheb[k, b]
                tot[s, b] = t if k == 0 else tot[s, b] + t

    def advance_ring(rows, rs, xn, first):
        wide = [[bf16(v) for v in r] for r in rows]

        def row_input(er, ec):
            t, q = ec // 4, ec % 4
            if q == 0:
                return bf16(jnp.where(lane >= 96, rows[er][t - 1], rows[er][t]))
            if q == 3:
                return bf16(jnp.where(low, rows[er][t + 1], rows[er][t]))
            return wide[er][t]

        def column_input(er, ec):
            g = (ec + 1) % 4
            at = jnp.logical_and(lane >= 32 * g, lane < 32 * g + 32)
            return bf16(jnp.where(at, shift(rows[er + 1][ec // 4], 1), rows[er][ec // 4]))

        inputs = {}
        for er, ec in RING:
            side = 0 if ec == 1 else 2 if ec == 10 else 1
            level = 0 if er == 1 else 2 if er == 4 else 1
            owner = {(0, 0): UL, (0, 1): U, (0, 2): UR, (1, 0): L, (1, 2): R,
                     (2, 0): DL, (2, 1): D, (2, 2): DR}[(level, side)]
            i = {1: 1, 2: 0, 3: 1, 4: 0}[er]
            j = (ec - 2) % BY
            base = er - i
            lhs, rhs = row_input(er + (1 if i else -1), ec), tr[owner, i, 1 + j]
            if j in (0, BY - 1):
                col = ec - 1 if j == 0 else ec + 1
                if (base, col) not in inputs:
                    inputs[(base, col)] = column_input(base, col)
                lhs = jnp.concatenate([lhs, inputs[(base, col)]], axis=1)
                rhs = jnp.concatenate([rhs, tr[owner, i, 0 if j == 0 else 9]], axis=1)
            acc = contract(lhs, rhs)
            own = shift(rs[owner, i, (j + 2) // 4], -ec)[:, :32]
            if first:
                v = shift(rows[er][ec // 4], -ec)[:SIG, :32]
                new = own + f * (acc[SIG:SIG + 1] * v - acc[:SIG])
            else:
                new = own - (2.0 * f) * acc
            xn[slot_of(er, ec), :, pl.ds(0, 32)] = bf16(new)

    add_totals(0)
    pl.semaphore_wait(in_y, 3)
    for o in rest:
        pl.semaphore_signal(in_xy, inc=1, device_id=other(o), device_id_type=MESH)
    wait_recv(*v_args[0])
    rows = rows_of(op1, rv1)
    unpack(rows, x1)
    for b in range(NB):
        acc = product(b, x1, idx)
        live = live_of(b)
        v = cheb[0, b]
        am = f * (acc[SIG:SIG + 1] * live) - 1.0
        amul[b] = jnp.broadcast_to(am, (8, TILE))
        cur = am * v - (f * live) * acc[:SIG]
        cheb[1, b] = cur
        place(b, cur, x2)
    wait_recv(*s_args[0])
    wait_recv(*t_args)
    advance_ring(rows, rs1, x2, 1)

    def step(b, k, xb):
        acc = product(b, xb, idx)
        am = amul[b]
        am = 2.0 * jnp.concatenate([am, am], axis=0)
        return am * cheb[k, b] - (2.0 * f * live_of(b)) * acc - cheb[k - 1, b]

    packs = {}
    for b in range(NB):
        cur = step(b, 1, x2)
        cheb[2, b] = cur
        place(b, cur, x3, packs)
    flush(packs, op3, True)
    send(*v_args[1])
    packs = {}
    for b in range(NB):
        local_part(b, x3, 2.0 * f, cheb[1, b, :, :32], 0, packs)
    flush(packs, sp3, False)
    send(*s_args[1])
    add_totals(1)
    add_totals(2)

    wait_recv(*v_args[1])
    rows = rows_of(op3, rv3)
    unpack(rows, x3)
    for b in range(NB):
        cur = step(b, 2, x3)
        cheb[3, b] = cur
        place(b, cur, x4)
    wait_recv(*s_args[1])
    advance_ring(rows, rs3, x4, 0)
    sq = [None] * SCALES
    for b in range(NB):
        cur = step(b, 3, x4)
        for s in range(SCALES):
            t = tot[s, b] + cof_s[s, 3] * cheb[3, b] + cof_s[s, 4] * cur
            tot[s, b] = t
            sq[s] = t * t if sq[s] is None else sq[s] + t * t

    m = jnp.concatenate(sq, axis=0)
    hi = m.astype(jnp.bfloat16)
    r1 = m - hi.astype(jnp.float32)
    mid = r1.astype(jnp.bfloat16)
    lo = (r1 - mid.astype(jnp.float32)).astype(jnp.bfloat16)
    ones = jnp.ones((16, TILE), jnp.bfloat16)
    row = None
    for part in (lo, mid, hi):
        p = lax.dot_general(ones, part, (((1,), (1,)), ((), ())), preferred_element_type=jnp.float32)
        row = p if row is None else row + p
    row = jnp.concatenate([row[0:1], jnp.zeros((1, TILE - SCALES * SIG), jnp.float32)], axis=1)

    ga[me] = row
    pl.semaphore_wait(in_xy, 7)
    for o in FAR_FIRST:
        pltpu.make_async_remote_copy(
            src_ref=ga.at[me], dst_ref=ga.at[me], send_sem=sa, recv_sem=ra,
            device_id=other(o), device_id_type=MESH).start()
    many = ga.at[pl.ds(0, DEVICES - 1)]
    pltpu.make_async_remote_copy(
        src_ref=many, dst_ref=many, send_sem=sa, recv_sem=ra, device_id=other(1), device_id_type=MESH).wait_recv()
    sums = [ga[q] for q in range(DEVICES)]
    while len(sums) > 1:
        sums = [u + v for u, v in zip(sums[::2], sums[1::2])]
    full = sums[0] * (1.0 / NODES)
    res = jnp.zeros((8, TILE), jnp.float32)
    sub = lax.broadcasted_iota(jnp.int32, (8, TILE), 0)
    full8 = jnp.broadcast_to(full, (8, TILE))
    for s in range(SCALES):
        v = pltpu.roll(full8, TILE - 16 * s, 1) if s else full8
        res = jnp.where(sub == s, v, res)
    en_ref[...] = res[:SCALES, :SIG]

    for src, dst, part, s_sem, r_sem in started:
        for d in range(8):
            @pl.when(have[d])
            def _(src=src, dst=dst, part=part, s_sem=s_sem, r_sem=r_sem, d=d):
                descriptor(src, dst, part, s_sem, r_sem, d, OPP[d], part(*DIRS[d])).wait_send()
    pltpu.make_async_remote_copy(
        src_ref=many, dst_ref=many, send_sem=sa, recv_sem=ra, device_id=other(1), device_id_type=MESH).wait_send()


def finish(tot, en, out_h, en_h, sem):
    a = pltpu.make_async_copy(tot, out_h, sem.at[0])
    b = pltpu.make_async_copy(en, en_h, sem.at[1])
    a.start()
    b.start()
    a.wait()
    b.wait()


def shards(signals, tiles, tile_dir, tile_mask, live_rows, bound_rows, scale_coeffs, spectral_bound):
    bf, f32, i32 = jnp.bfloat16, jnp.float32, jnp.int32
    vm, sm = pltpu.VMEM, pltpu.SMEM
    in_vmem = pl.BlockSpec(memory_space=pltpu.VMEM)
    hbm = pl.BlockSpec(memory_space=pl.ANY)
    dma = pltpu.SemaphoreType.DMA
    tot, energy = pl.pallas_call(
        kernel,
        out_shape=(pltpu.VMEM((SCALES, NB, SIG, TILE), f32), pltpu.VMEM((SCALES, SIG), f32)),
        in_specs=[hbm] * 7 + [pl.BlockSpec(memory_space=pltpu.HBM)],
        out_specs=(in_vmem, in_vmem),
        scratch_shapes=[
            sm((BX, SLOTS, BY), i32), sm((BX, SLOTS, BY), i32), sm((BX, BY), i32), sm((BX, BY), i32),
            sm((SCALES, DEG + 1), f32), sm((1,), f32),
            vm((BX, BY, SIG, TILE), f32), vm((NB, SLOTS, TILE, TILE), bf),
            sm((NB * SLOTS,), i32), sm((NB * SLOTS,), i32),
            vm((NX, 32, TILE), bf), vm((NX, SIG, TILE), bf), vm((NX, SIG, TILE), bf), vm((NX, SIG, TILE), bf),
            vm((DEG, NB, SIG, TILE), f32), vm((NB, 8, TILE), f32),
            vm((3, 2, 32, TILE), bf), vm((3, 2, SIG, TILE), bf),
            vm((2, 3, SIG, TILE), f32), vm((2, 3, SIG, TILE), f32), vm((2, 10, 32, TILE), bf),
            vm((8, 3, 2, 32, TILE), bf), vm((8, 3, 2, SIG, TILE), bf),
            vm((8, 2, 3, SIG, TILE), f32), vm((8, 2, 3, SIG, TILE), f32), vm((8, 2, 10, 32, TILE), bf),
            vm((DEVICES, 1, TILE), f32),
            dma((11,)), dma((2, 8)), dma((2, 8)), dma((2, 8)), dma((2, 8)), dma((8,)), dma((8,)),
            dma, dma, pltpu.SemaphoreType.REGULAR, pltpu.SemaphoreType.REGULAR,
        ],
        compiler_params=pltpu.CompilerParams(collective_id=0, has_side_effects=True),
        name="wavelet",
    )(signals, tiles, jnp.swapaxes(tile_dir, 1, 2), jnp.swapaxes(tile_mask, 1, 2), live_rows, bound_rows,
      scale_coeffs, spectral_bound)
    out, energy = pl.pallas_call(
        finish,
        out_shape=(jax.ShapeDtypeStruct((SCALES, NB, SIG, TILE), f32), jax.ShapeDtypeStruct((SCALES, SIG), f32)),
        in_specs=[in_vmem, in_vmem],
        out_specs=(hbm, hbm),
        scratch_shapes=[dma((2,))],
        name="finish",
    )(pltpu.with_memory_space_constraint(tot, pltpu.VMEM), pltpu.with_memory_space_constraint(energy, pltpu.VMEM))
    return out.reshape(SCALES, BX, BY, SIG, TILE), energy


def solution(mesh):
    placed = (
        P("gx", "gy", None, None),
        P("gx", "gy", None, None, None),
        P("gx", "gy", None),
        P("gx", "gy", None),
        P("gx", "gy"),
        P("gx", "gy"),
        P(),
        P(),
    )
    return jax.shard_map(
        shards,
        mesh=mesh,
        in_specs=placed,
        out_specs=(P(None, "gx", "gy", None, None), P()),
        check_vma=False,
    )
```

```python
import jax
import jax.numpy as jnp
from jax import lax
from jax.experimental import pallas as pl
from jax.experimental.pallas import tpu as pltpu
from jax.sharding import PartitionSpec as P

MESH = pl.DeviceIdType.MESH
SIG, SCALES, DEG, SLOTS, TILE = 16, 6, 4, 4, 128
BX, BY = 2, 8
NB = BX * BY
GXN, GYN = 32, 4
ZERO = 2 * NB
NX = ZERO + 1
NODES = 64 * 32 * 128
DIRS = [(-1, 0), (1, 0), (0, -1), (0, 1), (-1, -1), (-1, 1), (1, -1), (1, 1)]
OPP = [DIRS.index((-dx, -dy)) for dx, dy in DIRS]


def hops(o):
    ring = (0, 1, 2, 1)
    return ring[o & 3] + ring[o >> 3 & 3] + ring[o >> 5 & 3] + 0.1 * (o >> 2 & 1)


DEVICES = 128
FAR_FIRST = sorted(range(1, DEVICES), key=lambda o: (-hops(o), o))


def kernel(sig_h, til_h, dir_h, msk_h, liv_h, bnd_h, cof_h, spb_h,
           tot, en_ref,
           dir_s, msk_s, liv_s, bnd_s, cof_s, spb_s, sig, til, loc, x1, x2, x3, x4, cheb, base, amul, dloc,
           pw, qw, op1, op3, eg, sp1, sp3, tp, rv1, rv3, re, rs1, rs3, tr, ga,
           ld_sem, vs, vr, es, er_sem, ss, sr, ts, tr_sem, sa, ra, in_y, in_xy):
    gx, gy = lax.axis_index("gx"), lax.axis_index("gy")
    me = gx * GYN + gy
    early = []
    for n, (src, dst) in enumerate(((sig_h, sig), (liv_h, liv_s), (bnd_h, bnd_s), (dir_h, dir_s), (msk_h, msk_s),
                                    (cof_h, cof_s), (spb_h, spb_s))):
        cp = pltpu.make_async_copy(src, dst, ld_sem.at[n])
        cp.start()
        early.append(cp)

    def exists(d):
        dx, dy = DIRS[d]
        ok = None
        for step, pos, n in ((dx, gx, GXN), (dy, gy, GYN)):
            if step == 0:
                continue
            this = pos > 0 if step < 0 else pos < n - 1
            ok = this if ok is None else jnp.logical_and(ok, this)
        return ok

    have = [exists(d) for d in range(8)]
    peer = [(gx + dx, gy + dy) for dx, dy in DIRS]
    flip = lambda v: (v, v + 1 - 2 * (v % 2), (v + 2) % 4, 3 - v)
    xs, ys, zs = flip(gx // 8), flip(gx // 2 % 4), flip(gy)
    xyc = [8 * u + 2 * v + w for u in xs for v in ys for w in (gx % 2, 1 - gx % 2)]
    other = lambda o: (xyc[(o >> 5) * 8 + (o >> 3) % 4 * 2 + (o >> 2) % 2], zs[o % 4])
    rest = (1, 2, 3, 4, 5, 6, 7)
    ring_y, ring_x = (8, 16, 24), (32, 64, 96)
    bar = pltpu.get_barrier_semaphore()
    for d in (4, 5, 6, 7, 0, 1, 2, 3):
        @pl.when(have[d])
        def _(d=d):
            pl.semaphore_signal(bar, inc=1, device_id=peer[d], device_id_type=MESH)
    for o in ring_x + ring_y + rest:
        pl.semaphore_signal(bar, inc=1, device_id=other(o), device_id_type=MESH)
    count = jnp.int32(13)
    for d in range(8):
        count = count + have[d].astype(jnp.int32)
    til_cp = []
    for n in range(4):
        cp = pltpu.make_async_copy(til_h.at[n // 2, pl.ds(4 * (n % 2), 4)], til.at[pl.ds(4 * n, 4)], ld_sem.at[7 + n])
        cp.start()
        til_cp.append(cp)
    for cp in early:
        cp.wait()

    lane = lax.broadcasted_iota(jnp.int32, (1, TILE), 1)
    low, high, left = lane < 32, lane >= 96, lane < 64
    middle = jnp.logical_and(lane >= 32, lane < 96)
    f = 2.0 / spb_s[0]
    bf16 = lambda a: a.astype(jnp.bfloat16)
    f32 = lambda a: a.astype(jnp.float32)
    for xb in (x1, x2, x3, x4):
        xb[ZERO] = jnp.zeros(xb.shape[1:], xb.dtype)

    def live_of(b):
        return (lane < liv_s[b // BY, b % BY]).astype(jnp.float32)

    def edge_of(b):
        return (lane < bnd_s[b // BY, b % BY]).astype(jnp.float32)

    def shift(v, q):
        q = q % 4
        return pltpu.roll(v, 32 * q, 1) if q else v

    def add_to(packs, i, j, v):
        key = (i, (j + 2) // 4)
        v = shift(v, j + 2)
        packs[key] = v if key not in packs else packs[key] + v

    def place(b, v, xb, packs=None):
        xb[b] = bf16(v)
        e = v * edge_of(b)
        xb[NB + b] = bf16(e)
        if packs is not None:
            add_to(packs, b // BY, b % BY, e[:SIG])

    def part_v(dx, dy):
        return ({-1: pl.ds(0, 1), 1: pl.ds(2, 1), 0: pl.ds(0, 3)}[dy],)

    def part_s(dx, dy):
        return ({-1: pl.ds(0, 1), 1: pl.ds(1, 1), 0: pl.ds(0, 2)}[dx],
                {-1: pl.ds(0, 1), 1: pl.ds(2, 1), 0: pl.ds(0, 3)}[dy])

    def part_t(dx, dy):
        return ({-1: pl.ds(0, 1), 1: pl.ds(1, 1), 0: pl.ds(0, 2)}[dx],
                {-1: pl.ds(0, 2), 1: pl.ds(8, 2), 0: pl.ds(0, 10)}[dy])

    def descriptor(src, dst, part, s_sem, r_sem, d, o, at):
        return pltpu.make_async_remote_copy(
            src_ref=src.at[at], dst_ref=dst.at[(o,) + at], send_sem=s_sem.at[d],
            recv_sem=r_sem.at[o], device_id=peer[d], device_id_type=MESH)

    started = []

    def send(*messages):
        started.extend(messages)
        for d in (4, 5, 6, 7, 0, 1, 2, 3):
            @pl.when(have[d])
            def _(d=d):
                for src, dst, part, s_sem, r_sem in messages:
                    descriptor(src, dst, part, s_sem, r_sem, d, OPP[d], part(*DIRS[d])).start()

    def wait_recv(*messages):
        for d in range(8):
            @pl.when(have[d])
            def _(d=d):
                for src, dst, part, s_sem, r_sem in messages:
                    descriptor(src, dst, part, s_sem, r_sem, d, d, part(*DIRS[OPP[d]])).wait_recv()

    v_args = ((op1, rv1, part_v, vs.at[0], vr.at[0]), (op3, rv3, part_v, vs.at[1], vr.at[1]))
    e_args = (eg, re, part_v, es, er_sem)
    s_args = ((sp1, rs1, part_s, ss.at[0], sr.at[0]), (sp3, rs3, part_s, ss.at[1], sr.at[1]))
    t_args = (tp, tr, part_t, ts, tr_sem)
    U, D, L, R, UL, UR, DL, DR = range(8)

    def contract(lhs, rhs):
        return lax.dot_general(lhs, rhs, (((1,), (1,)), ((), ())), preferred_element_type=jnp.float32)

    packs, epacks = {}, {}
    top = lax.broadcasted_iota(jnp.int32, (16, TILE), 0) == 0
    for b in range(NB):
        live = live_of(b)
        v = sig[b // BY, b % BY] * live
        cheb[0, b] = v
        place(b, jnp.concatenate([v, jnp.where(top, live, 0.0)], axis=0), x1, packs)
        add_to(epacks, b // BY, b % BY, edge_of(b))
    for (i, t), v in packs.items():
        op1[t, i] = bf16(v)
    for (i, t), v in epacks.items():
        eg[t, i] = v

    for b in range(NB):
        i, j = b // BY, b % BY
        for s in range(SLOTS):
            d = dir_s[i, s, j]
            r = (d * 11) >> 5
            q = d - 3 * r
            off = jnp.where(d == 4, b, NB + (i + r - 1) * BY + j + q - 1)
            off = jnp.where(msk_s[i, s, j] == 1, off, ZERO)
            away = r == 2 * i
            if j in (0, BY - 1):
                away = jnp.logical_or(away, q == (0 if j == 0 else 2))
            loc[b * SLOTS + s] = jnp.where(away, ZERO, off)

    def sorted_rows(b, wanted, first):
        i, j = b // BY, b % BY
        total = None
        tiles = [f32(til[b, s, pl.ds(first, 32)]) for s in range(SLOTS)]
        for d, group in wanted:
            acc = None
            for s in range(SLOTS):
                on = jnp.logical_and(dir_s[i, s, j] == d, msk_s[i, s, j] == 1).astype(jnp.float32)
                t = tiles[s] * on
                acc = t if acc is None else acc + t
            acc = shift(jnp.where(low, acc, 0.0), group)
            total = acc if total is None else total + acc
        return total

    def directions(b):
        i, j = b // BY, b % BY
        yield None, [(6 * i + q, j + 1 + q) for q in range(3)]
        if j == 0:
            yield 0, [(3 - 3 * i, 1), (6 - 3 * i, 0)]
        if j == BY - 1:
            yield 1, [(5 - 3 * i, 2), (8 - 3 * i, 3)]

    def sort_tiles(first):
        for b in range(NB):
            i, j = b // BY, b % BY
            for side, wanted in directions(b):
                rows = sorted_rows(b, wanted, first)
                kept = bf16(rows)
                if side is None:
                    pw[b, pl.ds(first, 32)] = kept
                else:
                    qw[i, side, pl.ds(first, 32)] = kept
                if first == 0:
                    inside = lax.broadcasted_iota(jnp.int32, (32, TILE), 0) < bnd_s[i, j]
                    tp[i, 1 + j if side is None else 9 * side] = bf16(jnp.where(inside, rows, 0.0))

    def own_product(b, xb):
        acc = None
        for h in range(2):
            pick = [xb[loc[b * SLOTS + 2 * h + n]] for n in range(2)]
            rhs = [til[b, 2 * h + n] for n in range(2)]
            p = contract(jnp.concatenate(pick, axis=1), jnp.concatenate(rhs, axis=1))
            acc = p if acc is None else acc + p
        return acc

    def own_part(k, xb, sp=None):
        packs = {}
        for b in range(NB):
            acc = own_product(b, xb)
            fl = f * live_of(b)
            if k == 0:
                deg = fl * acc[SIG:SIG + 1]
                dloc[b] = jnp.broadcast_to(deg, (8, TILE))
                out = (deg - 1.0) * cheb[0, b] - fl * acc[:SIG]
            else:
                am = amul[b]
                out = jnp.concatenate([am, am], axis=0) * cheb[k, b] - (2.0 * fl) * acc - cheb[k - 1, b]
            base[b] = out
            if sp is not None:
                add_to(packs, b // BY, b % BY, out * edge_of(b))
        for (i, t), v in packs.items():
            sp[i, t] = v

    for cp in til_cp:
        cp.wait()
    sort_tiles(0)
    own_part(0, x1, sp1)
    pl.semaphore_wait(bar, count)
    send(v_args[0], e_args, s_args[0])
    send(t_args)
    for o in ring_x:
        pl.semaphore_signal(in_y, inc=1, device_id=other(o), device_id_type=MESH)

    for d in range(8):
        @pl.when(jnp.logical_not(have[d]))
        def _(d=d):
            for buf in (rv1, rv3, re, rs1, rs3, tr):
                buf[d] = jnp.zeros(buf.shape[1:], buf.dtype)

    for first in (32, 64, 96):
        sort_tiles(first)

    def add_totals(k):
        for s in range(SCALES):
            a = cof_s[s, k] * 0.5 if k == 0 else cof_s[s, k]
            for b in range(NB):
                t = a * cheb[k, b]
                tot[s, b] = t if k == 0 else tot[s, b] + t

    def rows_of(op, rv):
        rows = []
        for r in range(6):
            i = r % 2
            if r in (2, 3):
                lo, hi, mine = rv[L, 2, i], rv[R, 0, i], [op[t, i] for t in range(3)]
            else:
                u, ul, ur = (U, UL, UR) if r < 2 else (D, DL, DR)
                lo, hi, mine = rv[ul, 2, i], rv[ur, 0, i], [rv[u, t, i] for t in range(3)]
            mine = [f32(v) for v in mine]
            rows.append([jnp.where(left, f32(lo), mine[0]), mine[1], jnp.where(left, mine[2], f32(hi))])
        return rows

    def with_edges(rows, edges):
        return [[jnp.concatenate([v, jnp.where(top, e, 0.0)], axis=0) for v, e in zip(r, q)]
                for r, q in zip(rows, edges)]

    class Inputs:
        def __init__(self, rows):
            self.rows, self.made = rows, {}

        def get(self, key, make):
            if key not in self.made:
                self.made[key] = bf16(make())
            return self.made[key]

        def plain(self, r, t):
            return self.get(("p", r, t), lambda: self.rows[r][t])

        def row(self, r, c):
            t, q, rows = c // 4, c % 4, self.rows[r]
            if q == 0:
                return self.get(("a", r, t), lambda: jnp.where(high, rows[t - 1], rows[t]))
            if q == 3:
                return self.get(("b", r, t), lambda: jnp.where(low, rows[t + 1], rows[t]))
            return self.plain(r, t)

        def crossing(self, r, t):
            rows = self.rows[r]
            before = rows[t - 1] if t > 0 else jnp.zeros_like(rows[t])
            after = rows[t + 1] if t < 2 else jnp.zeros_like(rows[t])
            return self.get(("x", r, t), lambda: jnp.where(left, after, before))

        def column(self, r, t):
            one, two = self.rows[r][t], self.rows[r + 1][t]
            return self.get(("c", r, t), lambda: jnp.where(
                middle, one, jnp.where(left, shift(two, -1), shift(two, 1))))

    def away_product(b, ins):
        i, j = b // BY, b % BY
        lhs, rhs = ins.row(1 if i == 0 else 4, j + 2), pw[b]
        if j in (0, BY - 1):
            side = 0 if j == 0 else 1
            lhs = jnp.concatenate([lhs, ins.column(2, 2 * side)], axis=1)
            rhs = jnp.concatenate([rhs, qw[i, side]], axis=1)
        return contract(lhs, rhs)

    r_iota = lax.broadcasted_iota(jnp.int32, (TILE, TILE), 0)
    c_iota = lax.broadcasted_iota(jnp.int32, (TILE, TILE), 1)
    across = jnp.logical_or(jnp.logical_and(r_iota < 32, c_iota >= 96), jnp.logical_and(r_iota >= 96, c_iota < 32))

    def advance_ring(rows, ins, rs, first):
        none = jnp.zeros((32, TILE), jnp.bfloat16)
        zero = jnp.zeros((TILE, TILE), jnp.float32)

        def update(own, lhs, rhs, v):
            acc = contract(jnp.concatenate(lhs, axis=1), jnp.concatenate(rhs, axis=1))
            if first:
                return own + f * (acc[SIG:SIG + 1] * v[:SIG] - acc[:SIG])
            return own - (2.0 * f) * acc

        new = [[None] * 3 for _ in range(6)]
        for er, u, ul, ur in ((1, U, UL, UR), (4, D, DL, DR)):
            i = 1 if er == 1 else 0
            feed = er + 1 if i else er - 1
            edge = er - i
            for t in range(3):
                if t == 1:
                    w = [tr[u, i, 3 + n] for n in range(4)]
                    own, wq = rs[u, i, 1], None
                elif t == 0:
                    w = [none, tr[ul, i, 8], tr[u, i, 1], tr[u, i, 2]]
                    wq = [none, tr[ul, i, 9], tr[u, i, 0], none]
                    own = jnp.where(left, rs[ul, i, 2], rs[u, i, 0])
                else:
                    w = [tr[u, i, 7], tr[u, i, 8], tr[ur, i, 1], none]
                    wq = [none, tr[u, i, 9], tr[ur, i, 0], none]
                    own = jnp.where(left, rs[u, i, 2], rs[ur, i, 0])
                w = f32(jnp.concatenate(w, axis=0))
                lhs = [ins.plain(feed, t), ins.crossing(feed, t)]
                rhs = [bf16(jnp.where(across, zero, w)), bf16(jnp.where(across, w, zero))]
                if wq is not None:
                    lhs.append(ins.column(edge, t))
                    rhs.append(jnp.concatenate(wq, axis=0))
                new[er][t] = update(own, lhs, rhs, rows[er][t])
        for er, i in ((2, 0), (3, 1)):
            feed = er - 1 if i == 0 else er + 1
            for t, o, p, q in ((0, L, 8, 9), (2, R, 1, 0)):
                at = 1 if t == 0 else 2
                pad = lambda w: jnp.concatenate([none] * at + [w] + [none] * (3 - at), axis=0)
                new[er][t] = update(rs[o, i, 2 - t], [ins.plain(feed, t), ins.column(2, t)],
                                    [pad(tr[o, i, p]), pad(tr[o, i, q])], rows[er][t])
        return new

    add_totals(0)
    pl.semaphore_wait(in_y, 3)
    for o in rest:
        pl.semaphore_signal(in_xy, inc=1, device_id=other(o), device_id_type=MESH)

    wait_recv(v_args[0], e_args)
    rows = with_edges(rows_of(op1, rv1), rows_of(eg, re))
    ins = Inputs(rows)
    for b in range(NB):
        acc = away_product(b, ins)
        fl = f * live_of(b)
        deg = fl * acc[SIG:SIG + 1]
        amul[b] = 2.0 * (dloc[b] + jnp.broadcast_to(deg, (8, TILE)) - 1.0)
        cur = base[b] + deg * cheb[0, b] - fl * acc[:SIG]
        cheb[1, b] = cur
        place(b, cur, x2)
    own_part(1, x2)
    wait_recv(s_args[0], t_args)
    ring = Inputs(advance_ring(rows, ins, rs1, 1))

    packs = {}
    for b in range(NB):
        cur = base[b] - (2.0 * f * live_of(b)) * away_product(b, ring)
        cheb[2, b] = cur
        place(b, cur, x3, packs)
    for (i, t), v in packs.items():
        op3[t, i] = bf16(v)
    send(v_args[1])
    own_part(2, x3, sp3)
    send(s_args[1])
    add_totals(1)
    add_totals(2)

    wait_recv(v_args[1])
    rows = rows_of(op3, rv3)
    ins = Inputs(rows)
    for b in range(NB):
        cur = base[b] - (2.0 * f * live_of(b)) * away_product(b, ins)
        cheb[3, b] = cur
        place(b, cur, x4)
    own_part(3, x4)
    wait_recv(s_args[1])
    ring = Inputs(advance_ring(rows, ins, rs3, 0))
    sq = [None] * SCALES
    for b in range(NB):
        cur = base[b] - (2.0 * f * live_of(b)) * away_product(b, ring)
        for s in range(SCALES):
            t = tot[s, b] + cof_s[s, 3] * cheb[3, b] + cof_s[s, 4] * cur
            tot[s, b] = t
            sq[s] = t * t if sq[s] is None else sq[s] + t * t

    m = jnp.concatenate(sq, axis=0)
    hi = m.astype(jnp.bfloat16)
    r1 = m - hi.astype(jnp.float32)
    mid = r1.astype(jnp.bfloat16)
    lo = (r1 - mid.astype(jnp.float32)).astype(jnp.bfloat16)
    ones = jnp.ones((16, TILE), jnp.bfloat16)
    row = None
    for part in (lo, mid, hi):
        p = lax.dot_general(ones, part, (((1,), (1,)), ((), ())), preferred_element_type=jnp.float32)
        row = p if row is None else row + p
    row = jnp.concatenate([row[0:1], jnp.zeros((1, TILE - SCALES * SIG), jnp.float32)], axis=1)

    ga[me] = row
    pl.semaphore_wait(in_xy, 7)
    for o in FAR_FIRST:
        pltpu.make_async_remote_copy(
            src_ref=ga.at[me], dst_ref=ga.at[me], send_sem=sa, recv_sem=ra,
            device_id=other(o), device_id_type=MESH).start()
    many = ga.at[pl.ds(0, DEVICES - 1)]
    pltpu.make_async_remote_copy(
        src_ref=many, dst_ref=many, send_sem=sa, recv_sem=ra, device_id=other(1), device_id_type=MESH).wait_recv()
    sums = [ga[q] for q in range(DEVICES)]
    while len(sums) > 1:
        sums = [u + v for u, v in zip(sums[::2], sums[1::2])]
    full = sums[0] * (1.0 / NODES)
    res = jnp.zeros((8, TILE), jnp.float32)
    sub = lax.broadcasted_iota(jnp.int32, (8, TILE), 0)
    full8 = jnp.broadcast_to(full, (8, TILE))
    for s in range(SCALES):
        v = pltpu.roll(full8, TILE - 16 * s, 1) if s else full8
        res = jnp.where(sub == s, v, res)
    en_ref[...] = res[:SCALES, :SIG]

    for src, dst, part, s_sem, r_sem in started:
        for d in range(8):
            @pl.when(have[d])
            def _(src=src, dst=dst, part=part, s_sem=s_sem, r_sem=r_sem, d=d):
                descriptor(src, dst, part, s_sem, r_sem, d, OPP[d], part(*DIRS[d])).wait_send()
    pltpu.make_async_remote_copy(
        src_ref=many, dst_ref=many, send_sem=sa, recv_sem=ra, device_id=other(1), device_id_type=MESH).wait_send()


def finish(tot, en, out_h, en_h, sem):
    a = pltpu.make_async_copy(tot, out_h, sem.at[0])
    b = pltpu.make_async_copy(en, en_h, sem.at[1])
    a.start()
    b.start()
    a.wait()
    b.wait()


def shards(signals, tiles, tile_dir, tile_mask, live_rows, bound_rows, scale_coeffs, spectral_bound):
    bf, f32, i32 = jnp.bfloat16, jnp.float32, jnp.int32
    vm, sm = pltpu.VMEM, pltpu.SMEM
    in_vmem = pl.BlockSpec(memory_space=pltpu.VMEM)
    hbm = pl.BlockSpec(memory_space=pl.ANY)
    dma = pltpu.SemaphoreType.DMA
    tot, energy = pl.pallas_call(
        kernel,
        out_shape=(pltpu.VMEM((SCALES, NB, SIG, TILE), f32), pltpu.VMEM((SCALES, SIG), f32)),
        in_specs=[hbm] * 7 + [pl.BlockSpec(memory_space=pltpu.HBM)],
        out_specs=(in_vmem, in_vmem),
        scratch_shapes=[
            sm((BX, SLOTS, BY), i32), sm((BX, SLOTS, BY), i32), sm((BX, BY), i32), sm((BX, BY), i32),
            sm((SCALES, DEG + 1), f32), sm((1,), f32),
            vm((BX, BY, SIG, TILE), f32), vm((NB, SLOTS, TILE, TILE), bf),
            sm((NB * SLOTS,), i32),
            vm((NX, 32, TILE), bf), vm((NX, SIG, TILE), bf), vm((NX, SIG, TILE), bf), vm((NX, SIG, TILE), bf),
            vm((DEG, NB, SIG, TILE), f32), vm((NB, SIG, TILE), f32), vm((NB, 8, TILE), f32), vm((NB, 8, TILE), f32),
            vm((NB, TILE, TILE), bf), vm((BX, 2, TILE, TILE), bf),
            vm((3, 2, SIG, TILE), bf), vm((3, 2, SIG, TILE), bf), vm((3, 2, 1, TILE), f32),
            vm((2, 3, SIG, TILE), f32), vm((2, 3, SIG, TILE), f32), vm((2, 10, 32, TILE), bf),
            vm((8, 3, 2, SIG, TILE), bf), vm((8, 3, 2, SIG, TILE), bf), vm((8, 3, 2, 1, TILE), f32),
            vm((8, 2, 3, SIG, TILE), f32), vm((8, 2, 3, SIG, TILE), f32), vm((8, 2, 10, 32, TILE), bf),
            vm((DEVICES, 1, TILE), f32),
            dma((11,)), dma((2, 8)), dma((2, 8)), dma((8,)), dma((8,)), dma((2, 8)), dma((2, 8)), dma((8,)), dma((8,)),
            dma, dma, pltpu.SemaphoreType.REGULAR, pltpu.SemaphoreType.REGULAR,
        ],
        compiler_params=pltpu.CompilerParams(collective_id=0, has_side_effects=True),
        name="wavelet",
    )(signals, tiles, jnp.swapaxes(tile_dir, 1, 2), jnp.swapaxes(tile_mask, 1, 2), live_rows, bound_rows,
      scale_coeffs, spectral_bound)
    out, energy = pl.pallas_call(
        finish,
        out_shape=(jax.ShapeDtypeStruct((SCALES, NB, SIG, TILE), f32), jax.ShapeDtypeStruct((SCALES, SIG), f32)),
        in_specs=[in_vmem, in_vmem],
        out_specs=(hbm, hbm),
        scratch_shapes=[dma((2,))],
        name="finish",
    )(pltpu.with_memory_space_constraint(tot, pltpu.VMEM), pltpu.with_memory_space_constraint(energy, pltpu.VMEM))
    return out.reshape(SCALES, BX, BY, SIG, TILE), energy


def solution(mesh):
    placed = (
        P("gx", "gy", None, None),
        P("gx", "gy", None, None, None),
        P("gx", "gy", None),
        P("gx", "gy", None),
        P("gx", "gy"),
        P("gx", "gy"),
        P(),
        P(),
    )
    return jax.shard_map(
        shards,
        mesh=mesh,
        in_specs=placed,
        out_specs=(P(None, "gx", "gy", None, None), P()),
        check_vma=False,
    )
```

```python
import functools
import operator

import jax
import jax.numpy as jnp
from jax import lax
from jax.experimental import pallas as pl
from jax.experimental.pallas import tpu as pltpu
from jax.sharding import PartitionSpec as P

MESH = pl.DeviceIdType.MESH
SIG, SCALES, DEG, SLOTS, TILE = 16, 6, 4, 4, 128
BX, BY = 2, 8
NB = BX * BY
GXN, GYN = 32, 4
ZERO = NB + (BX + 2) * (BY + 2)
NX = ZERO + 1
NODES = 64 * 32 * 128
DIRS = [(-1, 0), (1, 0), (0, -1), (0, 1), (-1, -1), (-1, 1), (1, -1), (1, 1)]
OPP = [DIRS.index((-dx, -dy)) for dx, dy in DIRS]


def hops(o):
    ring = (0, 1, 2, 1)
    return ring[o & 3] + ring[o >> 3 & 3] + ring[o >> 5 & 3] + 0.1 * (o >> 2 & 1)


DEVICES = 128
FAR_FIRST = sorted(range(1, DEVICES), key=lambda o: (-hops(o), o))


def kernel(sig_h, til_h, dir_h, msk_h, liv_h, bnd_h, cof_h, spb_h,
           tot, en_ref,
           dir_s, msk_s, liv_s, bnd_s, cof_s, spb_s, sig, til, idx, loc, x1, x2, x3, x4, cheb, amul,
           op1, op3, eg, sp1, sp3, tp, rv1, rv3, re, rs1, rs3, tr, ga, units,
           ld, r1, w1, r3, r4, w3, sa, ra, in_y, in_xy):
    gx, gy = lax.axis_index("gx"), lax.axis_index("gy")
    me = gx * GYN + gy
    early = []
    for n, (src, dst) in enumerate(((sig_h, sig), (liv_h, liv_s), (bnd_h, bnd_s), (dir_h, dir_s), (msk_h, msk_s),
                                    (cof_h, cof_s), (spb_h, spb_s))):
        cp = pltpu.make_async_copy(src, dst, ld.at[n])
        cp.start()
        early.append(cp)

    def exists(d):
        dx, dy = DIRS[d]
        ok = None
        for step, pos, n in ((dx, gx, GXN), (dy, gy, GYN)):
            if step == 0:
                continue
            this = pos > 0 if step < 0 else pos < n - 1
            ok = this if ok is None else jnp.logical_and(ok, this)
        return ok

    have = [exists(d) for d in range(8)]
    peer = [(gx + dx, gy + dy) for dx, dy in DIRS]
    flip = lambda v: (v, v + 1 - 2 * (v % 2), (v + 2) % 4, 3 - v)
    xs, ys, zs = flip(gx // 8), flip(gx // 2 % 4), flip(gy)
    xyc = [8 * u + 2 * v + w for u in xs for v in ys for w in (gx % 2, 1 - gx % 2)]
    other = lambda o: (xyc[(o >> 5) * 8 + (o >> 3) % 4 * 2 + (o >> 2) % 2], zs[o % 4])
    rest = (1, 2, 3, 4, 5, 6, 7)
    ring_y, ring_x = (8, 16, 24), (32, 64, 96)
    bar = pltpu.get_barrier_semaphore()
    for d in (4, 5, 6, 7, 0, 1, 2, 3):
        @pl.when(have[d])
        def _(d=d):
            pl.semaphore_signal(bar, inc=1, device_id=peer[d], device_id_type=MESH)
    for o in ring_x + ring_y + rest:
        pl.semaphore_signal(bar, inc=1, device_id=other(o), device_id_type=MESH)
    count = jnp.int32(13)
    for d in range(8):
        count = count + have[d].astype(jnp.int32)
    til_cp = []
    for n in range(4):
        cp = pltpu.make_async_copy(til_h.at[n // 2, pl.ds(4 * (n % 2), 4)], til.at[pl.ds(4 * n, 4)], ld.at[7 + n])
        cp.start()
        til_cp.append(cp)
    for cp in early:
        cp.wait()

    lane = lax.broadcasted_iota(jnp.int32, (1, TILE), 1)
    low, high, left = lane < 32, lane >= 96, lane < 64
    middle = jnp.logical_and(lane >= 32, lane < 96)
    f = 2.0 / spb_s[0]
    bf16 = lambda a: a.astype(jnp.bfloat16)
    f32 = lambda a: a.astype(jnp.float32)
    for xb in (x1, x2, x3, x4):
        xb[ZERO] = jnp.zeros(xb.shape[1:], xb.dtype)

    def live_of(b):
        return (lane < liv_s[b // BY, b % BY]).astype(jnp.float32)

    def edge_of(b):
        return (lane < bnd_s[b // BY, b % BY]).astype(jnp.float32)

    def shift(v, q):
        q = q % 4
        return pltpu.roll(v, 32 * q, 1) if q else v

    def add_to(packs, i, j, v):
        key = (i, (j + 2) // 4)
        v = shift(v, j + 2)
        packs[key] = v if key not in packs else packs[key] + v

    RING = [(r, q) for r in (1, 4) for q in range(1, 11)] + [(r, q) for r in (2, 3) for q in (1, 10)]
    slot_of = lambda er, ec: NB + (er - 1) * (BY + 2) + ec - 1

    def place(b, v, xb, packs=None):
        xb[b] = bf16(v)
        e = v * edge_of(b)
        xb[slot_of(b // BY + 2, b % BY + 2)] = bf16(e)
        if packs is not None:
            add_to(packs, b // BY, b % BY, e[:SIG])

    def part_v(dx, dy):
        return ({-1: pl.ds(0, 1), 1: pl.ds(2, 1), 0: pl.ds(0, 3)}[dy],)

    def part_s(dx, dy):
        return ({-1: pl.ds(0, 1), 1: pl.ds(1, 1), 0: pl.ds(0, 2)}[dx],
                {-1: pl.ds(0, 1), 1: pl.ds(2, 1), 0: pl.ds(0, 3)}[dy])

    def part_t(dx, dy):
        return ({-1: pl.ds(0, 1), 1: pl.ds(1, 1), 0: pl.ds(0, 2)}[dx],
                {-1: pl.ds(0, 2), 1: pl.ds(8, 2), 0: pl.ds(0, 10)}[dy])

    def descriptor(src, dst, part, s_sem, r_sem, d, o, at):
        return pltpu.make_async_remote_copy(
            src_ref=src.at[at], dst_ref=dst.at[(o,) + at], send_sem=s_sem, recv_sem=r_sem,
            device_id=peer[d], device_id_type=MESH)

    def send(*messages):
        for d in (4, 5, 6, 7, 0, 1, 2, 3):
            @pl.when(have[d])
            def _(d=d):
                for src, dst, part, s_sem, r_sem in messages:
                    descriptor(src, dst, part, s_sem, r_sem, d, OPP[d], part(*DIRS[d])).start()

    inner_x = jnp.logical_and(gx > 0, gx < GXN - 1)
    inner_y = jnp.logical_and(gy > 0, gy < GYN - 1)

    def wait_all(sent, *messages):
        def size(d):
            n = 0
            for src, _, part, _, _ in messages:
                at = part(*DIRS[d])
                shape = [p.size for p in at] + list(src.shape[len(at):])
                n += src.dtype.itemsize * functools.reduce(operator.mul, shape) // 512
            return n

        _, _, _, s_sem, r_sem = messages[0]
        for nx in (1, 2):
            for ny in (1, 2):
                n = nx * size(0) + ny * size(2) + nx * ny * size(4)
                this = jnp.logical_and(inner_x == (nx == 2), inner_y == (ny == 2))

                @pl.when(this)
                def _(n=n):
                    ref = units.at[pl.ds(0, n)]
                    cp = pltpu.make_async_remote_copy(
                        src_ref=ref, dst_ref=ref, send_sem=s_sem, recv_sem=r_sem,
                        device_id=other(1), device_id_type=MESH)
                    cp.wait_send() if sent else cp.wait_recv()

    first = ((op1, rv1, part_v, w1, r1), (eg, re, part_v, w1, r1), (sp1, rs1, part_s, w1, r1), (tp, tr, part_t, w1, r1))
    v3, s3 = (op3, rv3, part_v, w3, r3), (sp3, rs3, part_s, w3, r4)
    U, D, L, R, UL, UR, DL, DR = range(8)

    def contract(lhs, rhs):
        return lax.dot_general(lhs, rhs, (((1,), (1,)), ((), ())), preferred_element_type=jnp.float32)

    packs, epacks = {}, {}
    top = lax.broadcasted_iota(jnp.int32, (16, TILE), 0) == 0
    for b in range(NB):
        live = live_of(b)
        v = sig[b // BY, b % BY] * live
        cheb[0, b] = v
        place(b, jnp.concatenate([v, jnp.where(top, live, 0.0)], axis=0), x1, packs)
        add_to(epacks, b // BY, b % BY, edge_of(b))
    for (i, t), v in packs.items():
        op1[t, i] = bf16(v)
    for (i, t), v in epacks.items():
        eg[t, i] = v

    for b in range(NB):
        i, j = b // BY, b % BY
        for s in range(SLOTS):
            d = dir_s[i, s, j]
            r = (d * 11) >> 5
            q = d - 3 * r
            off = jnp.where(d == 4, b, NB + (i + r) * (BY + 2) + (j + q))
            off = jnp.where(msk_s[i, s, j] == 1, off, ZERO)
            idx[b * SLOTS + s] = off
            away = r == 2 * i
            if j in (0, BY - 1):
                away = jnp.logical_or(away, q == (0 if j == 0 else 2))
            loc[b * SLOTS + s] = jnp.where(away, ZERO, off)

    def sorted_rows(b, wanted):
        i, j = b // BY, b % BY
        total = None
        tiles = [f32(til[b, s, pl.ds(0, 32)]) for s in range(SLOTS)]
        for d, group in wanted:
            acc = None
            for s in range(SLOTS):
                on = jnp.logical_and(dir_s[i, s, j] == d, msk_s[i, s, j] == 1).astype(jnp.float32)
                t = tiles[s] * on
                acc = t if acc is None else acc + t
            acc = shift(jnp.where(low, acc, 0.0), group)
            total = acc if total is None else total + acc
        inside = lax.broadcasted_iota(jnp.int32, (32, TILE), 0) < bnd_s[i, j]
        return bf16(jnp.where(inside, total, 0.0))

    def directions(b):
        i, j = b // BY, b % BY
        yield None, [(6 * i + q, j + 1 + q) for q in range(3)]
        if j == 0:
            yield 0, [(3 - 3 * i, 1), (6 - 3 * i, 0)]
        if j == BY - 1:
            yield 1, [(5 - 3 * i, 2), (8 - 3 * i, 3)]

    def product(b, xb, table, rows=TILE):
        acc = None
        for h in range(2):
            pick = [xb[table[b * SLOTS + 2 * h + n]] for n in range(2)]
            rhs = [til[b, 2 * h + n, :rows] for n in range(2)]
            p = contract(jnp.concatenate(pick, axis=1), jnp.concatenate(rhs, axis=1))
            acc = p if acc is None else acc + p
        return acc

    def local_part(k, xb, sp):
        packs = {}
        for b in range(NB):
            acc = product(b, xb, loc, 32)
            v = cheb[k, b, :, :32]
            if k == 0:
                out = (f * acc[SIG:SIG + 1] - 1.0) * v - f * acc[:SIG]
            else:
                out = amul[b, :1, :32] * v - (2.0 * f) * acc - cheb[k - 1, b, :, :32]
            out = out * edge_of(b)[:, :32]
            add_to(packs, b // BY, b % BY,
                   jnp.concatenate([out, jnp.zeros((SIG, TILE - 32), jnp.float32)], axis=1))
        for (i, t), v in packs.items():
            sp[i, t] = v

    for cp in til_cp:
        cp.wait()
    for b in range(NB):
        for side, wanted in directions(b):
            tp[b // BY, 1 + b % BY if side is None else 9 * side] = sorted_rows(b, wanted)
    local_part(0, x1, sp1)
    pl.semaphore_wait(bar, count)
    send(*first)
    for o in ring_x:
        pl.semaphore_signal(in_y, inc=1, device_id=other(o), device_id_type=MESH)

    for d in range(8):
        @pl.when(jnp.logical_not(have[d]))
        def _(d=d):
            for buf in (rv1, rv3, re, rs1, rs3, tr):
                buf[d] = jnp.zeros(buf.shape[1:], buf.dtype)

    def add_totals(k):
        for s in range(SCALES):
            a = cof_s[s, k] * 0.5 if k == 0 else cof_s[s, k]
            for b in range(NB):
                t = a * cheb[k, b]
                tot[s, b] = t if k == 0 else tot[s, b] + t

    def rows_of(op, rv):
        rows = []
        for r in range(6):
            i = r % 2
            if r in (2, 3):
                lo, hi, mine = rv[L, 2, i], rv[R, 0, i], [op[t, i] for t in range(3)]
            else:
                u, ul, ur = (U, UL, UR) if r < 2 else (D, DL, DR)
                lo, hi, mine = rv[ul, 2, i], rv[ur, 0, i], [rv[u, t, i] for t in range(3)]
            mine = [f32(v) for v in mine]
            rows.append([jnp.where(left, f32(lo), mine[0]), mine[1], jnp.where(left, mine[2], f32(hi))])
        return rows

    def with_edges(rows, edges):
        return [[jnp.concatenate([v, jnp.where(top, e, 0.0)], axis=0) for v, e in zip(r, q)]
                for r, q in zip(rows, edges)]

    class Inputs:
        def __init__(self, rows):
            self.rows, self.made = rows, {}

        def get(self, key, make):
            if key not in self.made:
                self.made[key] = bf16(make())
            return self.made[key]

        def plain(self, r, t):
            return self.get(("p", r, t), lambda: self.rows[r][t])

        def row(self, r, c):
            t, q, rows = c // 4, c % 4, self.rows[r]
            if q == 0:
                return self.get(("a", r, t), lambda: jnp.where(high, rows[t - 1], rows[t]))
            if q == 3:
                return self.get(("b", r, t), lambda: jnp.where(low, rows[t + 1], rows[t]))
            return self.plain(r, t)

        def crossing(self, r, t):
            rows = self.rows[r]
            before = rows[t - 1] if t > 0 else jnp.zeros_like(rows[t])
            after = rows[t + 1] if t < 2 else jnp.zeros_like(rows[t])
            return self.get(("x", r, t), lambda: jnp.where(left, after, before))

        def column(self, r, t):
            one, two = self.rows[r][t], self.rows[r + 1][t]
            return self.get(("c", r, t), lambda: jnp.where(
                middle, one, jnp.where(left, shift(two, -1), shift(two, 1))))

    def unpack(rows, xb):
        for er, ec in RING:
            v = jnp.where(low, shift(rows[er][ec // 4], -ec), 0.0)
            xb[slot_of(er, ec)] = bf16(v)

    r_iota = lax.broadcasted_iota(jnp.int32, (TILE, TILE), 0)
    c_iota = lax.broadcasted_iota(jnp.int32, (TILE, TILE), 1)
    across = jnp.logical_or(jnp.logical_and(r_iota < 32, c_iota >= 96), jnp.logical_and(r_iota >= 96, c_iota < 32))

    def advance_ring(rows, rs, first):
        ins = Inputs(rows)
        none = jnp.zeros((32, TILE), jnp.bfloat16)
        zero = jnp.zeros((TILE, TILE), jnp.float32)

        def update(own, lhs, rhs, v):
            acc = contract(jnp.concatenate(lhs, axis=1), jnp.concatenate(rhs, axis=1))
            if first:
                return own + f * (acc[SIG:SIG + 1] * v[:SIG] - acc[:SIG])
            return own - (2.0 * f) * acc

        new = [[None] * 3 for _ in range(6)]
        for er, u, ul, ur in ((1, U, UL, UR), (4, D, DL, DR)):
            i = 1 if er == 1 else 0
            feed = er + 1 if i else er - 1
            edge = er - i
            for t in range(3):
                if t == 1:
                    w = [tr[u, i, 3 + n] for n in range(4)]
                    own, wq = rs[u, i, 1], None
                elif t == 0:
                    w = [none, tr[ul, i, 8], tr[u, i, 1], tr[u, i, 2]]
                    wq = [none, tr[ul, i, 9], tr[u, i, 0], none]
                    own = jnp.where(left, rs[ul, i, 2], rs[u, i, 0])
                else:
                    w = [tr[u, i, 7], tr[u, i, 8], tr[ur, i, 1], none]
                    wq = [none, tr[u, i, 9], tr[ur, i, 0], none]
                    own = jnp.where(left, rs[u, i, 2], rs[ur, i, 0])
                w = f32(jnp.concatenate(w, axis=0))
                lhs = [ins.plain(feed, t), ins.crossing(feed, t)]
                rhs = [bf16(jnp.where(across, zero, w)), bf16(jnp.where(across, w, zero))]
                if wq is not None:
                    lhs.append(ins.column(edge, t))
                    rhs.append(jnp.concatenate(wq, axis=0))
                new[er][t] = update(own, lhs, rhs, rows[er][t])
        for er, i in ((2, 0), (3, 1)):
            feed = er - 1 if i == 0 else er + 1
            for t, o, p, q in ((0, L, 8, 9), (2, R, 1, 0)):
                at = 1 if t == 0 else 2
                pad = lambda w: jnp.concatenate([none] * at + [w] + [none] * (3 - at), axis=0)
                new[er][t] = update(rs[o, i, 2 - t], [ins.plain(feed, t), ins.column(2, t)],
                                    [pad(tr[o, i, p]), pad(tr[o, i, q])], rows[er][t])
        return new

    add_totals(0)
    pl.semaphore_wait(in_y, 3)
    for o in rest:
        pl.semaphore_signal(in_xy, inc=1, device_id=other(o), device_id_type=MESH)

    wait_all(False, *first)
    rows = with_edges(rows_of(op1, rv1), rows_of(eg, re))
    unpack(rows, x1)
    ring = advance_ring(rows, rs1, 1)
    for b in range(NB):
        acc = product(b, x1, idx)
        fl = f * live_of(b)
        am = fl * acc[SIG:SIG + 1] - 1.0
        amul[b] = jnp.broadcast_to(2.0 * am, (8, TILE))
        cur = am * cheb[0, b] - fl * acc[:SIG]
        cheb[1, b] = cur
        place(b, cur, x2)
    unpack(ring, x2)

    def step(b, k, xb):
        acc = product(b, xb, idx)
        am = amul[b]
        am = jnp.concatenate([am, am], axis=0)
        return am * cheb[k, b] - (2.0 * f * live_of(b)) * acc - cheb[k - 1, b]

    packs = {}
    for b in range(NB):
        cur = step(b, 1, x2)
        cheb[2, b] = cur
        place(b, cur, x3, packs)
    for (i, t), v in packs.items():
        op3[t, i] = bf16(v)
    send(v3)
    local_part(2, x3, sp3)
    send(s3)
    add_totals(1)
    add_totals(2)
    wait_all(True, *first)

    wait_all(False, v3)
    rows = rows_of(op3, rv3)
    unpack(rows, x3)
    for b in range(NB):
        cur = step(b, 2, x3)
        cheb[3, b] = cur
        place(b, cur, x4)
    add_totals(3)
    wait_all(False, s3)
    unpack(advance_ring(rows, rs3, 0), x4)
    sq = [None] * SCALES
    for b in range(NB):
        cur = step(b, 3, x4)
        for s in range(SCALES):
            t = tot[s, b] + cof_s[s, 4] * cur
            tot[s, b] = t
            sq[s] = t * t if sq[s] is None else sq[s] + t * t

    m = jnp.concatenate(sq, axis=0)
    hi = m.astype(jnp.bfloat16)
    r1 = m - hi.astype(jnp.float32)
    mid = r1.astype(jnp.bfloat16)
    lo = (r1 - mid.astype(jnp.float32)).astype(jnp.bfloat16)
    ones = jnp.ones((16, TILE), jnp.bfloat16)
    row = None
    for part in (lo, mid, hi):
        p = lax.dot_general(ones, part, (((1,), (1,)), ((), ())), preferred_element_type=jnp.float32)
        row = p if row is None else row + p
    row = jnp.concatenate([row[0:1], jnp.zeros((1, TILE - SCALES * SIG), jnp.float32)], axis=1)

    ga[me] = row
    pl.semaphore_wait(in_xy, 7)
    for o in FAR_FIRST:
        pltpu.make_async_remote_copy(
            src_ref=ga.at[me], dst_ref=ga.at[me], send_sem=sa, recv_sem=ra,
            device_id=other(o), device_id_type=MESH).start()
    wait_all(True, v3, s3)
    many = ga.at[pl.ds(0, DEVICES - 1)]
    pltpu.make_async_remote_copy(
        src_ref=many, dst_ref=many, send_sem=sa, recv_sem=ra, device_id=other(1), device_id_type=MESH).wait_recv()
    sums = [ga[q] for q in range(DEVICES)]
    while len(sums) > 1:
        sums = [u + v for u, v in zip(sums[::2], sums[1::2])]
    full = sums[0] * (1.0 / NODES)
    res = jnp.zeros((8, TILE), jnp.float32)
    sub = lax.broadcasted_iota(jnp.int32, (8, TILE), 0)
    full8 = jnp.broadcast_to(full, (8, TILE))
    for s in range(SCALES):
        v = pltpu.roll(full8, TILE - 16 * s, 1) if s else full8
        res = jnp.where(sub == s, v, res)
    en_ref[...] = res[:SCALES, :SIG]

    pltpu.make_async_remote_copy(
        src_ref=many, dst_ref=many, send_sem=sa, recv_sem=ra, device_id=other(1), device_id_type=MESH).wait_send()


def finish(tot, en, out_h, en_h, sem):
    a = pltpu.make_async_copy(tot, out_h, sem.at[0])
    b = pltpu.make_async_copy(en, en_h, sem.at[1])
    a.start()
    b.start()
    a.wait()
    b.wait()


def shards(signals, tiles, tile_dir, tile_mask, live_rows, bound_rows, scale_coeffs, spectral_bound):
    bf, f32, i32 = jnp.bfloat16, jnp.float32, jnp.int32
    vm, sm = pltpu.VMEM, pltpu.SMEM
    in_vmem = pl.BlockSpec(memory_space=pltpu.VMEM)
    hbm = pl.BlockSpec(memory_space=pl.ANY)
    dma = pltpu.SemaphoreType.DMA
    tot, energy = pl.pallas_call(
        kernel,
        out_shape=(pltpu.VMEM((SCALES, NB, SIG, TILE), f32), pltpu.VMEM((SCALES, SIG), f32)),
        in_specs=[hbm] * 7 + [pl.BlockSpec(memory_space=pltpu.HBM)],
        out_specs=(in_vmem, in_vmem),
        scratch_shapes=[
            sm((BX, SLOTS, BY), i32), sm((BX, SLOTS, BY), i32), sm((BX, BY), i32), sm((BX, BY), i32),
            sm((SCALES, DEG + 1), f32), sm((1,), f32),
            vm((BX, BY, SIG, TILE), f32), vm((NB, SLOTS, TILE, TILE), bf),
            sm((NB * SLOTS,), i32), sm((NB * SLOTS,), i32),
            vm((NX, 32, TILE), bf), vm((NX, SIG, TILE), bf), vm((NX, SIG, TILE), bf), vm((NX, SIG, TILE), bf),
            vm((DEG, NB, SIG, TILE), f32), vm((NB, 8, TILE), f32),
            vm((3, 2, SIG, TILE), bf), vm((3, 2, SIG, TILE), bf), vm((3, 2, 1, TILE), f32),
            vm((2, 3, SIG, TILE), f32), vm((2, 3, SIG, TILE), f32), vm((2, 10, 32, TILE), bf),
            vm((8, 3, 2, SIG, TILE), bf), vm((8, 3, 2, SIG, TILE), bf), vm((8, 3, 2, 1, TILE), f32),
            vm((8, 2, 3, SIG, TILE), f32), vm((8, 2, 3, SIG, TILE), f32), vm((8, 2, 10, 32, TILE), bf),
            vm((DEVICES, 1, TILE), f32), vm((1024, 1, TILE), f32),
            dma((11,)), dma, dma, dma, dma, dma,
            dma, dma, pltpu.SemaphoreType.REGULAR, pltpu.SemaphoreType.REGULAR,
        ],
        compiler_params=pltpu.CompilerParams(collective_id=0, has_side_effects=True),
        name="wavelet",
    )(signals, tiles, jnp.swapaxes(tile_dir, 1, 2), jnp.swapaxes(tile_mask, 1, 2), live_rows, bound_rows,
      scale_coeffs, spectral_bound)
    out, energy = pl.pallas_call(
        finish,
        out_shape=(jax.ShapeDtypeStruct((SCALES, NB, SIG, TILE), f32), jax.ShapeDtypeStruct((SCALES, SIG), f32)),
        in_specs=[in_vmem, in_vmem],
        out_specs=(hbm, hbm),
        scratch_shapes=[dma((2,))],
        name="finish",
    )(pltpu.with_memory_space_constraint(tot, pltpu.VMEM), pltpu.with_memory_space_constraint(energy, pltpu.VMEM))
    return out.reshape(SCALES, BX, BY, SIG, TILE), energy


def solution(mesh):
    placed = (
        P("gx", "gy", None, None),
        P("gx", "gy", None, None, None),
        P("gx", "gy", None),
        P("gx", "gy", None),
        P("gx", "gy"),
        P("gx", "gy"),
        P(),
        P(),
    )
    return jax.shard_map(
        shards,
        mesh=mesh,
        in_specs=placed,
        out_specs=(P(None, "gx", "gy", None, None), P()),
        check_vma=False,
    )
```

```python
import functools
import operator

import jax
import jax.numpy as jnp
from jax import lax
from jax.experimental import pallas as pl
from jax.experimental.pallas import tpu as pltpu
from jax.sharding import PartitionSpec as P

MESH = pl.DeviceIdType.MESH
SIG, SCALES, DEG, SLOTS, TILE = 16, 6, 4, 4, 128
BX, BY = 2, 8
NB = BX * BY
GXN, GYN = 32, 4
ZERO = NB + (BX + 2) * (BY + 2)
NX = ZERO + 1
NODES = 64 * 32 * 128
DIRS = [(-1, 0), (1, 0), (0, -1), (0, 1), (-1, -1), (-1, 1), (1, -1), (1, 1)]
OPP = [DIRS.index((-dx, -dy)) for dx, dy in DIRS]


def hops(o):
    ring = (0, 1, 2, 1)
    return ring[o & 3] + ring[o >> 3 & 3] + ring[o >> 5 & 3] + 0.1 * (o >> 2 & 1)


DEVICES = 128
FAR_FIRST = sorted(range(1, DEVICES), key=lambda o: (-hops(o), o))


def kernel(sig_h, til_h, dir_h, msk_h, liv_h, bnd_h, cof_h, spb_h,
           tot, en_ref,
           dir_s, msk_s, liv_s, bnd_s, cof_s, spb_s, sig, til, idx, loc, x1, x2, x3, x4, cheb, amul,
           op1, op3, eg, sp1, sp3, tp, rv1, rv3, re, rs1, rs3, tr, ga, units,
           ld, r1, r2, w1, r3, r4, w3, sa, ra, in_y, in_xy):
    gx, gy = lax.axis_index("gx"), lax.axis_index("gy")
    me = gx * GYN + gy
    early = []
    for n, (src, dst) in enumerate(((sig_h, sig), (liv_h, liv_s), (bnd_h, bnd_s), (dir_h, dir_s), (msk_h, msk_s),
                                    (cof_h, cof_s), (spb_h, spb_s))):
        cp = pltpu.make_async_copy(src, dst, ld.at[n])
        cp.start()
        early.append(cp)

    def exists(d):
        dx, dy = DIRS[d]
        ok = None
        for step, pos, n in ((dx, gx, GXN), (dy, gy, GYN)):
            if step == 0:
                continue
            this = pos > 0 if step < 0 else pos < n - 1
            ok = this if ok is None else jnp.logical_and(ok, this)
        return ok

    have = [exists(d) for d in range(8)]
    peer = [(gx + dx, gy + dy) for dx, dy in DIRS]
    flip = lambda v: (v, v + 1 - 2 * (v % 2), (v + 2) % 4, 3 - v)
    xs, ys, zs = flip(gx // 8), flip(gx // 2 % 4), flip(gy)
    xyc = [8 * u + 2 * v + w for u in xs for v in ys for w in (gx % 2, 1 - gx % 2)]
    other = lambda o: (xyc[(o >> 5) * 8 + (o >> 3) % 4 * 2 + (o >> 2) % 2], zs[o % 4])
    rest = (1, 2, 3, 4, 5, 6, 7)
    ring_y, ring_x = (8, 16, 24), (32, 64, 96)
    bar = pltpu.get_barrier_semaphore()
    for d in (4, 5, 6, 7, 0, 1, 2, 3):
        @pl.when(have[d])
        def _(d=d):
            pl.semaphore_signal(bar, inc=1, device_id=peer[d], device_id_type=MESH)
    for o in ring_x + ring_y + rest:
        pl.semaphore_signal(bar, inc=1, device_id=other(o), device_id_type=MESH)
    count = jnp.int32(13)
    for d in range(8):
        count = count + have[d].astype(jnp.int32)
    til_cp = []
    for n in range(4):
        cp = pltpu.make_async_copy(til_h.at[n // 2, pl.ds(4 * (n % 2), 4)], til.at[pl.ds(4 * n, 4)], ld.at[7 + n])
        cp.start()
        til_cp.append(cp)
    for cp in early:
        cp.wait()

    lane = lax.broadcasted_iota(jnp.int32, (1, TILE), 1)
    low, high, left = lane < 32, lane >= 96, lane < 64
    middle = jnp.logical_and(lane >= 32, lane < 96)
    f = 2.0 / spb_s[0]
    bf16 = lambda a: a.astype(jnp.bfloat16)
    f32 = lambda a: a.astype(jnp.float32)
    for xb in (x1, x2, x3, x4):
        xb[ZERO] = jnp.zeros(xb.shape[1:], xb.dtype)

    def live_of(b):
        return (lane < liv_s[b // BY, b % BY]).astype(jnp.float32)

    def edge_of(b):
        return (lane < bnd_s[b // BY, b % BY]).astype(jnp.float32)

    def shift(v, q):
        q = q % 4
        return pltpu.roll(v, 32 * q, 1) if q else v

    def add_to(packs, i, j, v):
        key = (i, (j + 2) // 4)
        v = shift(v, j + 2)
        packs[key] = v if key not in packs else packs[key] + v

    RING = [(r, q) for r in (1, 4) for q in range(1, 11)] + [(r, q) for r in (2, 3) for q in (1, 10)]
    slot_of = lambda er, ec: NB + (er - 1) * (BY + 2) + ec - 1

    def place(b, v, xb, packs=None):
        xb[b] = bf16(v)
        e = v * edge_of(b)
        xb[slot_of(b // BY + 2, b % BY + 2)] = bf16(e)
        if packs is not None:
            add_to(packs, b // BY, b % BY, e[:SIG])

    def part_v(dx, dy):
        return ({-1: pl.ds(0, 1), 1: pl.ds(2, 1), 0: pl.ds(0, 3)}[dy],)

    def part_s(dx, dy):
        return ({-1: pl.ds(0, 1), 1: pl.ds(1, 1), 0: pl.ds(0, 2)}[dx],
                {-1: pl.ds(0, 1), 1: pl.ds(2, 1), 0: pl.ds(0, 3)}[dy])

    def part_t(dx, dy):
        return ({-1: pl.ds(0, 1), 1: pl.ds(1, 1), 0: pl.ds(0, 2)}[dx],
                {-1: pl.ds(0, 2), 1: pl.ds(8, 2), 0: pl.ds(0, 10)}[dy])

    def descriptor(src, dst, part, s_sem, r_sem, d, o, at):
        return pltpu.make_async_remote_copy(
            src_ref=src.at[at], dst_ref=dst.at[(o,) + at], send_sem=s_sem, recv_sem=r_sem,
            device_id=peer[d], device_id_type=MESH)

    def send(*messages):
        for d in (4, 5, 6, 7, 0, 1, 2, 3):
            @pl.when(have[d])
            def _(d=d):
                for src, dst, part, s_sem, r_sem in messages:
                    descriptor(src, dst, part, s_sem, r_sem, d, OPP[d], part(*DIRS[d])).start()

    inner_x = jnp.logical_and(gx > 0, gx < GXN - 1)
    inner_y = jnp.logical_and(gy > 0, gy < GYN - 1)

    def wait_all(sent, *messages):
        def size(d):
            n = 0
            for src, _, part, _, _ in messages:
                at = part(*DIRS[d])
                shape = [p.size for p in at] + list(src.shape[len(at):])
                n += src.dtype.itemsize * functools.reduce(operator.mul, shape) // 512
            return n

        _, _, _, s_sem, r_sem = messages[0]
        for nx in (1, 2):
            for ny in (1, 2):
                n = nx * size(0) + ny * size(2) + nx * ny * size(4)
                this = jnp.logical_and(inner_x == (nx == 2), inner_y == (ny == 2))

                @pl.when(this)
                def _(n=n):
                    ref = units.at[pl.ds(0, n)]
                    cp = pltpu.make_async_remote_copy(
                        src_ref=ref, dst_ref=ref, send_sem=s_sem, recv_sem=r_sem,
                        device_id=other(1), device_id_type=MESH)
                    cp.wait_send() if sent else cp.wait_recv()

    first = ((op1, rv1, part_v, w1, r1), (eg, re, part_v, w1, r1), (sp1, rs1, part_s, w1, r2), (tp, tr, part_t, w1, r2))
    v3, s3 = (op3, rv3, part_v, w3, r3), (sp3, rs3, part_s, w3, r4)
    U, D, L, R, UL, UR, DL, DR = range(8)

    def contract(lhs, rhs):
        return lax.dot_general(lhs, rhs, (((1,), (1,)), ((), ())), preferred_element_type=jnp.float32)

    packs, epacks = {}, {}
    top = lax.broadcasted_iota(jnp.int32, (16, TILE), 0) == 0
    for b in range(NB):
        live = live_of(b)
        v = sig[b // BY, b % BY] * live
        cheb[0, b] = v
        place(b, jnp.concatenate([v, jnp.where(top, live, 0.0)], axis=0), x1, packs)
        add_to(epacks, b // BY, b % BY, edge_of(b))
    for (i, t), v in packs.items():
        op1[t, i] = bf16(v)
    for (i, t), v in epacks.items():
        eg[t, i] = v

    for b in range(NB):
        i, j = b // BY, b % BY
        for s in range(SLOTS):
            d = dir_s[i, s, j]
            r = (d * 11) >> 5
            q = d - 3 * r
            off = jnp.where(d == 4, b, NB + (i + r) * (BY + 2) + (j + q))
            off = jnp.where(msk_s[i, s, j] == 1, off, ZERO)
            idx[b * SLOTS + s] = off
            away = r == 2 * i
            if j in (0, BY - 1):
                away = jnp.logical_or(away, q == (0 if j == 0 else 2))
            loc[b * SLOTS + s] = jnp.where(away, ZERO, off)

    def sorted_rows(b, wanted):
        i, j = b // BY, b % BY
        total = None
        tiles = [f32(til[b, s, pl.ds(0, 32)]) for s in range(SLOTS)]
        for d, group in wanted:
            acc = None
            for s in range(SLOTS):
                on = jnp.logical_and(dir_s[i, s, j] == d, msk_s[i, s, j] == 1).astype(jnp.float32)
                t = tiles[s] * on
                acc = t if acc is None else acc + t
            acc = shift(jnp.where(low, acc, 0.0), group)
            total = acc if total is None else total + acc
        inside = lax.broadcasted_iota(jnp.int32, (32, TILE), 0) < bnd_s[i, j]
        return bf16(jnp.where(inside, total, 0.0))

    def directions(b):
        i, j = b // BY, b % BY
        yield None, [(6 * i + q, j + 1 + q) for q in range(3)]
        if j == 0:
            yield 0, [(3 - 3 * i, 1), (6 - 3 * i, 0)]
        if j == BY - 1:
            yield 1, [(5 - 3 * i, 2), (8 - 3 * i, 3)]

    def product(b, xb, table, rows=TILE):
        acc = None
        for h in range(2):
            pick = [xb[table[b * SLOTS + 2 * h + n]] for n in range(2)]
            rhs = [til[b, 2 * h + n, :rows] for n in range(2)]
            p = contract(jnp.concatenate(pick, axis=1), jnp.concatenate(rhs, axis=1))
            acc = p if acc is None else acc + p
        return acc

    def local_part(k, xb, sp):
        packs = {}
        for b in range(NB):
            acc = product(b, xb, loc, 32)
            v = cheb[k, b, :, :32]
            if k == 0:
                out = (f * acc[SIG:SIG + 1] - 1.0) * v - f * acc[:SIG]
            else:
                out = amul[b, :1, :32] * v - (2.0 * f) * acc - cheb[k - 1, b, :, :32]
            out = out * edge_of(b)[:, :32]
            add_to(packs, b // BY, b % BY,
                   jnp.concatenate([out, jnp.zeros((SIG, TILE - 32), jnp.float32)], axis=1))
        for (i, t), v in packs.items():
            sp[i, t] = v

    for cp in til_cp:
        cp.wait()
    for b in range(NB):
        for side, wanted in directions(b):
            tp[b // BY, 1 + b % BY if side is None else 9 * side] = sorted_rows(b, wanted)
    local_part(0, x1, sp1)
    pl.semaphore_wait(bar, count)
    for message in first:
        send(message)
    for o in ring_x:
        pl.semaphore_signal(in_y, inc=1, device_id=other(o), device_id_type=MESH)

    for d in range(8):
        @pl.when(jnp.logical_not(have[d]))
        def _(d=d):
            for buf in (rv1, rv3, re, rs1, rs3, tr):
                buf[d] = jnp.zeros(buf.shape[1:], buf.dtype)

    def add_totals(k):
        for s in range(SCALES):
            a = cof_s[s, k] * 0.5 if k == 0 else cof_s[s, k]
            for b in range(NB):
                t = a * cheb[k, b]
                tot[s, b] = t if k == 0 else tot[s, b] + t

    def rows_of(op, rv):
        rows = []
        for r in range(6):
            i = r % 2
            if r in (2, 3):
                lo, hi, mine = rv[L, 2, i], rv[R, 0, i], [op[t, i] for t in range(3)]
            else:
                u, ul, ur = (U, UL, UR) if r < 2 else (D, DL, DR)
                lo, hi, mine = rv[ul, 2, i], rv[ur, 0, i], [rv[u, t, i] for t in range(3)]
            mine = [f32(v) for v in mine]
            rows.append([jnp.where(left, f32(lo), mine[0]), mine[1], jnp.where(left, mine[2], f32(hi))])
        return rows

    def with_edges(rows, edges):
        return [[jnp.concatenate([v, jnp.where(top, e, 0.0)], axis=0) for v, e in zip(r, q)]
                for r, q in zip(rows, edges)]

    class Inputs:
        def __init__(self, rows):
            self.rows, self.made = rows, {}

        def get(self, key, make):
            if key not in self.made:
                self.made[key] = bf16(make())
            return self.made[key]

        def plain(self, r, t):
            return self.get(("p", r, t), lambda: self.rows[r][t])

        def row(self, r, c):
            t, q, rows = c // 4, c % 4, self.rows[r]
            if q == 0:
                return self.get(("a", r, t), lambda: jnp.where(high, rows[t - 1], rows[t]))
            if q == 3:
                return self.get(("b", r, t), lambda: jnp.where(low, rows[t + 1], rows[t]))
            return self.plain(r, t)

        def crossing(self, r, t):
            rows = self.rows[r]
            before = rows[t - 1] if t > 0 else jnp.zeros_like(rows[t])
            after = rows[t + 1] if t < 2 else jnp.zeros_like(rows[t])
            return self.get(("x", r, t), lambda: jnp.where(left, after, before))

        def column(self, r, t):
            one, two = self.rows[r][t], self.rows[r + 1][t]
            return self.get(("c", r, t), lambda: jnp.where(
                middle, one, jnp.where(left, shift(two, -1), shift(two, 1))))

    def unpack(rows, xb):
        for er, ec in RING:
            v = jnp.where(low, shift(rows[er][ec // 4], -ec), 0.0)
            xb[slot_of(er, ec)] = bf16(v)

    r_iota = lax.broadcasted_iota(jnp.int32, (TILE, TILE), 0)
    c_iota = lax.broadcasted_iota(jnp.int32, (TILE, TILE), 1)
    across = jnp.logical_or(jnp.logical_and(r_iota < 32, c_iota >= 96), jnp.logical_and(r_iota >= 96, c_iota < 32))

    def advance_ring(rows, rs, first):
        ins = Inputs(rows)
        none = jnp.zeros((32, TILE), jnp.bfloat16)
        zero = jnp.zeros((TILE, TILE), jnp.float32)

        def update(own, lhs, rhs, v):
            acc = contract(jnp.concatenate(lhs, axis=1), jnp.concatenate(rhs, axis=1))
            if first:
                return own + f * (acc[SIG:SIG + 1] * v[:SIG] - acc[:SIG])
            return own - (2.0 * f) * acc

        new = [[None] * 3 for _ in range(6)]
        for er, u, ul, ur in ((1, U, UL, UR), (4, D, DL, DR)):
            i = 1 if er == 1 else 0
            feed = er + 1 if i else er - 1
            edge = er - i
            for t in range(3):
                if t == 1:
                    w = [tr[u, i, 3 + n] for n in range(4)]
                    own, wq = rs[u, i, 1], None
                elif t == 0:
                    w = [none, tr[ul, i, 8], tr[u, i, 1], tr[u, i, 2]]
                    wq = [none, tr[ul, i, 9], tr[u, i, 0], none]
                    own = jnp.where(left, rs[ul, i, 2], rs[u, i, 0])
                else:
                    w = [tr[u, i, 7], tr[u, i, 8], tr[ur, i, 1], none]
                    wq = [none, tr[u, i, 9], tr[ur, i, 0], none]
                    own = jnp.where(left, rs[u, i, 2], rs[ur, i, 0])
                w = f32(jnp.concatenate(w, axis=0))
                lhs = [ins.plain(feed, t), ins.crossing(feed, t)]
                rhs = [bf16(jnp.where(across, zero, w)), bf16(jnp.where(across, w, zero))]
                if wq is not None:
                    lhs.append(ins.column(edge, t))
                    rhs.append(jnp.concatenate(wq, axis=0))
                new[er][t] = update(own, lhs, rhs, rows[er][t])
        for er, i in ((2, 0), (3, 1)):
            feed = er - 1 if i == 0 else er + 1
            for t, o, p, q in ((0, L, 8, 9), (2, R, 1, 0)):
                at = 1 if t == 0 else 2
                pad = lambda w: jnp.concatenate([none] * at + [w] + [none] * (3 - at), axis=0)
                new[er][t] = update(rs[o, i, 2 - t], [ins.plain(feed, t), ins.column(2, t)],
                                    [pad(tr[o, i, p]), pad(tr[o, i, q])], rows[er][t])
        return new

    add_totals(0)
    pl.semaphore_wait(in_y, 3)
    for o in rest:
        pl.semaphore_signal(in_xy, inc=1, device_id=other(o), device_id_type=MESH)

    wait_all(False, *first[:2])
    rows = with_edges(rows_of(op1, rv1), rows_of(eg, re))
    unpack(rows, x1)
    for b in range(NB):
        acc = product(b, x1, idx)
        fl = f * live_of(b)
        am = fl * acc[SIG:SIG + 1] - 1.0
        amul[b] = jnp.broadcast_to(2.0 * am, (8, TILE))
        cur = am * cheb[0, b] - fl * acc[:SIG]
        cheb[1, b] = cur
        place(b, cur, x2)
    wait_all(False, *first[2:])
    unpack(advance_ring(rows, rs1, 1), x2)

    def step(b, k, xb):
        acc = product(b, xb, idx)
        am = amul[b]
        am = jnp.concatenate([am, am], axis=0)
        return am * cheb[k, b] - (2.0 * f * live_of(b)) * acc - cheb[k - 1, b]

    packs = {}
    for b in range(NB):
        cur = step(b, 1, x2)
        cheb[2, b] = cur
        place(b, cur, x3, packs)
    for (i, t), v in packs.items():
        op3[t, i] = bf16(v)
    send(v3)
    local_part(2, x3, sp3)
    send(s3)
    add_totals(1)
    add_totals(2)
    wait_all(True, *first)

    wait_all(False, v3)
    rows = rows_of(op3, rv3)
    unpack(rows, x3)
    for b in range(NB):
        cur = step(b, 2, x3)
        cheb[3, b] = cur
        place(b, cur, x4)
    add_totals(3)
    wait_all(False, s3)
    unpack(advance_ring(rows, rs3, 0), x4)
    sq = [None] * SCALES
    for b in range(NB):
        cur = step(b, 3, x4)
        for s in range(SCALES):
            t = tot[s, b] + cof_s[s, 4] * cur
            tot[s, b] = t
            sq[s] = t * t if sq[s] is None else sq[s] + t * t

    m = jnp.concatenate(sq, axis=0)
    hi = m.astype(jnp.bfloat16)
    r1 = m - hi.astype(jnp.float32)
    mid = r1.astype(jnp.bfloat16)
    lo = (r1 - mid.astype(jnp.float32)).astype(jnp.bfloat16)
    ones = jnp.ones((16, TILE), jnp.bfloat16)
    row = None
    for part in (lo, mid, hi):
        p = lax.dot_general(ones, part, (((1,), (1,)), ((), ())), preferred_element_type=jnp.float32)
        row = p if row is None else row + p
    row = jnp.concatenate([row[0:1], jnp.zeros((1, TILE - SCALES * SIG), jnp.float32)], axis=1)

    ga[me] = row
    pl.semaphore_wait(in_xy, 7)
    for o in FAR_FIRST:
        pltpu.make_async_remote_copy(
            src_ref=ga.at[me], dst_ref=ga.at[me], send_sem=sa, recv_sem=ra,
            device_id=other(o), device_id_type=MESH).start()
    wait_all(True, v3, s3)
    many = ga.at[pl.ds(0, DEVICES - 1)]
    pltpu.make_async_remote_copy(
        src_ref=many, dst_ref=many, send_sem=sa, recv_sem=ra, device_id=other(1), device_id_type=MESH).wait_recv()
    sums = [ga[q] for q in range(DEVICES)]
    while len(sums) > 1:
        sums = [u + v for u, v in zip(sums[::2], sums[1::2])]
    full = sums[0] * (1.0 / NODES)
    res = jnp.zeros((8, TILE), jnp.float32)
    sub = lax.broadcasted_iota(jnp.int32, (8, TILE), 0)
    full8 = jnp.broadcast_to(full, (8, TILE))
    for s in range(SCALES):
        v = pltpu.roll(full8, TILE - 16 * s, 1) if s else full8
        res = jnp.where(sub == s, v, res)
    en_ref[...] = res[:SCALES, :SIG]

    pltpu.make_async_remote_copy(
        src_ref=many, dst_ref=many, send_sem=sa, recv_sem=ra, device_id=other(1), device_id_type=MESH).wait_send()


def finish(tot, en, out_h, en_h, sem):
    a = pltpu.make_async_copy(tot, out_h, sem.at[0])
    b = pltpu.make_async_copy(en, en_h, sem.at[1])
    a.start()
    b.start()
    a.wait()
    b.wait()


def shards(signals, tiles, tile_dir, tile_mask, live_rows, bound_rows, scale_coeffs, spectral_bound):
    bf, f32, i32 = jnp.bfloat16, jnp.float32, jnp.int32
    vm, sm = pltpu.VMEM, pltpu.SMEM
    in_vmem = pl.BlockSpec(memory_space=pltpu.VMEM)
    hbm = pl.BlockSpec(memory_space=pl.ANY)
    dma = pltpu.SemaphoreType.DMA
    tot, energy = pl.pallas_call(
        kernel,
        out_shape=(pltpu.VMEM((SCALES, NB, SIG, TILE), f32), pltpu.VMEM((SCALES, SIG), f32)),
        in_specs=[hbm] * 7 + [pl.BlockSpec(memory_space=pltpu.HBM)],
        out_specs=(in_vmem, in_vmem),
        scratch_shapes=[
            sm((BX, SLOTS, BY), i32), sm((BX, SLOTS, BY), i32), sm((BX, BY), i32), sm((BX, BY), i32),
            sm((SCALES, DEG + 1), f32), sm((1,), f32),
            vm((BX, BY, SIG, TILE), f32), vm((NB, SLOTS, TILE, TILE), bf),
            sm((NB * SLOTS,), i32), sm((NB * SLOTS,), i32),
            vm((NX, 32, TILE), bf), vm((NX, SIG, TILE), bf), vm((NX, SIG, TILE), bf), vm((NX, SIG, TILE), bf),
            vm((DEG, NB, SIG, TILE), f32), vm((NB, 8, TILE), f32),
            vm((3, 2, SIG, TILE), bf), vm((3, 2, SIG, TILE), bf), vm((3, 2, 1, TILE), f32),
            vm((2, 3, SIG, TILE), f32), vm((2, 3, SIG, TILE), f32), vm((2, 10, 32, TILE), bf),
            vm((8, 3, 2, SIG, TILE), bf), vm((8, 3, 2, SIG, TILE), bf), vm((8, 3, 2, 1, TILE), f32),
            vm((8, 2, 3, SIG, TILE), f32), vm((8, 2, 3, SIG, TILE), f32), vm((8, 2, 10, 32, TILE), bf),
            vm((DEVICES, 1, TILE), f32), vm((1024, 1, TILE), f32),
            dma((11,)), dma, dma, dma, dma, dma, dma,
            dma, dma, pltpu.SemaphoreType.REGULAR, pltpu.SemaphoreType.REGULAR,
        ],
        compiler_params=pltpu.CompilerParams(collective_id=0, has_side_effects=True),
        name="wavelet",
    )(signals, tiles, jnp.swapaxes(tile_dir, 1, 2), jnp.swapaxes(tile_mask, 1, 2), live_rows, bound_rows,
      scale_coeffs, spectral_bound)
    out, energy = pl.pallas_call(
        finish,
        out_shape=(jax.ShapeDtypeStruct((SCALES, NB, SIG, TILE), f32), jax.ShapeDtypeStruct((SCALES, SIG), f32)),
        in_specs=[in_vmem, in_vmem],
        out_specs=(hbm, hbm),
        scratch_shapes=[dma((2,))],
        name="finish",
    )(pltpu.with_memory_space_constraint(tot, pltpu.VMEM), pltpu.with_memory_space_constraint(energy, pltpu.VMEM))
    return out.reshape(SCALES, BX, BY, SIG, TILE), energy


def solution(mesh):
    placed = (
        P("gx", "gy", None, None),
        P("gx", "gy", None, None, None),
        P("gx", "gy", None),
        P("gx", "gy", None),
        P("gx", "gy"),
        P("gx", "gy"),
        P(),
        P(),
    )
    return jax.shard_map(
        shards,
        mesh=mesh,
        in_specs=placed,
        out_specs=(P(None, "gx", "gy", None, None), P()),
        check_vma=False,
    )
```

```python
import functools
import operator

import jax
import jax.numpy as jnp
from jax import lax
from jax.experimental import pallas as pl
from jax.experimental.pallas import tpu as pltpu
from jax.sharding import PartitionSpec as P

MESH = pl.DeviceIdType.MESH
SIG, SCALES, DEG, SLOTS, TILE = 16, 6, 4, 4, 128
BX, BY = 2, 8
NB = BX * BY
GXN, GYN = 32, 4
ZERO = NB + (BX + 2) * (BY + 2)
NX = ZERO + 1
NODES = 64 * 32 * 128
DIRS = [(-1, 0), (1, 0), (0, -1), (0, 1), (-1, -1), (-1, 1), (1, -1), (1, 1)]
OPP = [DIRS.index((-dx, -dy)) for dx, dy in DIRS]


def hops(o):
    ring = (0, 1, 2, 1)
    return ring[o & 3] + ring[o >> 3 & 3] + ring[o >> 5 & 3] + 0.1 * (o >> 2 & 1)


DEVICES = 128
FAR_FIRST = sorted(range(1, DEVICES), key=lambda o: (-hops(o), o))


def kernel(sig_h, til_h, dir_h, msk_h, liv_h, bnd_h, cof_h, spb_h,
           tot, en_ref,
           dir_s, msk_s, liv_s, bnd_s, cof_s, spb_s, sig, til, idx, loc, x1, x2, x3, x4, cheb, amul,
           op1, op3, eg, sp1, sp3, tp, oc1, oc3, ec1, sc1, sc3,
           rv1, rv3, re, rs1, rs3, tr, rc1, rc3, rec, rsc1, rsc3, ga, units,
           ld, r1, r2, w1, r3, r4, w3, sa, ra, in_y, in_xy):
    gx, gy = lax.axis_index("gx"), lax.axis_index("gy")
    me = gx * GYN + gy
    early = []
    for n, (src, dst) in enumerate(((sig_h, sig), (liv_h, liv_s), (bnd_h, bnd_s), (dir_h, dir_s), (msk_h, msk_s),
                                    (cof_h, cof_s), (spb_h, spb_s))):
        cp = pltpu.make_async_copy(src, dst, ld.at[n])
        cp.start()
        early.append(cp)

    def exists(d):
        dx, dy = DIRS[d]
        ok = None
        for step, pos, n in ((dx, gx, GXN), (dy, gy, GYN)):
            if step == 0:
                continue
            this = pos > 0 if step < 0 else pos < n - 1
            ok = this if ok is None else jnp.logical_and(ok, this)
        return ok

    have = [exists(d) for d in range(8)]
    peer = [(gx + dx, gy + dy) for dx, dy in DIRS]
    flip = lambda v: (v, v + 1 - 2 * (v % 2), (v + 2) % 4, 3 - v)
    xs, ys, zs = flip(gx // 8), flip(gx // 2 % 4), flip(gy)
    xyc = [8 * u + 2 * v + w for u in xs for v in ys for w in (gx % 2, 1 - gx % 2)]
    other = lambda o: (xyc[(o >> 5) * 8 + (o >> 3) % 4 * 2 + (o >> 2) % 2], zs[o % 4])
    rest = (1, 2, 3, 4, 5, 6, 7)
    ring_y, ring_x = (8, 16, 24), (32, 64, 96)
    bar = pltpu.get_barrier_semaphore()
    for d in (4, 5, 6, 7, 0, 1, 2, 3):
        @pl.when(have[d])
        def _(d=d):
            pl.semaphore_signal(bar, inc=1, device_id=peer[d], device_id_type=MESH)
    for o in ring_x + ring_y + rest:
        pl.semaphore_signal(bar, inc=1, device_id=other(o), device_id_type=MESH)
    count = jnp.int32(13)
    for d in range(8):
        count = count + have[d].astype(jnp.int32)
    til_cp = []
    for n in range(4):
        cp = pltpu.make_async_copy(til_h.at[n // 2, pl.ds(4 * (n % 2), 4)], til.at[pl.ds(4 * n, 4)], ld.at[7 + n])
        cp.start()
        til_cp.append(cp)
    for cp in early:
        cp.wait()

    lane = lax.broadcasted_iota(jnp.int32, (1, TILE), 1)
    low, high, left = lane < 32, lane >= 96, lane < 64
    middle = jnp.logical_and(lane >= 32, lane < 96)
    f = 2.0 / spb_s[0]
    bf16 = lambda a: a.astype(jnp.bfloat16)
    f32 = lambda a: a.astype(jnp.float32)
    for xb in (x1, x2, x3, x4):
        xb[ZERO] = jnp.zeros(xb.shape[1:], xb.dtype)

    def live_of(b):
        return (lane < liv_s[b // BY, b % BY]).astype(jnp.float32)

    def edge_of(b):
        return (lane < bnd_s[b // BY, b % BY]).astype(jnp.float32)

    def shift(v, q):
        q = q % 4
        return pltpu.roll(v, 32 * q, 1) if q else v

    def add_to(packs, i, j, v, column):
        for key, group in ((("m", i, (j + 2) // 4), j + 2),
                           (("c", 0 if j < BY // 2 else 1), j + 2 + 2 * i)):
            if key[0] == "c" and j not in column:
                continue
            w = shift(v, group)
            packs[key] = w if key not in packs else packs[key] + w

    def flush(packs, main, column, cast, tile_first):
        for key, v in packs.items():
            if key[0] == "c":
                column[key[1]] = cast(v)
            elif tile_first:
                main[key[2], key[1]] = cast(v)
            else:
                main[key[1], key[2]] = cast(v)

    same = lambda v: v
    TWO, ONE = (0, 1, 6, 7), (0, 7)

    RING = [(r, q) for r in (1, 4) for q in range(1, 11)] + [(r, q) for r in (2, 3) for q in (1, 10)]
    slot_of = lambda er, ec: NB + (er - 1) * (BY + 2) + ec - 1

    def place(b, v, xb, packs=None):
        xb[b] = bf16(v)
        e = v * edge_of(b)
        xb[slot_of(b // BY + 2, b % BY + 2)] = bf16(e)
        if packs is not None:
            add_to(packs, b // BY, b % BY, e[:SIG], TWO)

    def part_v(dx, dy):
        return (pl.ds(0, 3),) if dy == 0 else None

    def part_s(dx, dy):
        return ({-1: pl.ds(0, 1), 1: pl.ds(1, 1)}[dx], pl.ds(0, 3)) if dy == 0 else None

    def part_c(dx, dy):
        return (pl.ds((dy + 1) // 2, 1),) if dy != 0 else None

    def part_t(dx, dy):
        return ({-1: pl.ds(0, 1), 1: pl.ds(1, 1), 0: pl.ds(0, 2)}[dx],
                {-1: pl.ds(0, 2), 1: pl.ds(8, 2), 0: pl.ds(0, 10)}[dy])

    def descriptor(src, dst, part, s_sem, r_sem, d, o, at):
        return pltpu.make_async_remote_copy(
            src_ref=src.at[at], dst_ref=dst.at[(o,) + at], send_sem=s_sem, recv_sem=r_sem,
            device_id=peer[d], device_id_type=MESH)

    def send(*messages):
        for d in (4, 5, 6, 7, 0, 1, 2, 3):
            @pl.when(have[d])
            def _(d=d):
                for src, dst, part, s_sem, r_sem in messages:
                    at = part(*DIRS[d])
                    if at is not None:
                        descriptor(src, dst, part, s_sem, r_sem, d, OPP[d], at).start()

    inner_x = jnp.logical_and(gx > 0, gx < GXN - 1)
    inner_y = jnp.logical_and(gy > 0, gy < GYN - 1)

    def wait_all(sent, *messages):
        def size(d):
            n = 0
            for src, _, part, _, _ in messages:
                at = part(*DIRS[d])
                if at is None:
                    continue
                shape = [p.size for p in at] + list(src.shape[len(at):])
                n += src.dtype.itemsize * functools.reduce(operator.mul, shape) // 512
            return n

        _, _, _, s_sem, r_sem = messages[0]
        for nx in (1, 2):
            for ny in (1, 2):
                n = nx * size(0) + ny * size(2) + nx * ny * size(4)
                this = jnp.logical_and(inner_x == (nx == 2), inner_y == (ny == 2))

                @pl.when(this)
                def _(n=n):
                    ref = units.at[pl.ds(0, n)]
                    cp = pltpu.make_async_remote_copy(
                        src_ref=ref, dst_ref=ref, send_sem=s_sem, recv_sem=r_sem,
                        device_id=other(1), device_id_type=MESH)
                    cp.wait_send() if sent else cp.wait_recv()

    first = ((oc1, rc1, part_c, w1, r1), (op1, rv1, part_v, w1, r1), (eg, re, part_v, w1, r1), (ec1, rec, part_c, w1, r1),
             (sp1, rs1, part_s, w1, r2), (sc1, rsc1, part_c, w1, r2), (tp, tr, part_t, w1, r2))
    v3 = ((oc3, rc3, part_c, w3, r3), (op3, rv3, part_v, w3, r3))
    s3 = ((sp3, rs3, part_s, w3, r4), (sc3, rsc3, part_c, w3, r4))
    U, D, L, R, UL, UR, DL, DR = range(8)

    def contract(lhs, rhs):
        return lax.dot_general(lhs, rhs, (((1,), (1,)), ((), ())), preferred_element_type=jnp.float32)

    packs, epacks = {}, {}
    top = lax.broadcasted_iota(jnp.int32, (16, TILE), 0) == 0
    for b in range(NB):
        live = live_of(b)
        v = sig[b // BY, b % BY] * live
        cheb[0, b] = v
        place(b, jnp.concatenate([v, jnp.where(top, live, 0.0)], axis=0), x1, packs)
        add_to(epacks, b // BY, b % BY, edge_of(b), TWO)
    flush(packs, op1, oc1, bf16, True)
    flush(epacks, eg, ec1, same, True)

    for b in range(NB):
        i, j = b // BY, b % BY
        for s in range(SLOTS):
            d = dir_s[i, s, j]
            r = (d * 11) >> 5
            q = d - 3 * r
            off = jnp.where(d == 4, b, NB + (i + r) * (BY + 2) + (j + q))
            off = jnp.where(msk_s[i, s, j] == 1, off, ZERO)
            idx[b * SLOTS + s] = off
            away = r == 2 * i
            if j in (0, BY - 1):
                away = jnp.logical_or(away, q == (0 if j == 0 else 2))
            loc[b * SLOTS + s] = jnp.where(away, ZERO, off)

    def sorted_rows(b, wanted):
        i, j = b // BY, b % BY
        total = None
        tiles = [f32(til[b, s, pl.ds(0, 32)]) for s in range(SLOTS)]
        for d, group in wanted:
            acc = None
            for s in range(SLOTS):
                on = jnp.logical_and(dir_s[i, s, j] == d, msk_s[i, s, j] == 1).astype(jnp.float32)
                t = tiles[s] * on
                acc = t if acc is None else acc + t
            acc = shift(jnp.where(low, acc, 0.0), group)
            total = acc if total is None else total + acc
        inside = lax.broadcasted_iota(jnp.int32, (32, TILE), 0) < bnd_s[i, j]
        return bf16(jnp.where(inside, total, 0.0))

    def directions(b):
        i, j = b // BY, b % BY
        yield None, [(6 * i + q, j + 1 + q) for q in range(3)]
        if j == 0:
            yield 0, [(3 - 3 * i, 1), (6 - 3 * i, 0)]
        if j == BY - 1:
            yield 1, [(5 - 3 * i, 2), (8 - 3 * i, 3)]

    def product(b, xb, table, rows=TILE):
        acc = None
        for h in range(2):
            pick = [xb[table[b * SLOTS + 2 * h + n]] for n in range(2)]
            rhs = [til[b, 2 * h + n, :rows] for n in range(2)]
            p = contract(jnp.concatenate(pick, axis=1), jnp.concatenate(rhs, axis=1))
            acc = p if acc is None else acc + p
        return acc

    def local_part(k, xb, sp, sc):
        packs = {}
        for b in range(NB):
            acc = product(b, xb, loc, 32)
            v = cheb[k, b, :, :32]
            if k == 0:
                out = (f * acc[SIG:SIG + 1] - 1.0) * v - f * acc[:SIG]
            else:
                out = amul[b, :1, :32] * v - (2.0 * f) * acc - cheb[k - 1, b, :, :32]
            out = out * edge_of(b)[:, :32]
            add_to(packs, b // BY, b % BY,
                   jnp.concatenate([out, jnp.zeros((SIG, TILE - 32), jnp.float32)], axis=1), ONE)
        flush(packs, sp, sc, same, False)

    for cp in til_cp:
        cp.wait()
    for b in range(NB):
        for side, wanted in directions(b):
            tp[b // BY, 1 + b % BY if side is None else 9 * side] = sorted_rows(b, wanted)
    local_part(0, x1, sp1, sc1)
    pl.semaphore_wait(bar, count)
    for message in first:
        send(message)
    for o in ring_x:
        pl.semaphore_signal(in_y, inc=1, device_id=other(o), device_id_type=MESH)

    for d in range(8):
        @pl.when(jnp.logical_not(have[d]))
        def _(d=d):
            for buf in (rv1, rv3, re, rs1, rs3, tr, rc1, rc3, rec, rsc1, rsc3):
                buf[d] = jnp.zeros(buf.shape[1:], buf.dtype)

    def add_totals(k):
        for s in range(SCALES):
            a = cof_s[s, k] * 0.5 if k == 0 else cof_s[s, k]
            for b in range(NB):
                t = a * cheb[k, b]
                tot[s, b] = t if k == 0 else tot[s, b] + t

    def beside(rc, i, o):
        side = 1 if o in (L, UL, DL) else 0
        return shift(f32(rc[o, side]), 2 * i)

    def rows_of(op, rv, rc):
        rows = []
        for r in range(6):
            i = r % 2
            if r in (2, 3):
                ul, ur, mine = L, R, [op[t, i] for t in range(3)]
            else:
                u, ul, ur = (U, UL, UR) if r < 2 else (D, DL, DR)
                mine = [rv[u, t, i] for t in range(3)]
            mine = [f32(v) for v in mine]
            rows.append([jnp.where(left, beside(rc, i, ul), mine[0]), mine[1],
                         jnp.where(left, mine[2], beside(rc, i, ur))])
        return rows

    def with_edges(rows, edges):
        return [[jnp.concatenate([v, jnp.where(top, e, 0.0)], axis=0) for v, e in zip(r, q)]
                for r, q in zip(rows, edges)]

    class Inputs:
        def __init__(self, rows):
            self.rows, self.made = rows, {}

        def get(self, key, make):
            if key not in self.made:
                self.made[key] = bf16(make())
            return self.made[key]

        def plain(self, r, t):
            return self.get(("p", r, t), lambda: self.rows[r][t])

        def row(self, r, c):
            t, q, rows = c // 4, c % 4, self.rows[r]
            if q == 0:
                return self.get(("a", r, t), lambda: jnp.where(high, rows[t - 1], rows[t]))
            if q == 3:
                return self.get(("b", r, t), lambda: jnp.where(low, rows[t + 1], rows[t]))
            return self.plain(r, t)

        def crossing(self, r, t):
            rows = self.rows[r]
            before = rows[t - 1] if t > 0 else jnp.zeros_like(rows[t])
            after = rows[t + 1] if t < 2 else jnp.zeros_like(rows[t])
            return self.get(("x", r, t), lambda: jnp.where(left, after, before))

        def column(self, r, t):
            one, two = self.rows[r][t], self.rows[r + 1][t]
            return self.get(("c", r, t), lambda: jnp.where(
                middle, one, jnp.where(left, shift(two, -1), shift(two, 1))))

    def unpack(rows, xb, columns=None):
        for er, ec in RING:
            tile, group = rows[er][ec // 4], ec
            if columns is not None and ec in (1, 10):
                o = {1: {1: UL, 10: UR}, 2: {1: L, 10: R}, 3: {1: L, 10: R}, 4: {1: DL, 10: DR}}[er][ec]
                tile, group = columns(o), ec + 2 * (er % 2)
            v = jnp.where(low, shift(tile, -group), 0.0)
            xb[slot_of(er, ec)] = bf16(v)

    r_iota = lax.broadcasted_iota(jnp.int32, (TILE, TILE), 0)
    c_iota = lax.broadcasted_iota(jnp.int32, (TILE, TILE), 1)
    across = jnp.logical_or(jnp.logical_and(r_iota < 32, c_iota >= 96), jnp.logical_and(r_iota >= 96, c_iota < 32))

    def advance_ring(rows, rs, rsc, first):
        ins = Inputs(rows)
        none = jnp.zeros((32, TILE), jnp.bfloat16)
        zero = jnp.zeros((TILE, TILE), jnp.float32)

        def update(own, lhs, rhs, v):
            acc = contract(jnp.concatenate(lhs, axis=1), jnp.concatenate(rhs, axis=1))
            if first:
                return own + f * (acc[SIG:SIG + 1] * v[:SIG] - acc[:SIG])
            return own - (2.0 * f) * acc

        new = [[None] * 3 for _ in range(6)]
        for er, u, ul, ur in ((1, U, UL, UR), (4, D, DL, DR)):
            i = 1 if er == 1 else 0
            feed = er + 1 if i else er - 1
            edge = er - i
            for t in range(3):
                if t == 1:
                    w = [tr[u, i, 3 + n] for n in range(4)]
                    own, wq = rs[u, i, 1], None
                elif t == 0:
                    w = [none, tr[ul, i, 8], tr[u, i, 1], tr[u, i, 2]]
                    wq = [none, tr[ul, i, 9], tr[u, i, 0], none]
                    own = jnp.where(left, beside(rsc, i, ul), rs[u, i, 0])
                else:
                    w = [tr[u, i, 7], tr[u, i, 8], tr[ur, i, 1], none]
                    wq = [none, tr[u, i, 9], tr[ur, i, 0], none]
                    own = jnp.where(left, rs[u, i, 2], beside(rsc, i, ur))
                w = f32(jnp.concatenate(w, axis=0))
                lhs = [ins.plain(feed, t), ins.crossing(feed, t)]
                rhs = [bf16(jnp.where(across, zero, w)), bf16(jnp.where(across, w, zero))]
                if wq is not None:
                    lhs.append(ins.column(edge, t))
                    rhs.append(jnp.concatenate(wq, axis=0))
                new[er][t] = update(own, lhs, rhs, rows[er][t])
        for er, i in ((2, 0), (3, 1)):
            feed = er - 1 if i == 0 else er + 1
            for t, o, p, q in ((0, L, 8, 9), (2, R, 1, 0)):
                at = 1 if t == 0 else 2
                pad = lambda w: jnp.concatenate([none] * at + [w] + [none] * (3 - at), axis=0)
                new[er][t] = update(beside(rsc, i, o), [ins.plain(feed, t), ins.column(2, t)],
                                    [pad(tr[o, i, p]), pad(tr[o, i, q])], rows[er][t])
        return new

    add_totals(0)
    pl.semaphore_wait(in_y, 3)
    for o in rest:
        pl.semaphore_signal(in_xy, inc=1, device_id=other(o), device_id_type=MESH)

    wait_all(False, *first[:4])
    rows = with_edges(rows_of(op1, rv1, rc1), rows_of(eg, re, rec))

    def column1(o):
        side = 1 if o in (L, UL, DL) else 0
        return jnp.concatenate([f32(rc1[o, side]), jnp.where(top, rec[o, side], 0.0)], axis=0)

    unpack(rows, x1, column1)
    for b in range(NB):
        acc = product(b, x1, idx)
        fl = f * live_of(b)
        am = fl * acc[SIG:SIG + 1] - 1.0
        amul[b] = jnp.broadcast_to(2.0 * am, (8, TILE))
        cur = am * cheb[0, b] - fl * acc[:SIG]
        cheb[1, b] = cur
        place(b, cur, x2)
    wait_all(False, *first[4:])
    unpack(advance_ring(rows, rs1, rsc1, 1), x2)

    def step(b, k, xb):
        acc = product(b, xb, idx)
        am = amul[b]
        am = jnp.concatenate([am, am], axis=0)
        return am * cheb[k, b] - (2.0 * f * live_of(b)) * acc - cheb[k - 1, b]

    packs = {}
    for b in range(NB):
        cur = step(b, 1, x2)
        cheb[2, b] = cur
        place(b, cur, x3, packs)
    flush(packs, op3, oc3, bf16, True)
    for message in v3:
        send(message)
    local_part(2, x3, sp3, sc3)
    for message in s3:
        send(message)
    add_totals(1)
    add_totals(2)
    wait_all(True, *first)

    wait_all(False, *v3)
    rows = rows_of(op3, rv3, rc3)
    unpack(rows, x3, lambda o: f32(rc3[o, 1 if o in (L, UL, DL) else 0]))
    for b in range(NB):
        cur = step(b, 2, x3)
        cheb[3, b] = cur
        place(b, cur, x4)
    add_totals(3)
    wait_all(False, *s3)
    unpack(advance_ring(rows, rs3, rsc3, 0), x4)
    sq = [None] * SCALES
    for b in range(NB):
        cur = step(b, 3, x4)
        for s in range(SCALES):
            t = tot[s, b] + cof_s[s, 4] * cur
            tot[s, b] = t
            sq[s] = t * t if sq[s] is None else sq[s] + t * t

    m = jnp.concatenate(sq, axis=0)
    hi = m.astype(jnp.bfloat16)
    r1 = m - hi.astype(jnp.float32)
    mid = r1.astype(jnp.bfloat16)
    lo = (r1 - mid.astype(jnp.float32)).astype(jnp.bfloat16)
    ones = jnp.ones((16, TILE), jnp.bfloat16)
    row = None
    for part in (lo, mid, hi):
        p = lax.dot_general(ones, part, (((1,), (1,)), ((), ())), preferred_element_type=jnp.float32)
        row = p if row is None else row + p
    row = jnp.concatenate([row[0:1], jnp.zeros((1, TILE - SCALES * SIG), jnp.float32)], axis=1)

    ga[me] = row
    pl.semaphore_wait(in_xy, 7)
    for o in FAR_FIRST:
        pltpu.make_async_remote_copy(
            src_ref=ga.at[me], dst_ref=ga.at[me], send_sem=sa, recv_sem=ra,
            device_id=other(o), device_id_type=MESH).start()
    wait_all(True, *v3, *s3)
    many = ga.at[pl.ds(0, DEVICES - 1)]
    pltpu.make_async_remote_copy(
        src_ref=many, dst_ref=many, send_sem=sa, recv_sem=ra, device_id=other(1), device_id_type=MESH).wait_recv()
    sums = [ga[q] for q in range(DEVICES)]
    while len(sums) > 1:
        sums = [u + v for u, v in zip(sums[::2], sums[1::2])]
    full = sums[0] * (1.0 / NODES)
    res = jnp.zeros((8, TILE), jnp.float32)
    sub = lax.broadcasted_iota(jnp.int32, (8, TILE), 0)
    full8 = jnp.broadcast_to(full, (8, TILE))
    for s in range(SCALES):
        v = pltpu.roll(full8, TILE - 16 * s, 1) if s else full8
        res = jnp.where(sub == s, v, res)
    en_ref[...] = res[:SCALES, :SIG]

    pltpu.make_async_remote_copy(
        src_ref=many, dst_ref=many, send_sem=sa, recv_sem=ra, device_id=other(1), device_id_type=MESH).wait_send()


def finish(tot, en, out_h, en_h, sem):
    a = pltpu.make_async_copy(tot, out_h, sem.at[0])
    b = pltpu.make_async_copy(en, en_h, sem.at[1])
    a.start()
    b.start()
    a.wait()
    b.wait()


def shards(signals, tiles, tile_dir, tile_mask, live_rows, bound_rows, scale_coeffs, spectral_bound):
    bf, f32, i32 = jnp.bfloat16, jnp.float32, jnp.int32
    vm, sm = pltpu.VMEM, pltpu.SMEM
    in_vmem = pl.BlockSpec(memory_space=pltpu.VMEM)
    hbm = pl.BlockSpec(memory_space=pl.ANY)
    dma = pltpu.SemaphoreType.DMA
    tot, energy = pl.pallas_call(
        kernel,
        out_shape=(pltpu.VMEM((SCALES, NB, SIG, TILE), f32), pltpu.VMEM((SCALES, SIG), f32)),
        in_specs=[hbm] * 7 + [pl.BlockSpec(memory_space=pltpu.HBM)],
        out_specs=(in_vmem, in_vmem),
        scratch_shapes=[
            sm((BX, SLOTS, BY), i32), sm((BX, SLOTS, BY), i32), sm((BX, BY), i32), sm((BX, BY), i32),
            sm((SCALES, DEG + 1), f32), sm((1,), f32),
            vm((BX, BY, SIG, TILE), f32), vm((NB, SLOTS, TILE, TILE), bf),
            sm((NB * SLOTS,), i32), sm((NB * SLOTS,), i32),
            vm((NX, 32, TILE), bf), vm((NX, SIG, TILE), bf), vm((NX, SIG, TILE), bf), vm((NX, SIG, TILE), bf),
            vm((DEG, NB, SIG, TILE), f32), vm((NB, 8, TILE), f32),
            vm((3, 2, SIG, TILE), bf), vm((3, 2, SIG, TILE), bf), vm((3, 2, 1, TILE), f32),
            vm((2, 3, SIG, TILE), f32), vm((2, 3, SIG, TILE), f32), vm((2, 10, 32, TILE), bf),
            vm((2, SIG, TILE), bf), vm((2, SIG, TILE), bf), vm((2, 1, TILE), f32), vm((2, SIG, TILE), f32), vm((2, SIG, TILE), f32),
            vm((8, 3, 2, SIG, TILE), bf), vm((8, 3, 2, SIG, TILE), bf), vm((8, 3, 2, 1, TILE), f32),
            vm((8, 2, 3, SIG, TILE), f32), vm((8, 2, 3, SIG, TILE), f32), vm((8, 2, 10, 32, TILE), bf),
            vm((8, 2, SIG, TILE), bf), vm((8, 2, SIG, TILE), bf), vm((8, 2, 1, TILE), f32),
            vm((8, 2, SIG, TILE), f32), vm((8, 2, SIG, TILE), f32),
            vm((DEVICES, 1, TILE), f32), vm((1024, 1, TILE), f32),
            dma((11,)), dma, dma, dma, dma, dma, dma,
            dma, dma, pltpu.SemaphoreType.REGULAR, pltpu.SemaphoreType.REGULAR,
        ],
        compiler_params=pltpu.CompilerParams(collective_id=0, has_side_effects=True),
        name="wavelet",
    )(signals, tiles, jnp.swapaxes(tile_dir, 1, 2), jnp.swapaxes(tile_mask, 1, 2), live_rows, bound_rows,
      scale_coeffs, spectral_bound)
    out, energy = pl.pallas_call(
        finish,
        out_shape=(jax.ShapeDtypeStruct((SCALES, NB, SIG, TILE), f32), jax.ShapeDtypeStruct((SCALES, SIG), f32)),
        in_specs=[in_vmem, in_vmem],
        out_specs=(hbm, hbm),
        scratch_shapes=[dma((2,))],
        name="finish",
    )(pltpu.with_memory_space_constraint(tot, pltpu.VMEM), pltpu.with_memory_space_constraint(energy, pltpu.VMEM))
    return out.reshape(SCALES, BX, BY, SIG, TILE), energy


def solution(mesh):
    placed = (
        P("gx", "gy", None, None),
        P("gx", "gy", None, None, None),
        P("gx", "gy", None),
        P("gx", "gy", None),
        P("gx", "gy"),
        P("gx", "gy"),
        P(),
        P(),
    )
    return jax.shard_map(
        shards,
        mesh=mesh,
        in_specs=placed,
        out_specs=(P(None, "gx", "gy", None, None), P()),
        check_vma=False,
    )
```

```python
import functools
import operator

import jax
import jax.numpy as jnp
from jax import lax
from jax.experimental import pallas as pl
from jax.experimental.pallas import tpu as pltpu
from jax.sharding import PartitionSpec as P

MESH = pl.DeviceIdType.MESH
SIG, SCALES, DEG, SLOTS, TILE = 16, 6, 4, 4, 128
BX, BY = 2, 8
NB = BX * BY
GXN, GYN = 32, 4
ZERO = NB + (BX + 2) * (BY + 2)
NR = 24
NX = ZERO + 1
NODES = 64 * 32 * 128
DIRS = [(-1, 0), (1, 0), (0, -1), (0, 1), (-1, -1), (-1, 1), (1, -1), (1, 1)]
OPP = [DIRS.index((-dx, -dy)) for dx, dy in DIRS]


def hops(o):
    ring = (0, 1, 2, 1)
    return ring[o & 3] + ring[o >> 3 & 3] + ring[o >> 5 & 3] + 0.1 * (o >> 2 & 1)


DEVICES = 128
FAR_FIRST = sorted(range(1, DEVICES), key=lambda o: (-hops(o), o))


def kernel(sig_h, til_h, dir_h, msk_h, liv_h, bnd_h, cof_h, spb_h,
           tot, en_ref,
           dir_s, msk_s, liv_s, bnd_s, cof_s, spb_s, sig, til, idx, far, loc, x1, x2, x3, x4, y1, y3, cheb, base, amul, dloc, wr,
           op1, op3, eg, sp1, sp3, tp, oc1, oc3, ec1, sc1, sc3,
           rv1, rv3, re, rs1, rs3, tr, rc1, rc3, rec, rsc1, rsc3, ga, units,
           ld, r1, r2, w1, r3, r4, w3, sa, ra, in_y, in_xy):
    gx, gy = lax.axis_index("gx"), lax.axis_index("gy")
    me = gx * GYN + gy
    early = []
    for n, (src, dst) in enumerate(((sig_h, sig), (liv_h, liv_s), (bnd_h, bnd_s), (dir_h, dir_s), (msk_h, msk_s),
                                    (cof_h, cof_s), (spb_h, spb_s))):
        cp = pltpu.make_async_copy(src, dst, ld.at[n])
        cp.start()
        early.append(cp)

    def exists(d):
        dx, dy = DIRS[d]
        ok = None
        for step, pos, n in ((dx, gx, GXN), (dy, gy, GYN)):
            if step == 0:
                continue
            this = pos > 0 if step < 0 else pos < n - 1
            ok = this if ok is None else jnp.logical_and(ok, this)
        return ok

    have = [exists(d) for d in range(8)]
    peer = [(gx + dx, gy + dy) for dx, dy in DIRS]
    flip = lambda v: (v, v + 1 - 2 * (v % 2), (v + 2) % 4, 3 - v)
    xs, ys, zs = flip(gx // 8), flip(gx // 2 % 4), flip(gy)
    xyc = [8 * u + 2 * v + w for u in xs for v in ys for w in (gx % 2, 1 - gx % 2)]
    other = lambda o: (xyc[(o >> 5) * 8 + (o >> 3) % 4 * 2 + (o >> 2) % 2], zs[o % 4])
    rest = (1, 2, 3, 4, 5, 6, 7)
    ring_y, ring_x = (8, 16, 24), (32, 64, 96)
    bar = pltpu.get_barrier_semaphore()
    for d in (4, 5, 6, 7, 0, 1, 2, 3):
        @pl.when(have[d])
        def _(d=d):
            pl.semaphore_signal(bar, inc=1, device_id=peer[d], device_id_type=MESH)
    for o in ring_x + ring_y + rest:
        pl.semaphore_signal(bar, inc=1, device_id=other(o), device_id_type=MESH)
    count = jnp.int32(13)
    for d in range(8):
        count = count + have[d].astype(jnp.int32)
    til_cp = []
    for n in range(4):
        cp = pltpu.make_async_copy(til_h.at[n // 2, pl.ds(4 * (n % 2), 4)], til.at[pl.ds(4 * n, 4)], ld.at[7 + n])
        cp.start()
        til_cp.append(cp)
    for cp in early:
        cp.wait()

    lane = lax.broadcasted_iota(jnp.int32, (1, TILE), 1)
    low, high, left = lane < 32, lane >= 96, lane < 64
    middle = jnp.logical_and(lane >= 32, lane < 96)
    f = 2.0 / spb_s[0]
    bf16 = lambda a: a.astype(jnp.bfloat16)
    f32 = lambda a: a.astype(jnp.float32)
    for xb in (x1, x2, x3, x4):
        xb[ZERO] = jnp.zeros(xb.shape[1:], xb.dtype)
    for yb in (y1, y3):
        yb[NR] = jnp.zeros(yb.shape[1:], yb.dtype)

    def live_of(b):
        return (lane < liv_s[b // BY, b % BY]).astype(jnp.float32)

    def edge_of(b):
        return (lane < bnd_s[b // BY, b % BY]).astype(jnp.float32)

    def shift(v, q):
        q = q % 4
        return pltpu.roll(v, 32 * q, 1) if q else v

    def add_to(packs, i, j, v, column):
        for key, group in ((("m", i, (j + 2) // 4), j + 2),
                           (("c", 0 if j < BY // 2 else 1), j + 2 + 2 * i)):
            if key[0] == "c" and j not in column:
                continue
            w = shift(v, group)
            packs[key] = w if key not in packs else packs[key] + w

    def flush(packs, main, column, cast, tile_first):
        for key, v in packs.items():
            if key[0] == "c":
                column[key[1]] = cast(v)
            elif tile_first:
                main[key[2], key[1]] = cast(v)
            else:
                main[key[1], key[2]] = cast(v)

    same = lambda v: v
    TWO, ONE = (0, 1, 6, 7), (0, 7)

    RING = [(r, q) for r in (1, 4) for q in range(1, 11)] + [(r, q) for r in (2, 3) for q in (1, 10)]
    slot_of = lambda er, ec: NB + (er - 1) * (BY + 2) + ec - 1

    def place(b, v, xb, packs=None):
        xb[b] = bf16(v)
        e = v * edge_of(b)
        xb[slot_of(b // BY + 2, b % BY + 2)] = bf16(e)
        if packs is not None:
            add_to(packs, b // BY, b % BY, e[:SIG], TWO)

    def part_v(dx, dy):
        return (pl.ds(0, 3),) if dy == 0 else None

    def part_s(dx, dy):
        return ({-1: pl.ds(0, 1), 1: pl.ds(1, 1)}[dx], pl.ds(0, 3)) if dy == 0 else None

    def part_c(dx, dy):
        return (pl.ds((dy + 1) // 2, 1),) if dy != 0 else None

    def part_t(dx, dy):
        return ({-1: pl.ds(0, 1), 1: pl.ds(1, 1), 0: pl.ds(0, 2)}[dx],
                {-1: pl.ds(0, 2), 1: pl.ds(8, 2), 0: pl.ds(0, 10)}[dy])

    def descriptor(src, dst, part, s_sem, r_sem, d, o, at):
        return pltpu.make_async_remote_copy(
            src_ref=src.at[at], dst_ref=dst.at[(o,) + at], send_sem=s_sem, recv_sem=r_sem,
            device_id=peer[d], device_id_type=MESH)

    def send(*messages):
        for d in (4, 5, 6, 7, 0, 1, 2, 3):
            @pl.when(have[d])
            def _(d=d):
                for src, dst, part, s_sem, r_sem in messages:
                    at = part(*DIRS[d])
                    if at is not None:
                        descriptor(src, dst, part, s_sem, r_sem, d, OPP[d], at).start()

    inner_x = jnp.logical_and(gx > 0, gx < GXN - 1)
    inner_y = jnp.logical_and(gy > 0, gy < GYN - 1)

    def wait_all(sent, *messages):
        def size(d):
            n = 0
            for src, _, part, _, _ in messages:
                at = part(*DIRS[d])
                if at is None:
                    continue
                shape = [p.size for p in at] + list(src.shape[len(at):])
                n += src.dtype.itemsize * functools.reduce(operator.mul, shape) // 512
            return n

        _, _, _, s_sem, r_sem = messages[0]
        for nx in (1, 2):
            for ny in (1, 2):
                n = nx * size(0) + ny * size(2) + nx * ny * size(4)
                this = jnp.logical_and(inner_x == (nx == 2), inner_y == (ny == 2))

                @pl.when(this)
                def _(n=n):
                    ref = units.at[pl.ds(0, n)]
                    cp = pltpu.make_async_remote_copy(
                        src_ref=ref, dst_ref=ref, send_sem=s_sem, recv_sem=r_sem,
                        device_id=other(1), device_id_type=MESH)
                    cp.wait_send() if sent else cp.wait_recv()

    first = ((oc1, rc1, part_c, w1, r1), (op1, rv1, part_v, w1, r1), (eg, re, part_v, w1, r1), (ec1, rec, part_c, w1, r1),
             (sp1, rs1, part_s, w1, r2), (sc1, rsc1, part_c, w1, r2), (tp, tr, part_t, w1, r2))
    v3 = ((oc3, rc3, part_c, w3, r3), (op3, rv3, part_v, w3, r3))
    s3 = ((sp3, rs3, part_s, w3, r4), (sc3, rsc3, part_c, w3, r4))
    U, D, L, R, UL, UR, DL, DR = range(8)

    def contract(lhs, rhs):
        return lax.dot_general(lhs, rhs, (((1,), (1,)), ((), ())), preferred_element_type=jnp.float32)

    packs, epacks = {}, {}
    top = lax.broadcasted_iota(jnp.int32, (16, TILE), 0) == 0
    for b in range(NB):
        live = live_of(b)
        v = sig[b // BY, b % BY] * live
        cheb[0, b] = v
        place(b, jnp.concatenate([v, jnp.where(top, live, 0.0)], axis=0), x1, packs)
        add_to(epacks, b // BY, b % BY, edge_of(b), TWO)
    flush(packs, op1, oc1, bf16, True)
    flush(epacks, eg, ec1, same, True)

    def tables(own):
        for b in range(NB):
            i, j = b // BY, b % BY
            for s in range(SLOTS):
                d = dir_s[i, s, j]
                r = (d * 11) >> 5
                q = d - 3 * r
                used = msk_s[i, s, j] == 1
                off = jnp.where(d == 4, b, NB + (i + r) * (BY + 2) + (j + q))
                ring = 10 * i + j + q
                away = r == 2 * i
                if j in (0, BY - 1):
                    beyond = q == (0 if j == 0 else 2)
                    ring = jnp.where(away, ring, 20 + 2 * (i + r - 1) + (0 if j == 0 else 1))
                    away = jnp.logical_or(away, beyond)
                if own:
                    loc[b * SLOTS + s] = jnp.where(jnp.logical_and(used, jnp.logical_not(away)), off, ZERO)
                else:
                    idx[b * SLOTS + s] = jnp.where(used, off, ZERO)
                    far[b * SLOTS + s] = jnp.where(jnp.logical_and(used, away), ring, NR)

    tables(True)

    def sorted_rows(b, wanted):
        i, j = b // BY, b % BY
        total = None
        tiles = [f32(til[b, s, pl.ds(0, 32)]) for s in range(SLOTS)]
        for d, group in wanted:
            acc = None
            for s in range(SLOTS):
                on = jnp.logical_and(dir_s[i, s, j] == d, msk_s[i, s, j] == 1).astype(jnp.float32)
                t = tiles[s] * on
                acc = t if acc is None else acc + t
            acc = shift(jnp.where(low, acc, 0.0), group)
            total = acc if total is None else total + acc
        inside = lax.broadcasted_iota(jnp.int32, (32, TILE), 0) < bnd_s[i, j]
        return bf16(jnp.where(inside, total, 0.0))

    def directions(b):
        i, j = b // BY, b % BY
        yield None, [(6 * i + q, j + 1 + q) for q in range(3)]
        if j == 0:
            yield 0, [(3 - 3 * i, 1), (6 - 3 * i, 0)]
        if j == BY - 1:
            yield 1, [(5 - 3 * i, 2), (8 - 3 * i, 3)]

    def product(b, xb, table, rows=TILE):
        acc = None
        for h in range(2):
            pick = [xb[table[b * SLOTS + 2 * h + n]] for n in range(2)]
            rhs = [til[b, 2 * h + n, :rows] for n in range(2)]
            p = contract(jnp.concatenate(pick, axis=1), jnp.concatenate(rhs, axis=1))
            acc = p if acc is None else acc + p
        return acc

    def own_part(k, xb):
        for b in range(NB):
            acc = product(b, xb, loc)
            fl = f * live_of(b)
            if k == 0:
                deg = fl * acc[SIG:SIG + 1]
                dloc[b] = jnp.broadcast_to(deg, (8, TILE))
                base[b] = (deg - 1.0) * cheb[0, b] - fl * acc[:SIG]
            else:
                am = amul[b]
                am = jnp.concatenate([am, am], axis=0)
                base[b] = am * cheb[k, b] - (2.0 * fl) * acc - cheb[k - 1, b]

    def far_product(b, yb):
        parts = [yb[far[b * SLOTS + s], s] for s in range(SLOTS)]
        return contract((parts[0] + parts[1]) + (parts[2] + parts[3]), wr[b])

    def local_part(k, xb, sp, sc):
        packs = {}
        for b in range(NB):
            acc = product(b, xb, loc, 32)
            v = cheb[k, b, :, :32]
            if k == 0:
                out = (f * acc[SIG:SIG + 1] - 1.0) * v - f * acc[:SIG]
            else:
                out = amul[b, :1, :32] * v - (2.0 * f) * acc - cheb[k - 1, b, :, :32]
            out = out * edge_of(b)[:, :32]
            add_to(packs, b // BY, b % BY,
                   jnp.concatenate([out, jnp.zeros((SIG, TILE - 32), jnp.float32)], axis=1), ONE)
        flush(packs, sp, sc, same if k == 0 else bf16, False)

    for cp in til_cp:
        cp.wait()
    for b in range(NB):
        for side, wanted in directions(b):
            tp[b // BY, 1 + b % BY if side is None else 9 * side] = sorted_rows(b, wanted)
    local_part(0, x1, sp1, sc1)
    pl.semaphore_wait(bar, count)
    for message in first:
        send(message)
    for o in ring_x:
        pl.semaphore_signal(in_y, inc=1, device_id=other(o), device_id_type=MESH)

    for d in range(8):
        @pl.when(jnp.logical_not(have[d]))
        def _(d=d):
            for buf in (rv1, rv3, re, rs1, rs3, tr, rc1, rc3, rec, rsc1, rsc3):
                buf[d] = jnp.zeros(buf.shape[1:], buf.dtype)

    def add_totals(k):
        for s in range(SCALES):
            a = cof_s[s, k] * 0.5 if k == 0 else cof_s[s, k]
            for b in range(NB):
                t = a * cheb[k, b]
                tot[s, b] = t if k == 0 else tot[s, b] + t

    def beside(rc, i, o):
        side = 1 if o in (L, UL, DL) else 0
        return shift(f32(rc[o, side]), 2 * i)

    def rows_of(op, rv, rc):
        rows = []
        for r in range(6):
            i = r % 2
            if r in (2, 3):
                ul, ur, mine = L, R, [op[t, i] for t in range(3)]
            else:
                u, ul, ur = (U, UL, UR) if r < 2 else (D, DL, DR)
                mine = [rv[u, t, i] for t in range(3)]
            mine = [f32(v) for v in mine]
            rows.append([jnp.where(left, beside(rc, i, ul), mine[0]), mine[1],
                         jnp.where(left, mine[2], beside(rc, i, ur))])
        return rows

    def with_edges(rows, edges):
        return [[jnp.concatenate([v, jnp.where(top, e, 0.0)], axis=0) for v, e in zip(r, q)]
                for r, q in zip(rows, edges)]

    class Inputs:
        def __init__(self, rows):
            self.rows, self.made = rows, {}

        def get(self, key, make):
            if key not in self.made:
                self.made[key] = bf16(make())
            return self.made[key]

        def plain(self, r, t):
            return self.get(("p", r, t), lambda: self.rows[r][t])

        def row(self, r, c):
            t, q, rows = c // 4, c % 4, self.rows[r]
            if q == 0:
                return self.get(("a", r, t), lambda: jnp.where(high, rows[t - 1], rows[t]))
            if q == 3:
                return self.get(("b", r, t), lambda: jnp.where(low, rows[t + 1], rows[t]))
            return self.plain(r, t)

        def crossing(self, r, t):
            rows = self.rows[r]
            before = rows[t - 1] if t > 0 else jnp.zeros_like(rows[t])
            after = rows[t + 1] if t < 2 else jnp.zeros_like(rows[t])
            return self.get(("x", r, t), lambda: jnp.where(left, after, before))

        def column(self, r, t):
            one, two = self.rows[r][t], self.rows[r + 1][t]
            return self.get(("c", r, t), lambda: jnp.where(
                middle, one, jnp.where(left, shift(two, -1), shift(two, 1))))

    groups = [jnp.logical_and(lane >= 32 * s, lane < 32 * s + 32) for s in range(SLOTS)]

    groups = [jnp.logical_and(lane >= 32 * s, lane < 32 * s + 32) for s in range(SLOTS)]

    def unpack(rows, xb):
        for er, ec in RING:
            v = jnp.where(low, shift(rows[er][ec // 4], -ec), 0.0)
            xb[slot_of(er, ec)] = bf16(v)

    def unpack_far(rows, yb, columns):
        made = {}
        for n, (er, ec) in enumerate(RING):
            group = ec
            if ec in (1, 10):
                o = {1: {1: UL, 10: UR}, 2: {1: L, 10: R}, 3: {1: L, 10: R}, 4: {1: DL, 10: DR}}[er][ec]
                key, group = o, ec + 2 * (er % 2)
                made[key] = columns(o) if key not in made else made[key]
            else:
                key = (er, ec // 4)
                made[key] = bf16(rows[er][ec // 4]) if key not in made else made[key]
            for s in range(SLOTS):
                yb[n, s] = jnp.where(groups[s], shift(made[key], s - group), jnp.bfloat16(0))

    r_iota = lax.broadcasted_iota(jnp.int32, (TILE, TILE), 0)
    c_iota = lax.broadcasted_iota(jnp.int32, (TILE, TILE), 1)
    across = jnp.logical_or(jnp.logical_and(r_iota < 32, c_iota >= 96), jnp.logical_and(r_iota >= 96, c_iota < 32))

    def advance_ring(rows, rs, rsc, first):
        ins = Inputs(rows)
        none = jnp.zeros((32, TILE), jnp.bfloat16)
        zero = jnp.zeros((TILE, TILE), jnp.float32)

        def update(own, lhs, rhs, v):
            acc = contract(jnp.concatenate(lhs, axis=1), jnp.concatenate(rhs, axis=1))
            if first:
                return own + f * (acc[SIG:SIG + 1] * v[:SIG] - acc[:SIG])
            return own - (2.0 * f) * acc

        new = [[None] * 3 for _ in range(6)]
        for er, u, ul, ur in ((1, U, UL, UR), (4, D, DL, DR)):
            i = 1 if er == 1 else 0
            feed = er + 1 if i else er - 1
            edge = er - i
            for t in range(3):
                if t == 1:
                    w = [tr[u, i, 3 + n] for n in range(4)]
                    own, wq = f32(rs[u, i, 1]), None
                elif t == 0:
                    w = [none, tr[ul, i, 8], tr[u, i, 1], tr[u, i, 2]]
                    wq = [none, tr[ul, i, 9], tr[u, i, 0], none]
                    own = jnp.where(left, beside(rsc, i, ul), f32(rs[u, i, 0]))
                else:
                    w = [tr[u, i, 7], tr[u, i, 8], tr[ur, i, 1], none]
                    wq = [none, tr[u, i, 9], tr[ur, i, 0], none]
                    own = jnp.where(left, f32(rs[u, i, 2]), beside(rsc, i, ur))
                w = f32(jnp.concatenate(w, axis=0))
                lhs = [ins.plain(feed, t), ins.crossing(feed, t)]
                rhs = [bf16(jnp.where(across, zero, w)), bf16(jnp.where(across, w, zero))]
                if wq is not None:
                    lhs.append(ins.column(edge, t))
                    rhs.append(jnp.concatenate(wq, axis=0))
                new[er][t] = update(own, lhs, rhs, rows[er][t])
        for er, i in ((2, 0), (3, 1)):
            feed = er - 1 if i == 0 else er + 1
            for t, o, p, q in ((0, L, 8, 9), (2, R, 1, 0)):
                at = 1 if t == 0 else 2
                pad = lambda w: jnp.concatenate([none] * at + [w] + [none] * (3 - at), axis=0)
                new[er][t] = update(beside(rsc, i, o), [ins.plain(feed, t), ins.column(2, t)],
                                    [pad(tr[o, i, p]), pad(tr[o, i, q])], rows[er][t])
        return new

    tables(False)
    add_totals(0)
    for b in range(NB):
        packed = [shift(jnp.where(low, f32(til[b, s]), 0.0), s) for s in range(SLOTS)]
        wr[b] = bf16((packed[0] + packed[1]) + (packed[2] + packed[3]))
    own_part(0, x1)
    pl.semaphore_wait(in_y, 3)
    for o in rest:
        pl.semaphore_signal(in_xy, inc=1, device_id=other(o), device_id_type=MESH)

    wait_all(False, *first[:4])
    rows = with_edges(rows_of(op1, rv1, rc1), rows_of(eg, re, rec))

    def column1(o):
        side = 1 if o in (L, UL, DL) else 0
        return jnp.concatenate([rc1[o, side], bf16(jnp.where(top, rec[o, side], 0.0))], axis=0)

    unpack_far(rows, y1, column1)
    for b in range(NB):
        acc = far_product(b, y1)
        fl = f * live_of(b)
        deg = fl * acc[SIG:SIG + 1]
        amul[b] = 2.0 * (dloc[b] + jnp.broadcast_to(deg, (8, TILE)) - 1.0)
        cur = base[b] + deg * cheb[0, b] - fl * acc[:SIG]
        cheb[1, b] = cur
        place(b, cur, x2)
    wait_all(False, *first[4:])
    unpack(advance_ring(rows, rs1, rsc1, 1), x2)

    def step(b, k, xb):
        acc = product(b, xb, idx)
        am = amul[b]
        am = jnp.concatenate([am, am], axis=0)
        return am * cheb[k, b] - (2.0 * f * live_of(b)) * acc - cheb[k - 1, b]

    packs = {}
    for b in range(NB):
        cur = step(b, 1, x2)
        cheb[2, b] = cur
        place(b, cur, x3, packs)
    flush(packs, op3, oc3, bf16, True)
    for message in v3:
        send(message)
    local_part(2, x3, sp3, sc3)
    for message in s3:
        send(message)
    own_part(2, x3)
    add_totals(1)
    add_totals(2)
    wait_all(True, *first)

    wait_all(False, *v3)
    rows = rows_of(op3, rv3, rc3)
    unpack_far(rows, y3, lambda o: rc3[o, 1 if o in (L, UL, DL) else 0])
    for b in range(NB):
        cur = base[b] - (2.0 * f * live_of(b)) * far_product(b, y3)
        cheb[3, b] = cur
        place(b, cur, x4)
    add_totals(3)
    wait_all(False, *s3)
    unpack(advance_ring(rows, rs3, rsc3, 0), x4)
    sq = [None] * SCALES
    for b in range(NB):
        cur = step(b, 3, x4)
        for s in range(SCALES):
            t = tot[s, b] + cof_s[s, 4] * cur
            tot[s, b] = t
            sq[s] = t * t if sq[s] is None else sq[s] + t * t

    m = jnp.concatenate(sq, axis=0)
    hi = m.astype(jnp.bfloat16)
    r1 = m - hi.astype(jnp.float32)
    mid = r1.astype(jnp.bfloat16)
    lo = (r1 - mid.astype(jnp.float32)).astype(jnp.bfloat16)
    ones = jnp.ones((16, TILE), jnp.bfloat16)
    row = None
    for part in (lo, mid, hi):
        p = lax.dot_general(ones, part, (((1,), (1,)), ((), ())), preferred_element_type=jnp.float32)
        row = p if row is None else row + p
    row = jnp.concatenate([row[0:1], jnp.zeros((1, TILE - SCALES * SIG), jnp.float32)], axis=1)

    ga[me] = row
    pl.semaphore_wait(in_xy, 7)
    for o in FAR_FIRST:
        pltpu.make_async_remote_copy(
            src_ref=ga.at[me], dst_ref=ga.at[me], send_sem=sa, recv_sem=ra,
            device_id=other(o), device_id_type=MESH).start()
    wait_all(True, *v3, *s3)
    many = ga.at[pl.ds(0, DEVICES - 1)]
    pltpu.make_async_remote_copy(
        src_ref=many, dst_ref=many, send_sem=sa, recv_sem=ra, device_id=other(1), device_id_type=MESH).wait_recv()
    sums = [ga[q] for q in range(DEVICES)]
    while len(sums) > 1:
        sums = [u + v for u, v in zip(sums[::2], sums[1::2])]
    full = sums[0] * (1.0 / NODES)
    res = jnp.zeros((8, TILE), jnp.float32)
    sub = lax.broadcasted_iota(jnp.int32, (8, TILE), 0)
    full8 = jnp.broadcast_to(full, (8, TILE))
    for s in range(SCALES):
        v = pltpu.roll(full8, TILE - 16 * s, 1) if s else full8
        res = jnp.where(sub == s, v, res)
    en_ref[...] = res[:SCALES, :SIG]

    pltpu.make_async_remote_copy(
        src_ref=many, dst_ref=many, send_sem=sa, recv_sem=ra, device_id=other(1), device_id_type=MESH).wait_send()


def finish(tot, en, out_h, en_h, sem):
    a = pltpu.make_async_copy(tot, out_h, sem.at[0])
    b = pltpu.make_async_copy(en, en_h, sem.at[1])
    a.start()
    b.start()
    a.wait()
    b.wait()


def shards(signals, tiles, tile_dir, tile_mask, live_rows, bound_rows, scale_coeffs, spectral_bound):
    bf, f32, i32 = jnp.bfloat16, jnp.float32, jnp.int32
    vm, sm = pltpu.VMEM, pltpu.SMEM
    in_vmem = pl.BlockSpec(memory_space=pltpu.VMEM)
    hbm = pl.BlockSpec(memory_space=pl.ANY)
    dma = pltpu.SemaphoreType.DMA
    tot, energy = pl.pallas_call(
        kernel,
        out_shape=(pltpu.VMEM((SCALES, NB, SIG, TILE), f32), pltpu.VMEM((SCALES, SIG), f32)),
        in_specs=[hbm] * 7 + [pl.BlockSpec(memory_space=pltpu.HBM)],
        out_specs=(in_vmem, in_vmem),
        scratch_shapes=[
            sm((BX, SLOTS, BY), i32), sm((BX, SLOTS, BY), i32), sm((BX, BY), i32), sm((BX, BY), i32),
            sm((SCALES, DEG + 1), f32), sm((1,), f32),
            vm((BX, BY, SIG, TILE), f32), vm((NB, SLOTS, TILE, TILE), bf),
            sm((NB * SLOTS,), i32), sm((NB * SLOTS,), i32), sm((NB * SLOTS,), i32),
            vm((NX, 32, TILE), bf), vm((NX, SIG, TILE), bf), vm((NX, SIG, TILE), bf), vm((NX, SIG, TILE), bf),
            vm((NR + 1, SLOTS, 32, TILE), bf), vm((NR + 1, SLOTS, SIG, TILE), bf),
            vm((DEG, NB, SIG, TILE), f32), vm((NB, SIG, TILE), f32), vm((NB, 8, TILE), f32), vm((NB, 8, TILE), f32),
            vm((NB, TILE, TILE), bf),
            vm((3, 2, SIG, TILE), bf), vm((3, 2, SIG, TILE), bf), vm((3, 2, 1, TILE), f32),
            vm((2, 3, SIG, TILE), f32), vm((2, 3, SIG, TILE), bf), vm((2, 10, 32, TILE), bf),
            vm((2, SIG, TILE), bf), vm((2, SIG, TILE), bf), vm((2, 1, TILE), f32), vm((2, SIG, TILE), f32), vm((2, SIG, TILE), bf),
            vm((8, 3, 2, SIG, TILE), bf), vm((8, 3, 2, SIG, TILE), bf), vm((8, 3, 2, 1, TILE), f32),
            vm((8, 2, 3, SIG, TILE), f32), vm((8, 2, 3, SIG, TILE), bf), vm((8, 2, 10, 32, TILE), bf),
            vm((8, 2, SIG, TILE), bf), vm((8, 2, SIG, TILE), bf), vm((8, 2, 1, TILE), f32),
            vm((8, 2, SIG, TILE), f32), vm((8, 2, SIG, TILE), bf),
            vm((DEVICES, 1, TILE), f32), vm((1024, 1, TILE), f32),
            dma((11,)), dma, dma, dma, dma, dma, dma,
            dma, dma, pltpu.SemaphoreType.REGULAR, pltpu.SemaphoreType.REGULAR,
        ],
        compiler_params=pltpu.CompilerParams(collective_id=0, has_side_effects=True),
        name="wavelet",
    )(signals, tiles, jnp.swapaxes(tile_dir, 1, 2), jnp.swapaxes(tile_mask, 1, 2), live_rows, bound_rows,
      scale_coeffs, spectral_bound)
    out, energy = pl.pallas_call(
        finish,
        out_shape=(jax.ShapeDtypeStruct((SCALES, NB, SIG, TILE), f32), jax.ShapeDtypeStruct((SCALES, SIG), f32)),
        in_specs=[in_vmem, in_vmem],
        out_specs=(hbm, hbm),
        scratch_shapes=[dma((2,))],
        name="finish",
    )(pltpu.with_memory_space_constraint(tot, pltpu.VMEM), pltpu.with_memory_space_constraint(energy, pltpu.VMEM))
    return out.reshape(SCALES, BX, BY, SIG, TILE), energy


def solution(mesh):
    placed = (
        P("gx", "gy", None, None),
        P("gx", "gy", None, None, None),
        P("gx", "gy", None),
        P("gx", "gy", None),
        P("gx", "gy"),
        P("gx", "gy"),
        P(),
        P(),
    )
    return jax.shard_map(
        shards,
        mesh=mesh,
        in_specs=placed,
        out_specs=(P(None, "gx", "gy", None, None), P()),
        check_vma=False,
    )
```

```python
import functools
import operator

import jax
import jax.numpy as jnp
from jax import lax
from jax.experimental import pallas as pl
from jax.experimental.pallas import tpu as pltpu
from jax.sharding import PartitionSpec as P

MESH = pl.DeviceIdType.MESH
SIG, SCALES, DEG, SLOTS, TILE = 16, 6, 4, 4, 128
BX, BY = 2, 8
NB = BX * BY
GXN, GYN = 32, 4
ZERO = NB + (BX + 2) * (BY + 2)
NR = 24
NX = ZERO + 1
NODES = 64 * 32 * 128
DIRS = [(-1, 0), (1, 0), (0, -1), (0, 1), (-1, -1), (-1, 1), (1, -1), (1, 1)]
OPP = [DIRS.index((-dx, -dy)) for dx, dy in DIRS]


def hops(o):
    ring = (0, 1, 2, 1)
    return ring[o & 3] + ring[o >> 3 & 3] + ring[o >> 5 & 3] + 0.1 * (o >> 2 & 1)


DEVICES = 128
FAR_FIRST = sorted(range(1, DEVICES), key=lambda o: (-hops(o), o))


def kernel(sig_h, til_h, dir_h, msk_h, liv_h, bnd_h, cof_h, spb_h,
           tot, en_ref,
           dir_s, msk_s, liv_s, bnd_s, cof_s, spb_s, sig, til, idx, far, loc, x1, x2, x3, x4, y1, y3, cheb, base, amul, dloc, wr,
           op1, op3, eg, sp1, sp3, tp, oc1, oc3, ec1, sc1, sc3,
           rv1, rv3, re, rs1, rs3, tr, rc1, rc3, rec, rsc1, rsc3, ga, units,
           ld, r1, r2, w1, r3, r4, w3, sa, ra, in_y, in_xy):
    gx, gy = lax.axis_index("gx"), lax.axis_index("gy")
    me = gx * GYN + gy
    early = []
    for n, (src, dst) in enumerate(((sig_h, sig), (liv_h, liv_s), (bnd_h, bnd_s), (dir_h, dir_s), (msk_h, msk_s),
                                    (cof_h, cof_s), (spb_h, spb_s))):
        cp = pltpu.make_async_copy(src, dst, ld.at[n])
        cp.start()
        early.append(cp)

    def exists(d):
        dx, dy = DIRS[d]
        ok = None
        for step, pos, n in ((dx, gx, GXN), (dy, gy, GYN)):
            if step == 0:
                continue
            this = pos > 0 if step < 0 else pos < n - 1
            ok = this if ok is None else jnp.logical_and(ok, this)
        return ok

    have = [exists(d) for d in range(8)]
    peer = [(gx + dx, gy + dy) for dx, dy in DIRS]
    flip = lambda v: (v, v + 1 - 2 * (v % 2), (v + 2) % 4, 3 - v)
    xs, ys, zs = flip(gx // 8), flip(gx // 2 % 4), flip(gy)
    xyc = [8 * u + 2 * v + w for u in xs for v in ys for w in (gx % 2, 1 - gx % 2)]
    other = lambda o: (xyc[(o >> 5) * 8 + (o >> 3) % 4 * 2 + (o >> 2) % 2], zs[o % 4])
    rest = (1, 2, 3, 4, 5, 6, 7)
    ring_y, ring_x = (8, 16, 24), (32, 64, 96)
    bar = pltpu.get_barrier_semaphore()
    for d in (4, 5, 6, 7, 0, 1, 2, 3):
        @pl.when(have[d])
        def _(d=d):
            pl.semaphore_signal(bar, inc=1, device_id=peer[d], device_id_type=MESH)
    for o in ring_x + ring_y + rest:
        pl.semaphore_signal(bar, inc=1, device_id=other(o), device_id_type=MESH)
    count = jnp.int32(13)
    for d in range(8):
        count = count + have[d].astype(jnp.int32)
    til_cp = []
    for n in range(4):
        cp = pltpu.make_async_copy(til_h.at[n // 2, pl.ds(4 * (n % 2), 4)], til.at[pl.ds(4 * n, 4)], ld.at[7 + n])
        cp.start()
        til_cp.append(cp)
    for cp in early:
        cp.wait()

    lane = lax.broadcasted_iota(jnp.int32, (1, TILE), 1)
    low, high, left = lane < 32, lane >= 96, lane < 64
    middle = jnp.logical_and(lane >= 32, lane < 96)
    f = 2.0 / spb_s[0]
    bf16 = lambda a: a.astype(jnp.bfloat16)
    f32 = lambda a: a.astype(jnp.float32)
    for xb in (x1, x2, x3, x4):
        xb[ZERO] = jnp.zeros(xb.shape[1:], xb.dtype)
    for yb in (y1, y3):
        yb[NR] = jnp.zeros(yb.shape[1:], yb.dtype)

    def live_of(b):
        return (lane < liv_s[b // BY, b % BY]).astype(jnp.float32)

    def edge_of(b):
        return (lane < bnd_s[b // BY, b % BY]).astype(jnp.float32)

    def shift(v, q):
        q = q % 4
        return pltpu.roll(v, 32 * q, 1) if q else v

    def add_to(packs, i, j, v, column):
        for key, group in ((("m", i, j // 4), j),
                           (("c", 0 if j < BY // 2 else 1), j + 2 * i)):
            if key[0] == "c" and j not in column:
                continue
            w = shift(v, group)
            packs[key] = w if key not in packs else packs[key] + w

    def flush(packs, main, column, cast, tile_first):
        for key, v in packs.items():
            if key[0] == "c":
                column[key[1]] = cast(v)
            elif tile_first:
                main[key[2], key[1]] = cast(v)
            else:
                main[key[1], key[2]] = cast(v)

    same = lambda v: v
    TWO, ONE = (0, 1, 6, 7), (0, 7)

    RING = [(r, q) for r in (1, 4) for q in range(3, 13)] + [(r, q) for r in (2, 3) for q in (3, 12)]
    slot_of = lambda er, ec: NB + (er - 1) * (BY + 2) + ec - 3

    def place(b, v, xb, packs=None):
        xb[b] = bf16(v)
        e = v * edge_of(b)
        xb[slot_of(b // BY + 2, b % BY + 4)] = bf16(e)
        if packs is not None:
            add_to(packs, b // BY, b % BY, e[:SIG], TWO)

    def part_v(dx, dy):
        return (pl.ds(0, 2),) if dy == 0 else None

    def part_s(dx, dy):
        return ({-1: pl.ds(0, 1), 1: pl.ds(1, 1)}[dx], pl.ds(0, 2)) if dy == 0 else None

    def part_c(dx, dy):
        return (pl.ds((dy + 1) // 2, 1),) if dy != 0 else None

    def part_t(dx, dy):
        return ({-1: pl.ds(0, 1), 1: pl.ds(1, 1), 0: pl.ds(0, 2)}[dx],
                {-1: pl.ds(0, 2), 1: pl.ds(8, 2), 0: pl.ds(0, 9)}[dy])

    def descriptor(src, dst, part, s_sem, r_sem, d, o, at):
        return pltpu.make_async_remote_copy(
            src_ref=src.at[at], dst_ref=dst.at[(o,) + at], send_sem=s_sem, recv_sem=r_sem,
            device_id=peer[d], device_id_type=MESH)

    def send(*messages):
        for d in (4, 5, 6, 7, 0, 1, 2, 3):
            @pl.when(have[d])
            def _(d=d):
                for src, dst, part, s_sem, r_sem in messages:
                    at = part(*DIRS[d])
                    if at is not None:
                        descriptor(src, dst, part, s_sem, r_sem, d, OPP[d], at).start()

    inner_x = jnp.logical_and(gx > 0, gx < GXN - 1)
    inner_y = jnp.logical_and(gy > 0, gy < GYN - 1)

    def wait_all(sent, *messages):
        def size(d):
            n = 0
            for src, _, part, _, _ in messages:
                at = part(*DIRS[d])
                if at is None:
                    continue
                shape = [p.size for p in at] + list(src.shape[len(at):])
                n += src.dtype.itemsize * functools.reduce(operator.mul, shape) // 512
            return n

        _, _, _, s_sem, r_sem = messages[0]
        for nx in (1, 2):
            for ny in (1, 2):
                n = nx * size(0) + ny * size(2) + nx * ny * size(4)
                this = jnp.logical_and(inner_x == (nx == 2), inner_y == (ny == 2))

                @pl.when(this)
                def _(n=n):
                    ref = units.at[pl.ds(0, n)]
                    cp = pltpu.make_async_remote_copy(
                        src_ref=ref, dst_ref=ref, send_sem=s_sem, recv_sem=r_sem,
                        device_id=other(1), device_id_type=MESH)
                    cp.wait_send() if sent else cp.wait_recv()

    first = ((oc1, rc1, part_c, w1, r1), (op1, rv1, part_v, w1, r1), (eg, re, part_v, w1, r1), (ec1, rec, part_c, w1, r1),
             (sp1, rs1, part_s, w1, r2), (sc1, rsc1, part_c, w1, r2), (tp, tr, part_t, w1, r2))
    v3 = ((oc3, rc3, part_c, w3, r3), (op3, rv3, part_v, w3, r3))
    s3 = ((sp3, rs3, part_s, w3, r4), (sc3, rsc3, part_c, w3, r4))
    U, D, L, R, UL, UR, DL, DR = range(8)

    def contract(lhs, rhs):
        return lax.dot_general(lhs, rhs, (((1,), (1,)), ((), ())), preferred_element_type=jnp.float32)

    packs, epacks = {}, {}
    top = lax.broadcasted_iota(jnp.int32, (16, TILE), 0) == 0
    for b in range(NB):
        live = live_of(b)
        v = sig[b // BY, b % BY] * live
        cheb[0, b] = v
        place(b, jnp.concatenate([v, jnp.where(top, live, 0.0)], axis=0), x1, packs)
        add_to(epacks, b // BY, b % BY, edge_of(b), TWO)
    flush(packs, op1, oc1, bf16, True)
    flush(epacks, eg, ec1, same, True)

    def tables(own):
        for b in range(NB):
            i, j = b // BY, b % BY
            for s in range(SLOTS):
                d = dir_s[i, s, j]
                r = (d * 11) >> 5
                q = d - 3 * r
                used = msk_s[i, s, j] == 1
                off = jnp.where(d == 4, b, NB + (i + r) * (BY + 2) + (j + q))
                ring = 10 * i + j + q
                away = r == 2 * i
                if j in (0, BY - 1):
                    beyond = q == (0 if j == 0 else 2)
                    ring = jnp.where(away, ring, 20 + 2 * (i + r - 1) + (0 if j == 0 else 1))
                    away = jnp.logical_or(away, beyond)
                if own:
                    loc[b * SLOTS + s] = jnp.where(jnp.logical_and(used, jnp.logical_not(away)), off, ZERO)
                else:
                    idx[b * SLOTS + s] = jnp.where(used, off, ZERO)
                    far[b * SLOTS + s] = jnp.where(jnp.logical_and(used, away), ring, NR)

    tables(True)

    def sorted_rows(b, wanted):
        i, j = b // BY, b % BY
        total = None
        tiles = [f32(til[b, s, pl.ds(0, 32)]) for s in range(SLOTS)]
        for d, group in wanted:
            acc = None
            for s in range(SLOTS):
                on = jnp.logical_and(dir_s[i, s, j] == d, msk_s[i, s, j] == 1).astype(jnp.float32)
                t = tiles[s] * on
                acc = t if acc is None else acc + t
            acc = shift(jnp.where(low, acc, 0.0), group)
            total = acc if total is None else total + acc
        inside = lax.broadcasted_iota(jnp.int32, (32, TILE), 0) < bnd_s[i, j]
        return bf16(jnp.where(inside, total, 0.0))

    def directions(b):
        i, j = b // BY, b % BY
        yield None, [(6 * i + q, j + q - 1) for q in range(3)]
        if j == 0:
            yield 0, [(3 - 3 * i, 3), (6 - 3 * i, 2)]
        if j == BY - 1:
            yield 1, [(5 - 3 * i, 0), (8 - 3 * i, 1)]

    def product(b, xb, table, rows=TILE):
        acc = None
        for h in range(2):
            pick = [xb[table[b * SLOTS + 2 * h + n]] for n in range(2)]
            rhs = [til[b, 2 * h + n, :rows] for n in range(2)]
            p = contract(jnp.concatenate(pick, axis=1), jnp.concatenate(rhs, axis=1))
            acc = p if acc is None else acc + p
        return acc

    def own_part(k, xb):
        for b in range(NB):
            acc = product(b, xb, loc)
            fl = f * live_of(b)
            if k == 0:
                deg = fl * acc[SIG:SIG + 1]
                dloc[b] = jnp.broadcast_to(deg, (8, TILE))
                base[b] = (deg - 1.0) * cheb[0, b] - fl * acc[:SIG]
            else:
                am = amul[b]
                am = jnp.concatenate([am, am], axis=0)
                base[b] = am * cheb[k, b] - (2.0 * fl) * acc - cheb[k - 1, b]

    def far_product(b, yb):
        parts = [yb[far[b * SLOTS + s], s] for s in range(SLOTS)]
        return contract((parts[0] + parts[1]) + (parts[2] + parts[3]), wr[b])

    def local_part(k, xb, sp, sc):
        packs = {}
        for b in range(NB):
            acc = product(b, xb, loc, 32)
            v = cheb[k, b, :, :32]
            if k == 0:
                out = (f * acc[SIG:SIG + 1] - 1.0) * v - f * acc[:SIG]
            else:
                out = amul[b, :1, :32] * v - (2.0 * f) * acc - cheb[k - 1, b, :, :32]
            out = out * edge_of(b)[:, :32]
            add_to(packs, b // BY, b % BY,
                   jnp.concatenate([out, jnp.zeros((SIG, TILE - 32), jnp.float32)], axis=1), ONE)
        flush(packs, sp, sc, same if k == 0 else bf16, False)

    for cp in til_cp:
        cp.wait()
    ends = {}
    for b in range(NB):
        for side, wanted in directions(b):
            rows = sorted_rows(b, wanted)
            if side is None:
                tp[b // BY, 1 + b % BY] = rows
            else:
                ends[b // BY, side] = rows
    for i in range(BX):
        both = ends[i, 0] + ends[i, 1]
        tp[i, 0] = both
        tp[i, 9] = both
    local_part(0, x1, sp1, sc1)
    pl.semaphore_wait(bar, count)
    for message in first:
        send(message)
    for o in ring_x:
        pl.semaphore_signal(in_y, inc=1, device_id=other(o), device_id_type=MESH)

    for d in range(8):
        @pl.when(jnp.logical_not(have[d]))
        def _(d=d):
            for buf in (rv1, rv3, re, rs1, rs3, tr, rc1, rc3, rec, rsc1, rsc3):
                buf[d] = jnp.zeros(buf.shape[1:], buf.dtype)

    def add_totals(k):
        for s in range(SCALES):
            a = cof_s[s, k] * 0.5 if k == 0 else cof_s[s, k]
            for b in range(NB):
                t = a * cheb[k, b]
                tot[s, b] = t if k == 0 else tot[s, b] + t

    def beside(rc, i, o):
        side = 1 if o in (L, UL, DL) else 0
        return shift(f32(rc[o, side]), 2 * i)

    def rows_of(op, rv, rc):
        rows = []
        for r in range(6):
            i = r % 2
            if r in (2, 3):
                ul, ur, mine = L, R, [op[t, i] for t in range(2)]
            else:
                u, ul, ur = (U, UL, UR) if r < 2 else (D, DL, DR)
                mine = [rv[u, t, i] for t in range(2)]
            rows.append([beside(rc, i, ul), f32(mine[0]), f32(mine[1]), beside(rc, i, ur)])
        return rows

    def with_edges(rows, edges):
        return [[jnp.concatenate([v, jnp.where(top, e, 0.0)], axis=0) for v, e in zip(r, q)]
                for r, q in zip(rows, edges)]

    class Inputs:
        def __init__(self, rows):
            self.rows, self.made = rows, {}

        def get(self, key, make):
            if key not in self.made:
                self.made[key] = bf16(make())
            return self.made[key]

        def plain(self, r, t):
            return self.get(("p", r, t), lambda: self.rows[r][t])

        def row(self, r, c):
            t, q, rows = c // 4, c % 4, self.rows[r]
            if q == 0:
                return self.get(("a", r, t), lambda: jnp.where(high, rows[t - 1], rows[t]))
            if q == 3:
                return self.get(("b", r, t), lambda: jnp.where(low, rows[t + 1], rows[t]))
            return self.plain(r, t)

        def crossing(self, r, t):
            rows = self.rows[r]
            before = rows[t - 1] if t > 0 else jnp.zeros_like(rows[t])
            after = rows[t + 1] if t < 3 else jnp.zeros_like(rows[t])
            return self.get(("x", r, t), lambda: jnp.where(left, after, before))

        def column(self, r, t):
            one, two = self.rows[r][t], self.rows[r + 1][t]
            return self.get(("c", r, t), lambda: jnp.where(
                middle, jnp.where(left, shift(two, 1), shift(two, -1)), one))

    groups = [jnp.logical_and(lane >= 32 * s, lane < 32 * s + 32) for s in range(SLOTS)]

    groups = [jnp.logical_and(lane >= 32 * s, lane < 32 * s + 32) for s in range(SLOTS)]

    def unpack(rows, xb):
        for er, ec in RING:
            v = jnp.where(low, shift(rows[er][ec // 4], -ec), 0.0)
            xb[slot_of(er, ec)] = bf16(v)

    def unpack_far(rows, yb, columns):
        made = {}
        for n, (er, ec) in enumerate(RING):
            group = ec
            if ec in (3, 12):
                o = {1: {3: UL, 12: UR}, 2: {3: L, 12: R}, 3: {3: L, 12: R}, 4: {3: DL, 12: DR}}[er][ec]
                key, group = o, ec + 2 * (er % 2)
                made[key] = columns(o) if key not in made else made[key]
            else:
                key = (er, ec // 4)
                made[key] = bf16(rows[er][ec // 4]) if key not in made else made[key]
            for s in range(SLOTS):
                yb[n, s] = jnp.where(groups[s], shift(made[key], s - group), jnp.bfloat16(0))

    r_iota = lax.broadcasted_iota(jnp.int32, (TILE, TILE), 0)
    c_iota = lax.broadcasted_iota(jnp.int32, (TILE, TILE), 1)
    across = jnp.logical_or(jnp.logical_and(r_iota < 32, c_iota >= 96), jnp.logical_and(r_iota >= 96, c_iota < 32))

    def advance_ring(rows, rs, rsc, first):
        ins = Inputs(rows)
        none = jnp.zeros((32, TILE), jnp.bfloat16)
        zero = jnp.zeros((TILE, TILE), jnp.float32)

        def update(own, lhs, rhs, v):
            acc = contract(jnp.concatenate(lhs, axis=1), jnp.concatenate(rhs, axis=1))
            if first:
                return own + f * (acc[SIG:SIG + 1] * v[:SIG] - acc[:SIG])
            return own - (2.0 * f) * acc

        def at(w, group):
            return jnp.concatenate([none] * group + [w] + [none] * (3 - group), axis=0)

        def end(q, right):
            return jnp.where(left if right else jnp.logical_not(left), q, jnp.bfloat16(0))

        new = [[None] * 4 for _ in range(6)]
        for er, u, ul, ur in ((1, U, UL, UR), (2, None, L, R), (3, None, L, R), (4, D, DL, DR)):
            i = er % 2
            feed = er + 1 if er in (1, 3) else er - 1
            edge = er - i
            for t in range(4):
                if t == 0:
                    new[er][t] = update(beside(rsc, i, ul), [ins.row(feed, 3), ins.column(edge, 1)],
                                        [at(tr[ul, i, 8], 3), at(end(tr[ul, i, 9], True), 3)], rows[er][t])
                elif t == 3:
                    new[er][t] = update(beside(rsc, i, ur), [ins.row(feed, 12), ins.column(edge, 2)],
                                        [at(tr[ur, i, 1], 0), at(end(tr[ur, i, 0], False), 0)], rows[er][t])
                elif u is not None:
                    w = f32(jnp.concatenate([tr[u, i, 4 * t - 3 + n] for n in range(4)], axis=0))
                    q = at(end(tr[u, i, 0], t == 2), 0 if t == 1 else 3)
                    new[er][t] = update(
                        f32(rs[u, i, t - 1]),
                        [ins.plain(feed, t), ins.crossing(feed, t), ins.column(edge, 0 if t == 1 else 3)],
                        [bf16(jnp.where(across, zero, w)), bf16(jnp.where(across, w, zero)), q], rows[er][t])
        return new

    tables(False)
    add_totals(0)
    for b in range(NB):
        packed = [shift(jnp.where(low, f32(til[b, s]), 0.0), s) for s in range(SLOTS)]
        wr[b] = bf16((packed[0] + packed[1]) + (packed[2] + packed[3]))
    own_part(0, x1)
    pl.semaphore_wait(in_y, 3)
    for o in rest:
        pl.semaphore_signal(in_xy, inc=1, device_id=other(o), device_id_type=MESH)

    wait_all(False, *first[:4])
    rows = with_edges(rows_of(op1, rv1, rc1), rows_of(eg, re, rec))

    def column1(o):
        side = 1 if o in (L, UL, DL) else 0
        return jnp.concatenate([rc1[o, side], bf16(jnp.where(top, rec[o, side], 0.0))], axis=0)

    unpack_far(rows, y1, column1)
    for b in range(NB):
        acc = far_product(b, y1)
        fl = f * live_of(b)
        deg = fl * acc[SIG:SIG + 1]
        amul[b] = 2.0 * (dloc[b] + jnp.broadcast_to(deg, (8, TILE)) - 1.0)
        cur = base[b] + deg * cheb[0, b] - fl * acc[:SIG]
        cheb[1, b] = cur
        place(b, cur, x2)
    wait_all(False, *first[4:])
    unpack(advance_ring(rows, rs1, rsc1, 1), x2)

    def step(b, k, xb):
        acc = product(b, xb, idx)
        am = amul[b]
        am = jnp.concatenate([am, am], axis=0)
        return am * cheb[k, b] - (2.0 * f * live_of(b)) * acc - cheb[k - 1, b]

    packs = {}
    for b in range(NB):
        cur = step(b, 1, x2)
        cheb[2, b] = cur
        place(b, cur, x3, packs)
    flush(packs, op3, oc3, bf16, True)
    for message in v3:
        send(message)
    local_part(2, x3, sp3, sc3)
    for message in s3:
        send(message)
    own_part(2, x3)
    add_totals(1)
    add_totals(2)
    wait_all(True, *first)

    wait_all(False, *v3)
    rows = rows_of(op3, rv3, rc3)
    unpack_far(rows, y3, lambda o: rc3[o, 1 if o in (L, UL, DL) else 0])
    for b in range(NB):
        cur = base[b] - (2.0 * f * live_of(b)) * far_product(b, y3)
        cheb[3, b] = cur
        place(b, cur, x4)
    add_totals(3)
    wait_all(False, *s3)
    unpack(advance_ring(rows, rs3, rsc3, 0), x4)
    sq = [None] * SCALES
    for b in range(NB):
        cur = step(b, 3, x4)
        for s in range(SCALES):
            t = tot[s, b] + cof_s[s, 4] * cur
            tot[s, b] = t
            sq[s] = t * t if sq[s] is None else sq[s] + t * t

    m = jnp.concatenate(sq, axis=0)
    hi = m.astype(jnp.bfloat16)
    r1 = m - hi.astype(jnp.float32)
    mid = r1.astype(jnp.bfloat16)
    lo = (r1 - mid.astype(jnp.float32)).astype(jnp.bfloat16)
    ones = jnp.ones((16, TILE), jnp.bfloat16)
    row = None
    for part in (lo, mid, hi):
        p = lax.dot_general(ones, part, (((1,), (1,)), ((), ())), preferred_element_type=jnp.float32)
        row = p if row is None else row + p
    row = jnp.concatenate([row[0:1], jnp.zeros((1, TILE - SCALES * SIG), jnp.float32)], axis=1)

    ga[me] = row
    pl.semaphore_wait(in_xy, 7)
    for o in FAR_FIRST:
        pltpu.make_async_remote_copy(
            src_ref=ga.at[me], dst_ref=ga.at[me], send_sem=sa, recv_sem=ra,
            device_id=other(o), device_id_type=MESH).start()
    wait_all(True, *v3, *s3)
    many = ga.at[pl.ds(0, DEVICES - 1)]
    pltpu.make_async_remote_copy(
        src_ref=many, dst_ref=many, send_sem=sa, recv_sem=ra, device_id=other(1), device_id_type=MESH).wait_recv()
    sums = [ga[q] for q in range(DEVICES)]
    while len(sums) > 1:
        sums = [u + v for u, v in zip(sums[::2], sums[1::2])]
    full = sums[0] * (1.0 / NODES)
    res = jnp.zeros((8, TILE), jnp.float32)
    sub = lax.broadcasted_iota(jnp.int32, (8, TILE), 0)
    full8 = jnp.broadcast_to(full, (8, TILE))
    for s in range(SCALES):
        v = pltpu.roll(full8, TILE - 16 * s, 1) if s else full8
        res = jnp.where(sub == s, v, res)
    en_ref[...] = res[:SCALES, :SIG]

    pltpu.make_async_remote_copy(
        src_ref=many, dst_ref=many, send_sem=sa, recv_sem=ra, device_id=other(1), device_id_type=MESH).wait_send()


def finish(tot, en, out_h, en_h, sem):
    a = pltpu.make_async_copy(tot, out_h, sem.at[0])
    b = pltpu.make_async_copy(en, en_h, sem.at[1])
    a.start()
    b.start()
    a.wait()
    b.wait()


def shards(signals, tiles, tile_dir, tile_mask, live_rows, bound_rows, scale_coeffs, spectral_bound):
    bf, f32, i32 = jnp.bfloat16, jnp.float32, jnp.int32
    vm, sm = pltpu.VMEM, pltpu.SMEM
    in_vmem = pl.BlockSpec(memory_space=pltpu.VMEM)
    hbm = pl.BlockSpec(memory_space=pl.ANY)
    dma = pltpu.SemaphoreType.DMA
    tot, energy = pl.pallas_call(
        kernel,
        out_shape=(pltpu.VMEM((SCALES, NB, SIG, TILE), f32), pltpu.VMEM((SCALES, SIG), f32)),
        in_specs=[hbm] * 7 + [pl.BlockSpec(memory_space=pltpu.HBM)],
        out_specs=(in_vmem, in_vmem),
        scratch_shapes=[
            sm((BX, SLOTS, BY), i32), sm((BX, SLOTS, BY), i32), sm((BX, BY), i32), sm((BX, BY), i32),
            sm((SCALES, DEG + 1), f32), sm((1,), f32),
            vm((BX, BY, SIG, TILE), f32), vm((NB, SLOTS, TILE, TILE), bf),
            sm((NB * SLOTS,), i32), sm((NB * SLOTS,), i32), sm((NB * SLOTS,), i32),
            vm((NX, 32, TILE), bf), vm((NX, SIG, TILE), bf), vm((NX, SIG, TILE), bf), vm((NX, SIG, TILE), bf),
            vm((NR + 1, SLOTS, 32, TILE), bf), vm((NR + 1, SLOTS, SIG, TILE), bf),
            vm((DEG, NB, SIG, TILE), f32), vm((NB, SIG, TILE), f32), vm((NB, 8, TILE), f32), vm((NB, 8, TILE), f32),
            vm((NB, TILE, TILE), bf),
            vm((2, 2, SIG, TILE), bf), vm((2, 2, SIG, TILE), bf), vm((2, 2, 1, TILE), f32),
            vm((2, 2, SIG, TILE), f32), vm((2, 2, SIG, TILE), bf), vm((2, 10, 32, TILE), bf),
            vm((2, SIG, TILE), bf), vm((2, SIG, TILE), bf), vm((2, 1, TILE), f32), vm((2, SIG, TILE), f32), vm((2, SIG, TILE), bf),
            vm((8, 2, 2, SIG, TILE), bf), vm((8, 2, 2, SIG, TILE), bf), vm((8, 2, 2, 1, TILE), f32),
            vm((8, 2, 2, SIG, TILE), f32), vm((8, 2, 2, SIG, TILE), bf), vm((8, 2, 10, 32, TILE), bf),
            vm((8, 2, SIG, TILE), bf), vm((8, 2, SIG, TILE), bf), vm((8, 2, 1, TILE), f32),
            vm((8, 2, SIG, TILE), f32), vm((8, 2, SIG, TILE), bf),
            vm((DEVICES, 1, TILE), f32), vm((1024, 1, TILE), f32),
            dma((11,)), dma, dma, dma, dma, dma, dma,
            dma, dma, pltpu.SemaphoreType.REGULAR, pltpu.SemaphoreType.REGULAR,
        ],
        compiler_params=pltpu.CompilerParams(collective_id=0, has_side_effects=True),
        name="wavelet",
    )(signals, tiles, jnp.swapaxes(tile_dir, 1, 2), jnp.swapaxes(tile_mask, 1, 2), live_rows, bound_rows,
      scale_coeffs, spectral_bound)
    out, energy = pl.pallas_call(
        finish,
        out_shape=(jax.ShapeDtypeStruct((SCALES, NB, SIG, TILE), f32), jax.ShapeDtypeStruct((SCALES, SIG), f32)),
        in_specs=[in_vmem, in_vmem],
        out_specs=(hbm, hbm),
        scratch_shapes=[dma((2,))],
        name="finish",
    )(pltpu.with_memory_space_constraint(tot, pltpu.VMEM), pltpu.with_memory_space_constraint(energy, pltpu.VMEM))
    return out.reshape(SCALES, BX, BY, SIG, TILE), energy


def solution(mesh):
    placed = (
        P("gx", "gy", None, None),
        P("gx", "gy", None, None, None),
        P("gx", "gy", None),
        P("gx", "gy", None),
        P("gx", "gy"),
        P("gx", "gy"),
        P(),
        P(),
    )
    return jax.shard_map(
        shards,
        mesh=mesh,
        in_specs=placed,
        out_specs=(P(None, "gx", "gy", None, None), P()),
        check_vma=False,
    )
```

```python
import functools
import operator

import jax
import jax.numpy as jnp
from jax import lax
from jax.experimental import pallas as pl
from jax.experimental.pallas import tpu as pltpu
from jax.sharding import PartitionSpec as P

MESH = pl.DeviceIdType.MESH
SIG, SCALES, DEG, SLOTS, TILE = 16, 6, 4, 4, 128
BX, BY = 2, 8
NB = BX * BY
GXN, GYN = 32, 4
ZERO = NB + (BX + 2) * (BY + 2)
NR = 24
NX = ZERO + 1
NODES = 64 * 32 * 128
DIRS = [(-1, 0), (1, 0), (0, -1), (0, 1), (-1, -1), (-1, 1), (1, -1), (1, 1)]
OPP = [DIRS.index((-dx, -dy)) for dx, dy in DIRS]


def hops(o):
    ring = (0, 1, 2, 1)
    return ring[o & 3] + ring[o >> 3 & 3] + ring[o >> 5 & 3] + 0.1 * (o >> 2 & 1)


DEVICES = 128
FAR_FIRST = sorted(range(1, DEVICES), key=lambda o: (-hops(o), o))


def kernel(sig_h, til_h, dir_h, msk_h, liv_h, bnd_h, cof_h, spb_h,
           tot, en_ref,
           dir_s, msk_s, liv_s, bnd_s, cof_s, spb_s, sig, til, idx, far, loc, x1, x2, x3, x4, y1, y3, cheb, base, amul, dloc, wr,
           op1, op3, eg, sp1, sp3, tp, oc1, oc3, ec1, sc1, sc3,
           rv1, rv3, re, rs1, rs3, tr, rc1, rc3, rec, rsc1, rsc3, ga, units,
           ld, r1, r2, w1, r3, r4, w3, sa, ra, in_y, in_xy):
    gx, gy = lax.axis_index("gx"), lax.axis_index("gy")
    me = gx * GYN + gy
    early = []
    for n, (src, dst) in enumerate(((sig_h, sig), (liv_h, liv_s), (bnd_h, bnd_s), (dir_h, dir_s), (msk_h, msk_s),
                                    (cof_h, cof_s), (spb_h, spb_s))):
        cp = pltpu.make_async_copy(src, dst, ld.at[n])
        cp.start()
        early.append(cp)

    def exists(d):
        dx, dy = DIRS[d]
        ok = None
        for step, pos, n in ((dx, gx, GXN), (dy, gy, GYN)):
            if step == 0:
                continue
            this = pos > 0 if step < 0 else pos < n - 1
            ok = this if ok is None else jnp.logical_and(ok, this)
        return ok

    have = [exists(d) for d in range(8)]
    peer = [(gx + dx, gy + dy) for dx, dy in DIRS]
    flip = lambda v: (v, v + 1 - 2 * (v % 2), (v + 2) % 4, 3 - v)
    xs, ys, zs = flip(gx // 8), flip(gx // 2 % 4), flip(gy)
    xyc = [8 * u + 2 * v + w for u in xs for v in ys for w in (gx % 2, 1 - gx % 2)]
    other = lambda o: (xyc[(o >> 5) * 8 + (o >> 3) % 4 * 2 + (o >> 2) % 2], zs[o % 4])
    rest = (1, 2, 3, 4, 5, 6, 7)
    ring_y, ring_x = (8, 16, 24), (32, 64, 96)
    bar = pltpu.get_barrier_semaphore()
    for d in (4, 5, 6, 7, 0, 1, 2, 3):
        @pl.when(have[d])
        def _(d=d):
            pl.semaphore_signal(bar, inc=1, device_id=peer[d], device_id_type=MESH)
    for o in ring_x + ring_y + rest:
        pl.semaphore_signal(bar, inc=1, device_id=other(o), device_id_type=MESH)
    count = jnp.int32(13)
    for d in range(8):
        count = count + have[d].astype(jnp.int32)
    til_cp = []
    for n in range(4):
        cp = pltpu.make_async_copy(til_h.at[n // 2, pl.ds(4 * (n % 2), 4)], til.at[pl.ds(4 * n, 4)], ld.at[7 + n])
        cp.start()
        til_cp.append(cp)
    for cp in early:
        cp.wait()

    lane = lax.broadcasted_iota(jnp.int32, (1, TILE), 1)
    low, high, left = lane < 32, lane >= 96, lane < 64
    middle = jnp.logical_and(lane >= 32, lane < 96)
    groups = [jnp.logical_and(lane >= 32 * s, lane < 32 * s + 32) for s in range(SLOTS)]
    f = 2.0 / spb_s[0]
    bf16 = lambda a: a.astype(jnp.bfloat16)
    f32 = lambda a: a.astype(jnp.float32)
    for xb in (x1, x2, x3, x4):
        xb[ZERO] = jnp.zeros(xb.shape[1:], xb.dtype)
    for yb in (y1, y3):
        yb[NR] = jnp.zeros(yb.shape[1:], yb.dtype)

    def live_of(b):
        return (lane < liv_s[b // BY, b % BY]).astype(jnp.float32)

    def edge_of(b):
        return (lane < bnd_s[b // BY, b % BY]).astype(jnp.float32)

    def shift(v, q):
        q = q % 4
        return pltpu.roll(v, 32 * q, 1) if q else v

    def add_to(packs, i, j, v, column):
        for key, group in ((("m", i, j // 4), j),
                           (("c", 0 if j < BY // 2 else 1), j + 2 * i)):
            if key[0] == "c" and j not in column:
                continue
            w = shift(v, group)
            packs[key] = w if key not in packs else packs[key] + w

    def flush(packs, main, column, cast, tile_first):
        for key, v in packs.items():
            if key[0] == "c":
                column[key[1]] = cast(v)
            elif tile_first:
                main[key[2], key[1]] = cast(v)
            else:
                main[key[1], key[2]] = cast(v)

    same = lambda v: v
    TWO, ONE = (0, 1, 6, 7), (0, 7)

    RING = [(r, q) for r in (1, 4) for q in range(3, 13)] + [(r, q) for r in (2, 3) for q in (3, 12)]
    slot_of = lambda er, ec: NB + (er - 1) * (BY + 2) + ec - 3

    def place(b, v, xb, packs=None):
        xb[b] = bf16(v)
        e = v * edge_of(b)
        xb[slot_of(b // BY + 2, b % BY + 4)] = bf16(e)
        if packs is not None:
            add_to(packs, b // BY, b % BY, e[:SIG], TWO)

    def part_v(dx, dy):
        return (pl.ds(0, 2),) if dy == 0 else None

    def part_s(dx, dy):
        return ({-1: pl.ds(0, 1), 1: pl.ds(1, 1)}[dx], pl.ds(0, 2)) if dy == 0 else None

    def part_c(dx, dy):
        return (pl.ds((dy + 1) // 2, 1),) if dy != 0 else None

    def part_t(dx, dy):
        return ({-1: pl.ds(0, 1), 1: pl.ds(1, 1), 0: pl.ds(0, 2)}[dx],
                {-1: pl.ds(0, 2), 1: pl.ds(7, 2), 0: pl.ds(0, 7)}[dy])

    def descriptor(src, dst, part, s_sem, r_sem, d, o, at):
        return pltpu.make_async_remote_copy(
            src_ref=src.at[at], dst_ref=dst.at[(o,) + at], send_sem=s_sem, recv_sem=r_sem,
            device_id=peer[d], device_id_type=MESH)

    def send(*messages):
        for d in (4, 5, 6, 7, 0, 1, 2, 3):
            @pl.when(have[d])
            def _(d=d):
                for src, dst, part, s_sem, r_sem in messages:
                    at = part(*DIRS[d])
                    if at is not None:
                        descriptor(src, dst, part, s_sem, r_sem, d, OPP[d], at).start()

    inner_x = jnp.logical_and(gx > 0, gx < GXN - 1)
    inner_y = jnp.logical_and(gy > 0, gy < GYN - 1)

    def wait_all(sent, *messages):
        def size(d):
            n = 0
            for src, _, part, _, _ in messages:
                at = part(*DIRS[d])
                if at is None:
                    continue
                shape = [p.size for p in at] + list(src.shape[len(at):])
                n += src.dtype.itemsize * functools.reduce(operator.mul, shape) // 512
            return n

        _, _, _, s_sem, r_sem = messages[0]
        for nx in (1, 2):
            for ny in (1, 2):
                n = nx * size(0) + ny * size(2) + nx * ny * size(4)
                this = jnp.logical_and(inner_x == (nx == 2), inner_y == (ny == 2))

                @pl.when(this)
                def _(n=n):
                    ref = units.at[pl.ds(0, n)]
                    cp = pltpu.make_async_remote_copy(
                        src_ref=ref, dst_ref=ref, send_sem=s_sem, recv_sem=r_sem,
                        device_id=other(1), device_id_type=MESH)
                    cp.wait_send() if sent else cp.wait_recv()

    first = ((oc1, rc1, part_c, w1, r1), (op1, rv1, part_v, w1, r1), (eg, re, part_v, w1, r1), (ec1, rec, part_c, w1, r1),
             (sp1, rs1, part_s, w1, r2), (sc1, rsc1, part_c, w1, r2), (tp, tr, part_t, w1, r2))
    v3 = ((oc3, rc3, part_c, w3, r3), (op3, rv3, part_v, w3, r3))
    s3 = ((sp3, rs3, part_s, w3, r4), (sc3, rsc3, part_c, w3, r4))
    U, D, L, R, UL, UR, DL, DR = range(8)

    def contract(lhs, rhs):
        return lax.dot_general(lhs, rhs, (((1,), (1,)), ((), ())), preferred_element_type=jnp.float32)

    packs, epacks = {}, {}
    top = lax.broadcasted_iota(jnp.int32, (16, TILE), 0) == 0
    for b in range(NB):
        live = live_of(b)
        v = sig[b // BY, b % BY] * live
        cheb[0, b] = v
        place(b, jnp.concatenate([v, jnp.where(top, live, 0.0)], axis=0), x1, packs)
        add_to(epacks, b // BY, b % BY, edge_of(b), TWO)
    flush(packs, op1, oc1, bf16, True)
    flush(epacks, eg, ec1, same, True)

    def tables(own):
        for b in range(NB):
            i, j = b // BY, b % BY
            for s in range(SLOTS):
                d = dir_s[i, s, j]
                r = (d * 11) >> 5
                q = d - 3 * r
                used = msk_s[i, s, j] == 1
                off = jnp.where(d == 4, b, NB + (i + r) * (BY + 2) + (j + q))
                ring = 10 * i + j + q
                away = r == 2 * i
                if j in (0, BY - 1):
                    beyond = q == (0 if j == 0 else 2)
                    ring = jnp.where(away, ring, 20 + 2 * (i + r - 1) + (0 if j == 0 else 1))
                    away = jnp.logical_or(away, beyond)
                if own:
                    loc[b * SLOTS + s] = jnp.where(jnp.logical_and(used, jnp.logical_not(away)), off, ZERO)
                else:
                    idx[b * SLOTS + s] = jnp.where(used, off, ZERO)
                    far[b * SLOTS + s] = jnp.where(jnp.logical_and(used, away), ring, NR)

    tables(True)

    def sorted_rows(b, wanted):
        i, j = b // BY, b % BY
        total = None
        tiles = [f32(til[b, s, pl.ds(0, 32)]) for s in range(SLOTS)]
        for d, group in wanted:
            acc = None
            for s in range(SLOTS):
                on = jnp.logical_and(dir_s[i, s, j] == d, msk_s[i, s, j] == 1).astype(jnp.float32)
                t = tiles[s] * on
                acc = t if acc is None else acc + t
            acc = shift(jnp.where(low, acc, 0.0), group)
            total = acc if total is None else total + acc
        inside = lax.broadcasted_iota(jnp.int32, (32, TILE), 0) < bnd_s[i, j]
        return bf16(jnp.where(inside, total, 0.0))

    def directions(b):
        i, j = b // BY, b % BY
        yield None, [(6 * i + q, j + q - 1) for q in range(3)]
        if j == 0:
            yield 0, [(3 - 3 * i, 3), (6 - 3 * i, 2)]
        if j == BY - 1:
            yield 1, [(5 - 3 * i, 0), (8 - 3 * i, 1)]

    def product(b, xb, table, rows=TILE):
        acc = None
        for h in range(2):
            pick = [xb[table[b * SLOTS + 2 * h + n]] for n in range(2)]
            rhs = [til[b, 2 * h + n, :rows] for n in range(2)]
            p = contract(jnp.concatenate(pick, axis=1), jnp.concatenate(rhs, axis=1))
            acc = p if acc is None else acc + p
        return acc

    def own_part(k, xb):
        for b in range(NB):
            acc = product(b, xb, loc)
            fl = f * live_of(b)
            if k == 0:
                deg = fl * acc[SIG:SIG + 1]
                dloc[b] = jnp.broadcast_to(deg, (8, TILE))
                base[b] = (deg - 1.0) * cheb[0, b] - fl * acc[:SIG]
            else:
                am = amul[b]
                am = jnp.concatenate([am, am], axis=0)
                base[b] = am * cheb[k, b] - (2.0 * fl) * acc - cheb[k - 1, b]

    def far_product(b, yb):
        parts = [yb[far[b * SLOTS + s], s] for s in range(SLOTS)]
        return contract((parts[0] + parts[1]) + (parts[2] + parts[3]), wr[b])

    def local_part(k, xb, sp, sc):
        packs = {}
        for b in range(NB):
            acc = product(b, xb, loc, 32)
            v = cheb[k, b, :, :32]
            if k == 0:
                out = (f * acc[SIG:SIG + 1] - 1.0) * v - f * acc[:SIG]
            else:
                out = amul[b, :1, :32] * v - (2.0 * f) * acc - cheb[k - 1, b, :, :32]
            out = out * edge_of(b)[:, :32]
            add_to(packs, b // BY, b % BY,
                   jnp.concatenate([out, jnp.zeros((SIG, TILE - 32), jnp.float32)], axis=1), ONE)
        flush(packs, sp, sc, same if k == 0 else bf16, False)

    for cp in til_cp:
        cp.wait()
    ends, p = {}, {}
    for b in range(NB):
        for side, wanted in directions(b):
            rows = sorted_rows(b, wanted)
            if side is None:
                p[b // BY, b % BY] = rows
            else:
                ends[b // BY, side] = rows
    for i in range(BX):
        for h in range(2):
            for n in range(3):
                spare = jnp.where(groups[(n + 2) % 4], p[i, 4 * h + 3], jnp.bfloat16(0))
                tp[i, 1 + 3 * h + n] = p[i, 4 * h + n] + spare
        both = ends[i, 0] + ends[i, 1]
        tp[i, 0] = both
        tp[i, 7] = p[i, 7]
        tp[i, 8] = both
    local_part(0, x1, sp1, sc1)
    pl.semaphore_wait(bar, count)
    for message in first:
        send(message)
    for o in ring_x:
        pl.semaphore_signal(in_y, inc=1, device_id=other(o), device_id_type=MESH)

    for d in range(8):
        @pl.when(jnp.logical_not(have[d]))
        def _(d=d):
            for buf in (rv1, rv3, re, rs1, rs3, tr, rc1, rc3, rec, rsc1, rsc3):
                buf[d] = jnp.zeros(buf.shape[1:], buf.dtype)

    def add_totals(k):
        for s in range(SCALES):
            a = cof_s[s, k] * 0.5 if k == 0 else cof_s[s, k]
            for b in range(NB):
                t = a * cheb[k, b]
                tot[s, b] = t if k == 0 else tot[s, b] + t

    def beside(rc, i, o):
        side = 1 if o in (L, UL, DL) else 0
        return shift(f32(rc[o, side]), 2 * i)

    def rows_of(op, rv, rc):
        rows = []
        for r in range(6):
            i = r % 2
            if r in (2, 3):
                ul, ur, mine = L, R, [op[t, i] for t in range(2)]
            else:
                u, ul, ur = (U, UL, UR) if r < 2 else (D, DL, DR)
                mine = [rv[u, t, i] for t in range(2)]
            rows.append([beside(rc, i, ul), f32(mine[0]), f32(mine[1]), beside(rc, i, ur)])
        return rows

    def with_edges(rows, edges):
        return [[jnp.concatenate([v, jnp.where(top, e, 0.0)], axis=0) for v, e in zip(r, q)]
                for r, q in zip(rows, edges)]

    class Inputs:
        def __init__(self, rows):
            self.rows, self.made = rows, {}

        def get(self, key, make):
            if key not in self.made:
                self.made[key] = bf16(make())
            return self.made[key]

        def plain(self, r, t):
            return self.get(("p", r, t), lambda: self.rows[r][t])

        def row(self, r, c):
            t, q, rows = c // 4, c % 4, self.rows[r]
            if q == 0:
                return self.get(("a", r, t), lambda: jnp.where(high, rows[t - 1], rows[t]))
            if q == 3:
                return self.get(("b", r, t), lambda: jnp.where(low, rows[t + 1], rows[t]))
            return self.plain(r, t)

        def crossing(self, r, t):
            rows = self.rows[r]
            before = rows[t - 1] if t > 0 else jnp.zeros_like(rows[t])
            after = rows[t + 1] if t < 3 else jnp.zeros_like(rows[t])
            return self.get(("x", r, t), lambda: jnp.where(left, after, before))

        def column(self, r, t):
            one, two = self.rows[r][t], self.rows[r + 1][t]
            return self.get(("c", r, t), lambda: jnp.where(
                middle, jnp.where(left, shift(two, 1), shift(two, -1)), one))

    def unpack(rows, xb):
        for er, ec in RING:
            v = jnp.where(low, shift(rows[er][ec // 4], -ec), 0.0)
            xb[slot_of(er, ec)] = bf16(v)

    def unpack_far(rows, yb, columns):
        made = {}
        for n, (er, ec) in enumerate(RING):
            group = ec
            if ec in (3, 12):
                o = {1: {3: UL, 12: UR}, 2: {3: L, 12: R}, 3: {3: L, 12: R}, 4: {3: DL, 12: DR}}[er][ec]
                key, group = o, ec + 2 * (er % 2)
                made[key] = columns(o) if key not in made else made[key]
            else:
                key = (er, ec // 4)
                made[key] = bf16(rows[er][ec // 4]) if key not in made else made[key]
            for s in range(SLOTS):
                yb[n, s] = jnp.where(groups[s], shift(made[key], s - group), jnp.bfloat16(0))

    r_iota = lax.broadcasted_iota(jnp.int32, (TILE, TILE), 0)
    c_iota = lax.broadcasted_iota(jnp.int32, (TILE, TILE), 1)
    across = jnp.logical_or(jnp.logical_and(r_iota < 32, c_iota >= 96), jnp.logical_and(r_iota >= 96, c_iota < 32))

    def advance_ring(rows, rs, rsc, first):
        ins = Inputs(rows)
        none = jnp.zeros((32, TILE), jnp.bfloat16)
        zero = jnp.zeros((TILE, TILE), jnp.float32)
        nil = jnp.bfloat16(0)

        def update(own, lhs, rhs, v):
            acc = contract(jnp.concatenate(lhs, axis=1), jnp.concatenate(rhs, axis=1))
            if first:
                return own + f * (acc[SIG:SIG + 1] * v[:SIG] - acc[:SIG])
            return own - (2.0 * f) * acc

        def at(w, group):
            return jnp.concatenate([none] * group + [w] + [none] * (3 - group), axis=0)

        def end(q, right):
            return jnp.where(left if right else jnp.logical_not(left), q, jnp.bfloat16(0))

        new = [[None] * 4 for _ in range(6)]
        for er, u, ul, ur in ((1, U, UL, UR), (2, None, L, R), (3, None, L, R), (4, D, DL, DR)):
            i = er % 2
            feed = er + 1 if er in (1, 3) else er - 1
            edge = er - i
            for t in range(4):
                if t == 0:
                    new[er][t] = update(beside(rsc, i, ul), [ins.row(feed, 3), ins.column(edge, 1)],
                                        [at(tr[ul, i, 7], 3), at(end(tr[ul, i, 8], True), 3)], rows[er][t])
                elif t == 3:
                    new[er][t] = update(beside(rsc, i, ur), [ins.row(feed, 12), ins.column(edge, 2)],
                                        [at(jnp.where(groups[2], nil, tr[ur, i, 1]), 0), at(end(tr[ur, i, 0], False), 0)], rows[er][t])
                elif u is not None:
                    held = [tr[u, i, 3 * t - 2 + n] for n in range(3)]
                    w = [jnp.where(groups[(n + 2) % 4], nil, held[n]) for n in range(3)]
                    w.append(jnp.where(groups[2], held[0], jnp.where(groups[3], held[1], jnp.where(groups[0], held[2], nil))))
                    w = f32(jnp.concatenate(w, axis=0))
                    q = at(end(tr[u, i, 0], t == 2), 0 if t == 1 else 3)
                    new[er][t] = update(
                        f32(rs[u, i, t - 1]),
                        [ins.plain(feed, t), ins.crossing(feed, t), ins.column(edge, 0 if t == 1 else 3)],
                        [bf16(jnp.where(across, zero, w)), bf16(jnp.where(across, w, zero)), q], rows[er][t])
        return new

    tables(False)
    add_totals(0)
    for b in range(NB):
        packed = [shift(jnp.where(low, f32(til[b, s]), 0.0), s) for s in range(SLOTS)]
        wr[b] = bf16((packed[0] + packed[1]) + (packed[2] + packed[3]))
    own_part(0, x1)
    pl.semaphore_wait(in_y, 3)
    for o in rest:
        pl.semaphore_signal(in_xy, inc=1, device_id=other(o), device_id_type=MESH)

    wait_all(False, *first[:4])
    rows = with_edges(rows_of(op1, rv1, rc1), rows_of(eg, re, rec))

    def column1(o):
        side = 1 if o in (L, UL, DL) else 0
        return jnp.concatenate([rc1[o, side], bf16(jnp.where(top, rec[o, side], 0.0))], axis=0)

    unpack_far(rows, y1, column1)
    for b in range(NB):
        acc = far_product(b, y1)
        fl = f * live_of(b)
        deg = fl * acc[SIG:SIG + 1]
        amul[b] = 2.0 * (dloc[b] + jnp.broadcast_to(deg, (8, TILE)) - 1.0)
        cur = base[b] + deg * cheb[0, b] - fl * acc[:SIG]
        cheb[1, b] = cur
        place(b, cur, x2)
    wait_all(False, *first[4:])
    unpack(advance_ring(rows, rs1, rsc1, 1), x2)

    def step(b, k, xb):
        acc = product(b, xb, idx)
        am = amul[b]
        am = jnp.concatenate([am, am], axis=0)
        return am * cheb[k, b] - (2.0 * f * live_of(b)) * acc - cheb[k - 1, b]

    packs = {}
    for b in range(NB):
        cur = step(b, 1, x2)
        cheb[2, b] = cur
        place(b, cur, x3, packs)
    flush(packs, op3, oc3, bf16, True)
    for message in v3:
        send(message)
    local_part(2, x3, sp3, sc3)
    for message in s3:
        send(message)
    own_part(2, x3)
    add_totals(1)
    add_totals(2)
    wait_all(True, *first)

    wait_all(False, *v3)
    rows = rows_of(op3, rv3, rc3)
    unpack_far(rows, y3, lambda o: rc3[o, 1 if o in (L, UL, DL) else 0])
    for b in range(NB):
        cur = base[b] - (2.0 * f * live_of(b)) * far_product(b, y3)
        cheb[3, b] = cur
        place(b, cur, x4)
    add_totals(3)
    wait_all(False, *s3)
    unpack(advance_ring(rows, rs3, rsc3, 0), x4)
    sq = [None] * SCALES
    for b in range(NB):
        cur = step(b, 3, x4)
        for s in range(SCALES):
            t = tot[s, b] + cof_s[s, 4] * cur
            tot[s, b] = t
            sq[s] = t * t if sq[s] is None else sq[s] + t * t

    m = jnp.concatenate(sq, axis=0)
    hi = m.astype(jnp.bfloat16)
    r1 = m - hi.astype(jnp.float32)
    mid = r1.astype(jnp.bfloat16)
    lo = (r1 - mid.astype(jnp.float32)).astype(jnp.bfloat16)
    ones = jnp.ones((16, TILE), jnp.bfloat16)
    row = None
    for part in (lo, mid, hi):
        p = lax.dot_general(ones, part, (((1,), (1,)), ((), ())), preferred_element_type=jnp.float32)
        row = p if row is None else row + p
    row = jnp.concatenate([row[0:1], jnp.zeros((1, TILE - SCALES * SIG), jnp.float32)], axis=1)

    ga[me] = row
    pl.semaphore_wait(in_xy, 7)
    for o in FAR_FIRST:
        pltpu.make_async_remote_copy(
            src_ref=ga.at[me], dst_ref=ga.at[me], send_sem=sa, recv_sem=ra,
            device_id=other(o), device_id_type=MESH).start()
    wait_all(True, *v3, *s3)
    many = ga.at[pl.ds(0, DEVICES - 1)]
    pltpu.make_async_remote_copy(
        src_ref=many, dst_ref=many, send_sem=sa, recv_sem=ra, device_id=other(1), device_id_type=MESH).wait_recv()
    sums = [ga[q] for q in range(DEVICES)]
    while len(sums) > 1:
        sums = [u + v for u, v in zip(sums[::2], sums[1::2])]
    full = sums[0] * (1.0 / NODES)
    res = jnp.zeros((8, TILE), jnp.float32)
    sub = lax.broadcasted_iota(jnp.int32, (8, TILE), 0)
    full8 = jnp.broadcast_to(full, (8, TILE))
    for s in range(SCALES):
        v = pltpu.roll(full8, TILE - 16 * s, 1) if s else full8
        res = jnp.where(sub == s, v, res)
    en_ref[...] = res[:SCALES, :SIG]

    pltpu.make_async_remote_copy(
        src_ref=many, dst_ref=many, send_sem=sa, recv_sem=ra, device_id=other(1), device_id_type=MESH).wait_send()


def finish(tot, en, out_h, en_h, sem):
    a = pltpu.make_async_copy(tot, out_h, sem.at[0])
    b = pltpu.make_async_copy(en, en_h, sem.at[1])
    a.start()
    b.start()
    a.wait()
    b.wait()


def shards(signals, tiles, tile_dir, tile_mask, live_rows, bound_rows, scale_coeffs, spectral_bound):
    bf, f32, i32 = jnp.bfloat16, jnp.float32, jnp.int32
    vm, sm = pltpu.VMEM, pltpu.SMEM
    in_vmem = pl.BlockSpec(memory_space=pltpu.VMEM)
    hbm = pl.BlockSpec(memory_space=pl.ANY)
    dma = pltpu.SemaphoreType.DMA
    tot, energy = pl.pallas_call(
        kernel,
        out_shape=(pltpu.VMEM((SCALES, NB, SIG, TILE), f32), pltpu.VMEM((SCALES, SIG), f32)),
        in_specs=[hbm] * 7 + [pl.BlockSpec(memory_space=pltpu.HBM)],
        out_specs=(in_vmem, in_vmem),
        scratch_shapes=[
            sm((BX, SLOTS, BY), i32), sm((BX, SLOTS, BY), i32), sm((BX, BY), i32), sm((BX, BY), i32),
            sm((SCALES, DEG + 1), f32), sm((1,), f32),
            vm((BX, BY, SIG, TILE), f32), vm((NB, SLOTS, TILE, TILE), bf),
            sm((NB * SLOTS,), i32), sm((NB * SLOTS,), i32), sm((NB * SLOTS,), i32),
            vm((NX, 32, TILE), bf), vm((NX, SIG, TILE), bf), vm((NX, SIG, TILE), bf), vm((NX, SIG, TILE), bf),
            vm((NR + 1, SLOTS, 32, TILE), bf), vm((NR + 1, SLOTS, SIG, TILE), bf),
            vm((DEG, NB, SIG, TILE), f32), vm((NB, SIG, TILE), f32), vm((NB, 8, TILE), f32), vm((NB, 8, TILE), f32),
            vm((NB, TILE, TILE), bf),
            vm((2, 2, SIG, TILE), bf), vm((2, 2, SIG, TILE), bf), vm((2, 2, 1, TILE), f32),
            vm((2, 2, SIG, TILE), f32), vm((2, 2, SIG, TILE), bf), vm((2, 9, 32, TILE), bf),
            vm((2, SIG, TILE), bf), vm((2, SIG, TILE), bf), vm((2, 1, TILE), f32), vm((2, SIG, TILE), f32), vm((2, SIG, TILE), bf),
            vm((8, 2, 2, SIG, TILE), bf), vm((8, 2, 2, SIG, TILE), bf), vm((8, 2, 2, 1, TILE), f32),
            vm((8, 2, 2, SIG, TILE), f32), vm((8, 2, 2, SIG, TILE), bf), vm((8, 2, 9, 32, TILE), bf),
            vm((8, 2, SIG, TILE), bf), vm((8, 2, SIG, TILE), bf), vm((8, 2, 1, TILE), f32),
            vm((8, 2, SIG, TILE), f32), vm((8, 2, SIG, TILE), bf),
            vm((DEVICES, 1, TILE), f32), vm((1024, 1, TILE), f32),
            dma((11,)), dma, dma, dma, dma, dma, dma,
            dma, dma, pltpu.SemaphoreType.REGULAR, pltpu.SemaphoreType.REGULAR,
        ],
        compiler_params=pltpu.CompilerParams(collective_id=0, has_side_effects=True),
        name="wavelet",
    )(signals, tiles, jnp.swapaxes(tile_dir, 1, 2), jnp.swapaxes(tile_mask, 1, 2), live_rows, bound_rows,
      scale_coeffs, spectral_bound)
    out, energy = pl.pallas_call(
        finish,
        out_shape=(jax.ShapeDtypeStruct((SCALES, NB, SIG, TILE), f32), jax.ShapeDtypeStruct((SCALES, SIG), f32)),
        in_specs=[in_vmem, in_vmem],
        out_specs=(hbm, hbm),
        scratch_shapes=[dma((2,))],
        name="finish",
    )(pltpu.with_memory_space_constraint(tot, pltpu.VMEM), pltpu.with_memory_space_constraint(energy, pltpu.VMEM))
    return out.reshape(SCALES, BX, BY, SIG, TILE), energy


def solution(mesh):
    placed = (
        P("gx", "gy", None, None),
        P("gx", "gy", None, None, None),
        P("gx", "gy", None),
        P("gx", "gy", None),
        P("gx", "gy"),
        P("gx", "gy"),
        P(),
        P(),
    )
    return jax.shard_map(
        shards,
        mesh=mesh,
        in_specs=placed,
        out_specs=(P(None, "gx", "gy", None, None), P()),
        check_vma=False,
    )
```

```python
import functools
import operator

import jax
import jax.numpy as jnp
from jax import lax
from jax.experimental import pallas as pl
from jax.experimental.pallas import tpu as pltpu
from jax.sharding import PartitionSpec as P

MESH = pl.DeviceIdType.MESH
SIG, SCALES, DEG, SLOTS, TILE = 16, 6, 4, 4, 128
BX, BY = 2, 8
NB = BX * BY
GXN, GYN = 32, 4
ZERO = NB + (BX + 2) * (BY + 2)
NR = 24
NX = ZERO + 1
NODES = 64 * 32 * 128
DIRS = [(-1, 0), (1, 0), (0, -1), (0, 1), (-1, -1), (-1, 1), (1, -1), (1, 1)]
OPP = [DIRS.index((-dx, -dy)) for dx, dy in DIRS]


def hops(o):
    ring = (0, 1, 2, 1)
    return ring[o & 3] + ring[o >> 3 & 3] + ring[o >> 5 & 3] + 0.1 * (o >> 2 & 1)


DEVICES = 128
FAR_FIRST = sorted(range(1, DEVICES), key=lambda o: (-hops(o), o))


def kernel(sig_h, til_h, dir_h, msk_h, liv_h, bnd_h, cof_h, spb_h,
           tot, en_ref,
           dir_s, msk_s, liv_s, bnd_s, cof_s, spb_s, sig, til, idx, far, loc, x1, x2, x3, x4, y1, y3, cheb, base, amul, dloc, wr,
           op1, op3, eg, sp1, sp3, tp, oc1, oc3, ec1, sc1, sc3,
           rv1, rv3, re, rs1, rs3, tr, rc1, rc3, rec, rsc1, rsc3, ga, units,
           ld, r1, r2, w1, r3, r4, w3, sa, ra, in_y, in_xy):
    gx, gy = lax.axis_index("gx"), lax.axis_index("gy")
    me = gx * GYN + gy
    def exists(d):
        dx, dy = DIRS[d]
        ok = None
        for step, pos, n in ((dx, gx, GXN), (dy, gy, GYN)):
            if step == 0:
                continue
            this = pos > 0 if step < 0 else pos < n - 1
            ok = this if ok is None else jnp.logical_and(ok, this)
        return ok

    have = [exists(d) for d in range(8)]
    peer = [(gx + dx, gy + dy) for dx, dy in DIRS]
    rest = (1, 2, 3, 4, 5, 6, 7)
    ring_y, ring_x = (8, 16, 24), (32, 64, 96)
    bar = pltpu.get_barrier_semaphore()
    for d in (4, 5, 6, 7, 0, 1, 2, 3):
        @pl.when(have[d])
        def _(d=d):
            pl.semaphore_signal(bar, inc=1, device_id=peer[d], device_id_type=MESH)
    flip = lambda v: (v, v + 1 - 2 * (v % 2), (v + 2) % 4, 3 - v)
    xs, ys, zs = flip(gx // 8), flip(gx // 2 % 4), flip(gy)
    xyc = [8 * u + 2 * v + w for u in xs for v in ys for w in (gx % 2, 1 - gx % 2)]
    other = lambda o: (xyc[(o >> 5) * 8 + (o >> 3) % 4 * 2 + (o >> 2) % 2], zs[o % 4])
    early = []
    for n, (src, dst) in enumerate(((sig_h, sig), (liv_h, liv_s), (bnd_h, bnd_s), (dir_h, dir_s), (msk_h, msk_s),
                                    (cof_h, cof_s), (spb_h, spb_s))):
        cp = pltpu.make_async_copy(src, dst, ld.at[n])
        cp.start()
        early.append(cp)
    for o in ring_x + ring_y + rest:
        pl.semaphore_signal(bar, inc=1, device_id=other(o), device_id_type=MESH)
    count = jnp.int32(13)
    for d in range(8):
        count = count + have[d].astype(jnp.int32)
    til_cp = []
    for n in range(4):
        cp = pltpu.make_async_copy(til_h.at[n // 2, pl.ds(4 * (n % 2), 4)], til.at[pl.ds(4 * n, 4)], ld.at[7 + n])
        cp.start()
        til_cp.append(cp)
    for cp in early:
        cp.wait()

    lane = lax.broadcasted_iota(jnp.int32, (1, TILE), 1)
    low, high, left = lane < 32, lane >= 96, lane < 64
    middle = jnp.logical_and(lane >= 32, lane < 96)
    groups = [jnp.logical_and(lane >= 32 * s, lane < 32 * s + 32) for s in range(SLOTS)]
    f = 2.0 / spb_s[0]
    bf16 = lambda a: a.astype(jnp.bfloat16)
    f32 = lambda a: a.astype(jnp.float32)
    for xb in (x1, x2, x3, x4):
        xb[ZERO] = jnp.zeros(xb.shape[1:], xb.dtype)
    for yb in (y1, y3):
        yb[NR] = jnp.zeros(yb.shape[1:], yb.dtype)

    def live_of(b):
        return (lane < liv_s[b // BY, b % BY]).astype(jnp.float32)

    def edge_of(b):
        return (lane < bnd_s[b // BY, b % BY]).astype(jnp.float32)

    def shift(v, q):
        q = q % 4
        return pltpu.roll(v, 32 * q, 1) if q else v

    def add_to(packs, i, j, v, column):
        for key, group in ((("m", i, j // 4), j),
                           (("c", 0 if j < BY // 2 else 1), j + 2 * i)):
            if key[0] == "c" and j not in column:
                continue
            w = shift(v, group)
            packs[key] = w if key not in packs else packs[key] + w

    def flush(packs, main, column, cast, tile_first):
        for key, v in packs.items():
            if key[0] == "c":
                column[key[1]] = cast(v)
            elif tile_first:
                main[key[2], key[1]] = cast(v)
            else:
                main[key[1], key[2]] = cast(v)

    same = lambda v: v
    TWO, ONE = (0, 1, 6, 7), (0, 7)

    RING = [(r, q) for r in (1, 4) for q in range(3, 13)] + [(r, q) for r in (2, 3) for q in (3, 12)]
    slot_of = lambda er, ec: NB + (er - 1) * (BY + 2) + ec - 3

    def place(b, v, xb, packs=None):
        xb[b] = bf16(v)
        e = v * edge_of(b)
        xb[slot_of(b // BY + 2, b % BY + 4)] = bf16(e)
        if packs is not None:
            add_to(packs, b // BY, b % BY, e[:SIG], TWO)

    def part_v(dx, dy):
        return (pl.ds(0, 2),) if dy == 0 else None

    def part_s(dx, dy):
        return ({-1: pl.ds(0, 1), 1: pl.ds(1, 1)}[dx], pl.ds(0, 2)) if dy == 0 else None

    def part_c(dx, dy):
        return (pl.ds((dy + 1) // 2, 1),) if dy != 0 else None

    def part_t(dx, dy):
        return ({-1: pl.ds(0, 1), 1: pl.ds(1, 1), 0: pl.ds(0, 2)}[dx],
                {-1: pl.ds(0, 2), 1: pl.ds(7, 2), 0: pl.ds(0, 7)}[dy])

    def descriptor(src, dst, part, s_sem, r_sem, d, o, at):
        return pltpu.make_async_remote_copy(
            src_ref=src.at[at], dst_ref=dst.at[(o,) + at], send_sem=s_sem, recv_sem=r_sem,
            device_id=peer[d], device_id_type=MESH)

    def send(*messages):
        for d in (4, 5, 6, 7, 0, 1, 2, 3):
            @pl.when(have[d])
            def _(d=d):
                for src, dst, part, s_sem, r_sem in messages:
                    at = part(*DIRS[d])
                    if at is not None:
                        descriptor(src, dst, part, s_sem, r_sem, d, OPP[d], at).start()

    inner_x = jnp.logical_and(gx > 0, gx < GXN - 1)
    inner_y = jnp.logical_and(gy > 0, gy < GYN - 1)

    def wait_all(sent, *messages):
        def size(d):
            n = 0
            for src, _, part, _, _ in messages:
                at = part(*DIRS[d])
                if at is None:
                    continue
                shape = [p.size for p in at] + list(src.shape[len(at):])
                n += src.dtype.itemsize * functools.reduce(operator.mul, shape) // 512
            return n

        _, _, _, s_sem, r_sem = messages[0]
        for nx in (1, 2):
            for ny in (1, 2):
                n = nx * size(0) + ny * size(2) + nx * ny * size(4)
                this = jnp.logical_and(inner_x == (nx == 2), inner_y == (ny == 2))

                @pl.when(this)
                def _(n=n):
                    ref = units.at[pl.ds(0, n)]
                    cp = pltpu.make_async_remote_copy(
                        src_ref=ref, dst_ref=ref, send_sem=s_sem, recv_sem=r_sem,
                        device_id=other(1), device_id_type=MESH)
                    cp.wait_send() if sent else cp.wait_recv()

    first = ((oc1, rc1, part_c, w1, r1), (op1, rv1, part_v, w1, r1), (eg, re, part_v, w1, r1), (ec1, rec, part_c, w1, r1),
             (sp1, rs1, part_s, w1, r2), (sc1, rsc1, part_c, w1, r2), (tp, tr, part_t, w1, r2))
    v3 = ((oc3, rc3, part_c, w3, r3), (op3, rv3, part_v, w3, r3))
    s3 = ((sp3, rs3, part_s, w3, r4), (sc3, rsc3, part_c, w3, r4))
    U, D, L, R, UL, UR, DL, DR = range(8)

    def contract(lhs, rhs):
        return lax.dot_general(lhs, rhs, (((1,), (1,)), ((), ())), preferred_element_type=jnp.float32)

    packs, epacks = {}, {}
    top = lax.broadcasted_iota(jnp.int32, (16, TILE), 0) == 0
    for b in range(NB):
        live = live_of(b)
        v = sig[b // BY, b % BY] * live
        cheb[0, b] = v
        place(b, jnp.concatenate([v, jnp.where(top, live, 0.0)], axis=0), x1, packs)
        add_to(epacks, b // BY, b % BY, edge_of(b), TWO)
    flush(packs, op1, oc1, bf16, True)
    flush(epacks, eg, ec1, same, True)

    def tables(own):
        for b in range(NB):
            i, j = b // BY, b % BY
            for s in range(SLOTS):
                d = dir_s[i, s, j]
                r = (d * 11) >> 5
                q = d - 3 * r
                used = msk_s[i, s, j] == 1
                off = jnp.where(d == 4, b, NB + (i + r) * (BY + 2) + (j + q))
                ring = 10 * i + j + q
                away = r == 2 * i
                if j in (0, BY - 1):
                    beyond = q == (0 if j == 0 else 2)
                    ring = jnp.where(away, ring, 20 + 2 * (i + r - 1) + (0 if j == 0 else 1))
                    away = jnp.logical_or(away, beyond)
                if own:
                    loc[b * SLOTS + s] = jnp.where(jnp.logical_and(used, jnp.logical_not(away)), off, ZERO)
                else:
                    idx[b * SLOTS + s] = jnp.where(used, off, ZERO)
                    far[b * SLOTS + s] = jnp.where(jnp.logical_and(used, away), ring, NR)

    tables(True)

    def sorted_rows(b, wanted):
        i, j = b // BY, b % BY
        total = None
        tiles = [f32(til[b, s, pl.ds(0, 32)]) for s in range(SLOTS)]
        for d, group in wanted:
            acc = None
            for s in range(SLOTS):
                on = jnp.logical_and(dir_s[i, s, j] == d, msk_s[i, s, j] == 1).astype(jnp.float32)
                t = tiles[s] * on
                acc = t if acc is None else acc + t
            acc = shift(jnp.where(low, acc, 0.0), group)
            total = acc if total is None else total + acc
        inside = lax.broadcasted_iota(jnp.int32, (32, TILE), 0) < bnd_s[i, j]
        return bf16(jnp.where(inside, total, 0.0))

    def directions(b):
        i, j = b // BY, b % BY
        yield None, [(6 * i + q, j + q - 1) for q in range(3)]
        if j == 0:
            yield 0, [(3 - 3 * i, 3), (6 - 3 * i, 2)]
        if j == BY - 1:
            yield 1, [(5 - 3 * i, 0), (8 - 3 * i, 1)]

    def product(b, xb, table, rows=TILE):
        acc = None
        for h in range(2):
            pick = [xb[table[b * SLOTS + 2 * h + n]] for n in range(2)]
            rhs = [til[b, 2 * h + n, :rows] for n in range(2)]
            p = contract(jnp.concatenate(pick, axis=1), jnp.concatenate(rhs, axis=1))
            acc = p if acc is None else acc + p
        return acc

    def own_part(k, xb):
        for b in range(NB):
            acc = product(b, xb, loc)
            fl = f * live_of(b)
            if k == 0:
                deg = fl * acc[SIG:SIG + 1]
                dloc[b] = jnp.broadcast_to(deg, (8, TILE))
                base[b] = (deg - 1.0) * cheb[0, b] - fl * acc[:SIG]
            else:
                am = amul[b]
                am = jnp.concatenate([am, am], axis=0)
                base[b] = am * cheb[k, b] - (2.0 * fl) * acc - cheb[k - 1, b]

    def far_product(b, yb):
        parts = [yb[far[b * SLOTS + s], s] for s in range(SLOTS)]
        return contract((parts[0] + parts[1]) + (parts[2] + parts[3]), wr[b])

    def local_part(k, xb, sp, sc):
        packs = {}
        for b in range(NB):
            acc = product(b, xb, loc, 32)
            v = cheb[k, b, :, :32]
            if k == 0:
                out = (f * acc[SIG:SIG + 1] - 1.0) * v - f * acc[:SIG]
            else:
                out = amul[b, :1, :32] * v - (2.0 * f) * acc - cheb[k - 1, b, :, :32]
            out = out * edge_of(b)[:, :32]
            add_to(packs, b // BY, b % BY,
                   jnp.concatenate([out, jnp.zeros((SIG, TILE - 32), jnp.float32)], axis=1), ONE)
        flush(packs, sp, sc, same if k == 0 else bf16, False)

    for cp in til_cp:
        cp.wait()
    ends, p = {}, {}
    for b in range(NB):
        for side, wanted in directions(b):
            rows = sorted_rows(b, wanted)
            if side is None:
                p[b // BY, b % BY] = rows
            else:
                ends[b // BY, side] = rows
    for i in range(BX):
        for h in range(2):
            for n in range(3):
                spare = jnp.where(groups[(n + 2) % 4], p[i, 4 * h + 3], jnp.bfloat16(0))
                tp[i, 1 + 3 * h + n] = p[i, 4 * h + n] + spare
        both = ends[i, 0] + ends[i, 1]
        tp[i, 0] = both
        tp[i, 7] = p[i, 7]
        tp[i, 8] = both
    local_part(0, x1, sp1, sc1)
    pl.semaphore_wait(bar, count)
    for message in first:
        send(message)
    for o in ring_x:
        pl.semaphore_signal(in_y, inc=1, device_id=other(o), device_id_type=MESH)

    for d in range(8):
        @pl.when(jnp.logical_not(have[d]))
        def _(d=d):
            for buf in (rv1, rv3, re, rs1, rs3, tr, rc1, rc3, rec, rsc1, rsc3):
                buf[d] = jnp.zeros(buf.shape[1:], buf.dtype)

    def add_totals(k):
        for s in range(SCALES):
            a = cof_s[s, k] * 0.5 if k == 0 else cof_s[s, k]
            for b in range(NB):
                t = a * cheb[k, b]
                tot[s, b] = t if k == 0 else tot[s, b] + t

    def beside(rc, i, o):
        side = 1 if o in (L, UL, DL) else 0
        return shift(f32(rc[o, side]), 2 * i)

    def rows_of(op, rv, rc):
        rows = []
        for r in range(6):
            i = r % 2
            if r in (2, 3):
                ul, ur, mine = L, R, [op[t, i] for t in range(2)]
            else:
                u, ul, ur = (U, UL, UR) if r < 2 else (D, DL, DR)
                mine = [rv[u, t, i] for t in range(2)]
            rows.append([beside(rc, i, ul), f32(mine[0]), f32(mine[1]), beside(rc, i, ur)])
        return rows

    def with_edges(rows, edges):
        return [[jnp.concatenate([v, jnp.where(top, e, 0.0)], axis=0) for v, e in zip(r, q)]
                for r, q in zip(rows, edges)]

    class Inputs:
        def __init__(self, rows):
            self.rows, self.made = rows, {}

        def get(self, key, make):
            if key not in self.made:
                self.made[key] = bf16(make())
            return self.made[key]

        def plain(self, r, t):
            return self.get(("p", r, t), lambda: self.rows[r][t])

        def row(self, r, c):
            t, q, rows = c // 4, c % 4, self.rows[r]
            if q == 0:
                return self.get(("a", r, t), lambda: jnp.where(high, rows[t - 1], rows[t]))
            if q == 3:
                return self.get(("b", r, t), lambda: jnp.where(low, rows[t + 1], rows[t]))
            return self.plain(r, t)

        def crossing(self, r, t):
            rows = self.rows[r]
            before = rows[t - 1] if t > 0 else jnp.zeros_like(rows[t])
            after = rows[t + 1] if t < 3 else jnp.zeros_like(rows[t])
            return self.get(("x", r, t), lambda: jnp.where(left, after, before))

        def column(self, r, t):
            one, two = self.rows[r][t], self.rows[r + 1][t]
            return self.get(("c", r, t), lambda: jnp.where(
                middle, jnp.where(left, shift(two, 1), shift(two, -1)), one))

    def unpack(rows, xb):
        for er, ec in RING:
            v = jnp.where(low, shift(rows[er][ec // 4], -ec), 0.0)
            xb[slot_of(er, ec)] = bf16(v)

    def unpack_far(rows, yb, columns):
        made = {}
        for n, (er, ec) in enumerate(RING):
            group = ec
            if ec in (3, 12):
                o = {1: {3: UL, 12: UR}, 2: {3: L, 12: R}, 3: {3: L, 12: R}, 4: {3: DL, 12: DR}}[er][ec]
                key, group = o, ec + 2 * (er % 2)
                made[key] = columns(o) if key not in made else made[key]
            else:
                key = (er, ec // 4)
                made[key] = bf16(rows[er][ec // 4]) if key not in made else made[key]
            for s in range(SLOTS):
                yb[n, s] = jnp.where(groups[s], shift(made[key], s - group), jnp.bfloat16(0))

    r_iota = lax.broadcasted_iota(jnp.int32, (TILE, TILE), 0)
    c_iota = lax.broadcasted_iota(jnp.int32, (TILE, TILE), 1)
    across = jnp.logical_or(jnp.logical_and(r_iota < 32, c_iota >= 96), jnp.logical_and(r_iota >= 96, c_iota < 32))

    def advance_ring(rows, rs, rsc, first):
        ins = Inputs(rows)
        none = jnp.zeros((32, TILE), jnp.bfloat16)
        zero = jnp.zeros((TILE, TILE), jnp.float32)
        nil = jnp.bfloat16(0)

        def update(own, lhs, rhs, v):
            acc = contract(jnp.concatenate(lhs, axis=1), jnp.concatenate(rhs, axis=1))
            if first:
                return own + f * (acc[SIG:SIG + 1] * v[:SIG] - acc[:SIG])
            return own - (2.0 * f) * acc

        def at(w, group):
            return jnp.concatenate([none] * group + [w] + [none] * (3 - group), axis=0)

        def end(q, right):
            return jnp.where(left if right else jnp.logical_not(left), q, jnp.bfloat16(0))

        new = [[None] * 4 for _ in range(6)]
        for er, u, ul, ur in ((1, U, UL, UR), (2, None, L, R), (3, None, L, R), (4, D, DL, DR)):
            i = er % 2
            feed = er + 1 if er in (1, 3) else er - 1
            edge = er - i
            for t in range(4):
                if t == 0:
                    new[er][t] = update(beside(rsc, i, ul), [ins.row(feed, 3), ins.column(edge, 1)],
                                        [at(tr[ul, i, 7], 3), at(end(tr[ul, i, 8], True), 3)], rows[er][t])
                elif t == 3:
                    new[er][t] = update(beside(rsc, i, ur), [ins.row(feed, 12), ins.column(edge, 2)],
                                        [at(jnp.where(groups[2], nil, tr[ur, i, 1]), 0), at(end(tr[ur, i, 0], False), 0)], rows[er][t])
                elif u is not None:
                    held = [tr[u, i, 3 * t - 2 + n] for n in range(3)]
                    w = [jnp.where(groups[(n + 2) % 4], nil, held[n]) for n in range(3)]
                    w.append(jnp.where(groups[2], held[0], jnp.where(groups[3], held[1], jnp.where(groups[0], held[2], nil))))
                    w = f32(jnp.concatenate(w, axis=0))
                    q = at(end(tr[u, i, 0], t == 2), 0 if t == 1 else 3)
                    new[er][t] = update(
                        f32(rs[u, i, t - 1]),
                        [ins.plain(feed, t), ins.crossing(feed, t), ins.column(edge, 0 if t == 1 else 3)],
                        [bf16(jnp.where(across, zero, w)), bf16(jnp.where(across, w, zero)), q], rows[er][t])
        return new

    tables(False)
    add_totals(0)
    for b in range(NB):
        packed = [shift(jnp.where(low, f32(til[b, s]), 0.0), s) for s in range(SLOTS)]
        wr[b] = bf16((packed[0] + packed[1]) + (packed[2] + packed[3]))
    own_part(0, x1)
    pl.semaphore_wait(in_y, 3)
    for o in rest:
        pl.semaphore_signal(in_xy, inc=1, device_id=other(o), device_id_type=MESH)

    wait_all(False, *first[:4])
    rows = with_edges(rows_of(op1, rv1, rc1), rows_of(eg, re, rec))

    def column1(o):
        side = 1 if o in (L, UL, DL) else 0
        return jnp.concatenate([rc1[o, side], bf16(jnp.where(top, rec[o, side], 0.0))], axis=0)

    unpack_far(rows, y1, column1)
    for b in range(NB):
        acc = far_product(b, y1)
        fl = f * live_of(b)
        deg = fl * acc[SIG:SIG + 1]
        amul[b] = 2.0 * (dloc[b] + jnp.broadcast_to(deg, (8, TILE)) - 1.0)
        cur = base[b] + deg * cheb[0, b] - fl * acc[:SIG]
        cheb[1, b] = cur
        place(b, cur, x2)
    wait_all(False, *first[4:])
    unpack(advance_ring(rows, rs1, rsc1, 1), x2)

    def step(b, k, xb):
        acc = product(b, xb, idx)
        am = amul[b]
        am = jnp.concatenate([am, am], axis=0)
        return am * cheb[k, b] - (2.0 * f * live_of(b)) * acc - cheb[k - 1, b]

    packs = {}
    for b in range(NB):
        cur = step(b, 1, x2)
        cheb[2, b] = cur
        place(b, cur, x3, packs)
    flush(packs, op3, oc3, bf16, True)
    for message in v3:
        send(message)
    local_part(2, x3, sp3, sc3)
    for message in s3:
        send(message)
    own_part(2, x3)
    add_totals(1)
    add_totals(2)
    wait_all(True, *first)

    wait_all(False, *v3)
    rows = rows_of(op3, rv3, rc3)
    unpack_far(rows, y3, lambda o: rc3[o, 1 if o in (L, UL, DL) else 0])
    for b in range(NB):
        cur = base[b] - (2.0 * f * live_of(b)) * far_product(b, y3)
        cheb[3, b] = cur
        place(b, cur, x4)
    add_totals(3)
    wait_all(False, *s3)
    unpack(advance_ring(rows, rs3, rsc3, 0), x4)
    sq = [None] * SCALES
    for b in range(NB):
        cur = step(b, 3, x4)
        for s in range(SCALES):
            t = tot[s, b] + cof_s[s, 4] * cur
            tot[s, b] = t
            sq[s] = t * t if sq[s] is None else sq[s] + t * t

    m = jnp.concatenate(sq, axis=0)
    hi = m.astype(jnp.bfloat16)
    r1 = m - hi.astype(jnp.float32)
    mid = r1.astype(jnp.bfloat16)
    lo = (r1 - mid.astype(jnp.float32)).astype(jnp.bfloat16)
    ones = jnp.ones((16, TILE), jnp.bfloat16)
    row = None
    for part in (lo, mid, hi):
        p = lax.dot_general(ones, part, (((1,), (1,)), ((), ())), preferred_element_type=jnp.float32)
        row = p if row is None else row + p
    row = jnp.concatenate([row[0:1], jnp.zeros((1, TILE - SCALES * SIG), jnp.float32)], axis=1)

    ga[me] = row
    pl.semaphore_wait(in_xy, 7)
    for o in FAR_FIRST:
        pltpu.make_async_remote_copy(
            src_ref=ga.at[me], dst_ref=ga.at[me], send_sem=sa, recv_sem=ra,
            device_id=other(o), device_id_type=MESH).start()
    wait_all(True, *v3, *s3)
    many = ga.at[pl.ds(0, DEVICES - 1)]
    pltpu.make_async_remote_copy(
        src_ref=many, dst_ref=many, send_sem=sa, recv_sem=ra, device_id=other(1), device_id_type=MESH).wait_recv()
    sums = [ga[q] for q in range(DEVICES)]
    while len(sums) > 1:
        sums = [u + v for u, v in zip(sums[::2], sums[1::2])]
    full = sums[0] * (1.0 / NODES)
    res = jnp.zeros((8, TILE), jnp.float32)
    sub = lax.broadcasted_iota(jnp.int32, (8, TILE), 0)
    full8 = jnp.broadcast_to(full, (8, TILE))
    for s in range(SCALES):
        v = pltpu.roll(full8, TILE - 16 * s, 1) if s else full8
        res = jnp.where(sub == s, v, res)
    en_ref[...] = res[:SCALES, :SIG]

    pltpu.make_async_remote_copy(
        src_ref=many, dst_ref=many, send_sem=sa, recv_sem=ra, device_id=other(1), device_id_type=MESH).wait_send()


def finish(tot, en, out_h, en_h, sem):
    a = pltpu.make_async_copy(tot, out_h, sem.at[0])
    b = pltpu.make_async_copy(en, en_h, sem.at[1])
    a.start()
    b.start()
    a.wait()
    b.wait()


def shards(signals, tiles, tile_dir, tile_mask, live_rows, bound_rows, scale_coeffs, spectral_bound):
    bf, f32, i32 = jnp.bfloat16, jnp.float32, jnp.int32
    vm, sm = pltpu.VMEM, pltpu.SMEM
    in_vmem = pl.BlockSpec(memory_space=pltpu.VMEM)
    hbm = pl.BlockSpec(memory_space=pl.ANY)
    dma = pltpu.SemaphoreType.DMA
    tot, energy = pl.pallas_call(
        kernel,
        out_shape=(pltpu.VMEM((SCALES, NB, SIG, TILE), f32), pltpu.VMEM((SCALES, SIG), f32)),
        in_specs=[hbm] * 7 + [pl.BlockSpec(memory_space=pltpu.HBM)],
        out_specs=(in_vmem, in_vmem),
        scratch_shapes=[
            sm((BX, SLOTS, BY), i32), sm((BX, SLOTS, BY), i32), sm((BX, BY), i32), sm((BX, BY), i32),
            sm((SCALES, DEG + 1), f32), sm((1,), f32),
            vm((BX, BY, SIG, TILE), f32), vm((NB, SLOTS, TILE, TILE), bf),
            sm((NB * SLOTS,), i32), sm((NB * SLOTS,), i32), sm((NB * SLOTS,), i32),
            vm((NX, 32, TILE), bf), vm((NX, SIG, TILE), bf), vm((NX, SIG, TILE), bf), vm((NX, SIG, TILE), bf),
            vm((NR + 1, SLOTS, 32, TILE), bf), vm((NR + 1, SLOTS, SIG, TILE), bf),
            vm((DEG, NB, SIG, TILE), f32), vm((NB, SIG, TILE), f32), vm((NB, 8, TILE), f32), vm((NB, 8, TILE), f32),
            vm((NB, TILE, TILE), bf),
            vm((2, 2, SIG, TILE), bf), vm((2, 2, SIG, TILE), bf), vm((2, 2, 1, TILE), f32),
            vm((2, 2, SIG, TILE), f32), vm((2, 2, SIG, TILE), bf), vm((2, 9, 32, TILE), bf),
            vm((2, SIG, TILE), bf), vm((2, SIG, TILE), bf), vm((2, 1, TILE), f32), vm((2, SIG, TILE), f32), vm((2, SIG, TILE), bf),
            vm((8, 2, 2, SIG, TILE), bf), vm((8, 2, 2, SIG, TILE), bf), vm((8, 2, 2, 1, TILE), f32),
            vm((8, 2, 2, SIG, TILE), f32), vm((8, 2, 2, SIG, TILE), bf), vm((8, 2, 9, 32, TILE), bf),
            vm((8, 2, SIG, TILE), bf), vm((8, 2, SIG, TILE), bf), vm((8, 2, 1, TILE), f32),
            vm((8, 2, SIG, TILE), f32), vm((8, 2, SIG, TILE), bf),
            vm((DEVICES, 1, TILE), f32), vm((1024, 1, TILE), f32),
            dma((11,)), dma, dma, dma, dma, dma, dma,
            dma, dma, pltpu.SemaphoreType.REGULAR, pltpu.SemaphoreType.REGULAR,
        ],
        compiler_params=pltpu.CompilerParams(collective_id=0, has_side_effects=True),
        name="wavelet",
    )(signals, tiles, jnp.swapaxes(tile_dir, 1, 2), jnp.swapaxes(tile_mask, 1, 2), live_rows, bound_rows,
      scale_coeffs, spectral_bound)
    out, energy = pl.pallas_call(
        finish,
        out_shape=(jax.ShapeDtypeStruct((SCALES, NB, SIG, TILE), f32), jax.ShapeDtypeStruct((SCALES, SIG), f32)),
        in_specs=[in_vmem, in_vmem],
        out_specs=(hbm, hbm),
        scratch_shapes=[dma((2,))],
        name="finish",
    )(pltpu.with_memory_space_constraint(tot, pltpu.VMEM), pltpu.with_memory_space_constraint(energy, pltpu.VMEM))
    return out.reshape(SCALES, BX, BY, SIG, TILE), energy


def solution(mesh):
    placed = (
        P("gx", "gy", None, None),
        P("gx", "gy", None, None, None),
        P("gx", "gy", None),
        P("gx", "gy", None),
        P("gx", "gy"),
        P("gx", "gy"),
        P(),
        P(),
    )
    return jax.shard_map(
        shards,
        mesh=mesh,
        in_specs=placed,
        out_specs=(P(None, "gx", "gy", None, None), P()),
        check_vma=False,
    )
```
